128 devices in a mesh: lat: 16 (over y, z), lon: 8 (over x, core).
Axes of the slice: x: 4, y: 4, z: 4, core: 2. Of those that a mesh axis runs over, the one named last changes fastest.
Arguments:
- features: bfloat16 [1572864, 128], P(('lat', 'lon')), may hold values from -6 to 6
- cell_index: int32 [1572864], P(('lat', 'lon')), may hold values from 0 to 2547
- tile_rows: int32 [16384], P(('lat', 'lon')), may hold values from 1 to 96, as said below
- spread: float32 [3, 3], replicated, may hold values from 0.2 to 1
- w_in: bfloat16 [128, 256], replicated, may hold values from -0.5 to 0.5
- w_dens: float32 [256], replicated, may hold values from -3 to 3
- w_one: bfloat16 [3, 3, 256, 256], replicated, may hold values from -0.125 to 0.125
- w_two: bfloat16 [3, 3, 256, 256], replicated, may hold values from -0.125 to 0.125
Outputs:
- encoded: bfloat16 [384, 768, 256], P('lat', 'lon')
The draws below stay inside these ranges and needn't reach their ends.
Inputs may be any that keep to these rules, and one draw needn't show every extreme that they name: `tile_rows`: every block has 1 to 96 used slots; on every device some block has exactly 96.
All inputs are finite; a program needn't handle non-finite values.
Results may differ from the reference program's by a relative error of at most 0.0054.
Values may be sent and summed in bfloat16 or wider, within the bound.
No kernel may reach another device: no remote copies, remote signals or barrier semaphores. Data moves between devices by JAX's collectives and lax.ppermute only.
A program may use at most 64 MiB of HBM per device.

```python
import math
import jax
import jax.numpy as jnp
from jax import lax

TH = 24
TW = 96
F = 128
C = 256
CAP = 96
TILES = 128
OBS_ALL = 1572864
PH = 26
PW = 98
GH = 384
GW = 768
N_LAT = 16
N_LON = 8
DEVICES = 128


def draw_tile_rows(key, part):
    heat = jax.random.randint(jax.random.fold_in(key, 11), (TILES,), 1, 5)
    low = jnp.maximum(1, heat * CAP // 8)
    high = heat * CAP // 4 + 1
    counts = jax.random.randint(jax.random.fold_in(key, 12), (DEVICES, TILES), low[None, :], high[None, :])
    counts = jnp.minimum(counts, CAP)
    forced = jax.random.randint(jax.random.fold_in(key, 13), (DEVICES,), 0, TILES)
    tile_ids = jnp.arange(TILES, dtype=jnp.int32)
    counts = jnp.where(tile_ids[None, :] == forced[:, None], CAP, counts)
    return counts.reshape(DEVICES * TILES).astype(jnp.int32)


def with_ends(entries, own_key, smallest, largest):
    longest = entries.shape.index(max(entries.shape))
    spots = []
    for shift in (0, 1):
        where = [jax.random.randint(jax.random.fold_in(own_key, axis), (), 0, length) for axis, length in enumerate(entries.shape)]
        where[longest] = (where[longest] + shift) % entries.shape[longest]
        spots.append(tuple(where))
    return entries.at[spots[0]].set(smallest).at[spots[1]].set(largest)


def level_of(key, extent, cuts, low, high):
    gain, own = 1.0, jax.random.fold_in(key, 6)
    for position, blocks in cuts:
        steps = jnp.exp(jax.random.uniform(jax.random.fold_in(own, position), (blocks,), jnp.float32, low / len(cuts), high / len(cuts)))
        gain = gain * jnp.repeat(steps, extent[position] // blocks).reshape([-1 if axis == position else 1 for axis in range(len(extent))])
    return gain


def bell_draw(key, shape, scale, limit, cuts=(), held_as=jnp.bfloat16):
    values = jax.random.normal(key, shape, jnp.float32) * scale
    if len(cuts) > 0:
        values = level_of(key, shape, cuts, -0.22, 0.18) * values
    return jnp.clip(values, min=-limit, max=limit).astype(held_as)


def setup_inputs(seed: int = 0) -> dict:
    seeds = jax.random.split(jax.random.key(seed), 9)
    return {
        "features": bell_draw(seeds[0], (OBS_ALL, F), 1.0, 6.0, ((0, 128),)),
        "cell_index": with_ends(jax.random.randint(seeds[1], (OBS_ALL,), 0, PH * PW), jax.random.fold_in(seeds[1], 1), 0, (PH * PW) - 1).astype(jnp.int32),
        "tile_rows": draw_tile_rows(jax.random.fold_in(seeds[8], 71), 0),
        "spread": jnp.clip(jnp.exp(jax.random.uniform(seeds[3], (3, 3), jnp.float32, math.log(0.2), math.log(1.0))), 0.2, 1.0),
        "w_in": bell_draw(seeds[4], (F, C), F ** -0.5, 0.5),
        "w_dens": bell_draw(seeds[5], (C,), 0.5, 3.0, (), jnp.float32),
        "w_one": bell_draw(seeds[6], (3, 3, C, C), (9 * C) ** -0.5, 0.125),
        "w_two": bell_draw(seeds[7], (3, 3, C, C), (9 * C) ** -0.5, 0.125),
    }


def wrap_pad(field):
    cols = jnp.concatenate([field[:, -1:], field, field[:, :1]], axis=1)
    return jnp.pad(cols, ((1, 1), (0, 0), (0, 0)))


def conv_grid(field, weight):
    padded = wrap_pad(field)
    rows_all, cols_all, chans = field.shape
    total = jnp.zeros((rows_all * cols_all, weight.shape[3]), jnp.float32)
    for row_off in range(3):
        for col_off in range(3):
            window = padded[row_off:row_off + rows_all, col_off:col_off + cols_all].reshape(-1, chans)
            total = total + jnp.dot(window, weight[row_off, col_off], preferred_element_type=jnp.float32)
    return total.reshape(rows_all, cols_all, -1)


def reference(features, cell_index, tile_rows, spread, w_in, w_dens, w_one, w_two):
    tiles = N_LAT * N_LON
    frame_cells = PH * PW
    blocks = features.reshape(DEVICES, tiles, CAP, F)
    cell_blocks = cell_index.reshape(DEVICES, tiles, CAP)
    counts = tile_rows.reshape(DEVICES, tiles)
    slot_ids = jnp.arange(CAP, dtype=jnp.int32)

    def one_tile(tile):
        rows = lax.dynamic_index_in_dim(blocks, tile, 1, keepdims=False)
        cells = lax.dynamic_index_in_dim(cell_blocks, tile, 1, keepdims=False)
        used = lax.dynamic_index_in_dim(counts, tile, 1, keepdims=False)
        valid = slot_ids[None, :] < used[:, None]
        segment = jnp.where(valid, cells, frame_cells).reshape(-1).astype(jnp.int32)
        sums = jax.ops.segment_sum(rows.reshape(-1, F).astype(jnp.float32), segment, num_segments=frame_cells + 1)
        numbers = jax.ops.segment_sum(jnp.ones(segment.shape, jnp.float32), segment, num_segments=frame_cells + 1)
        return sums[:frame_cells], numbers[:frame_cells]

    frame_sum, frame_count = lax.map(one_tile, jnp.arange(tiles, dtype=jnp.int32))
    frame_sum = frame_sum.reshape(tiles, PH, PW, F)
    frame_count = frame_count.reshape(tiles, PH, PW)
    data = jnp.zeros((tiles, TH, TW, F), jnp.float32)
    density = jnp.zeros((tiles, TH, TW), jnp.float32)
    for row_off in range(3):
        for col_off in range(3):
            data = data + spread[row_off, col_off] * frame_sum[:, row_off:row_off + TH, col_off:col_off + TW]
            density = density + spread[row_off, col_off] * frame_count[:, row_off:row_off + TH, col_off:col_off + TW]
    mean = (data / (1.0 + density)[..., None]).astype(jnp.bfloat16)
    grid = jnp.dot(mean.reshape(-1, F), w_in, preferred_element_type=jnp.float32)
    grid = grid + jnp.log1p(density).reshape(-1, 1) * w_dens[None, :]
    grid = grid.astype(jnp.bfloat16).reshape(N_LAT, N_LON, TH, TW, C)
    grid = jnp.transpose(grid, (0, 2, 1, 3, 4)).reshape(GH, GW, C)
    hidden = jax.nn.silu(conv_grid(grid, w_one)).astype(jnp.bfloat16)
    encoded = grid.astype(jnp.float32) + conv_grid(hidden, w_two)
    return encoded.astype(jnp.bfloat16)
```

```python
import functools

import jax
import jax.numpy as jnp
from jax import lax
from jax.experimental import pallas as pl
from jax.experimental.pallas import tpu as pltpu
from jax.sharding import PartitionSpec as P

TH = 24
TW = 96
F = 128
C = 256
CAP = 96
PH = 26
PW = 98
NP = 6
NQ = 16
HALF = PH // 2
SOURCES = 128
ROWS = CAP + 8
MAIN = HALF * TW
LHS = MAIN + 32
GROUPS = 4
BF = jnp.bfloat16
F32 = jnp.float32


def dot(a, b):
    return jnp.dot(a, b, preferred_element_type=F32)


def iota(shape, dim):
    return lax.broadcasted_iota(jnp.int32, shape, dim)


def with_row(tile, shift, row, at):
    rolled = pltpu.roll(tile, shift, 0)
    return jnp.where(iota(tile.shape, 0) == at, row, rolled)


def frame_kernel(
    x_ref, spread_ref, win_ref, wdens_ref, grid_ref, west_ref, east_ref, c32, lanes, acc, cnt, fr, mean, cols
):
    c32[...] = x_ref[:, CAP:, :].astype(F32).reshape(SOURCES * 8, 128)

    def placed(which):
        return [pltpu.roll(c32[pl.ds(8 * j + which, 32, stride=32), :], (96 * j) % 128, 1) for j in range(4)]

    lane = iota((32, 128), 1)

    def joined(parts):
        return [
            jnp.where(lane < 96, parts[0], parts[1]),
            jnp.where(lane < 64, parts[1], parts[2]),
            jnp.where(lane < 32, parts[2], parts[3]),
        ]

    for v, (r, pos) in enumerate(zip(joined(placed(0)), joined(placed(1)))):
        low = jnp.where(r >= HALF, r - HALF, r)
        edge = jnp.where(pos >= TW, low + HALF * (pos - TW), -1.0)
        lanes[0, v] = r
        lanes[1, v] = low
        lanes[2, v] = pos
        lanes[3, v] = edge
    upper = jnp.where(c32[pl.ds(0, SOURCES, stride=8), :] >= HALF, 1.0, 0.0)
    upper = jnp.transpose(upper)

    per = SOURCES // GROUPS
    for g in range(GROUPS):
        units = per // 4

        def row(which):
            pieces = [lanes[which, v, pl.ds(g * units + u, 1), :] for u in range(units) for v in range(3)]
            return jnp.broadcast_to(jnp.concatenate(pieces, axis=1), (16, per * CAP)).astype(BF)

        r16, low16, pos16, edge16 = (row(w) for w in range(4))
        one, zero = jnp.ones((), BF), jnp.zeros((), BF)
        ids = iota((16, per * CAP), 0).astype(F32).astype(BF)

        def hot(values, tile):
            return jnp.where(ids + jnp.asarray(16 * tile, BF) == values, one, zero)

        place = [hot(pos16, t) for t in range(8)]
        parts = []
        for k in range(HALF):
            at = jnp.where(low16 == jnp.asarray(k, BF), one, zero)
            parts += [b * at for b in place[:NP]]
        parts += [hot(edge16, 0), hot(edge16, 1)]
        left = jnp.concatenate(parts, axis=0)
        right = []
        for s in range(g * per, (g + 1) * per):
            x = x_ref[s, :CAP, :]
            up = x * jnp.broadcast_to(upper[:CAP, s : s + 1], (CAP, 128)).astype(BF)
            right.append(jnp.concatenate([x - up, up], axis=1))
        part = dot(left, jnp.concatenate(right, axis=0))
        some = lax.dot_general(
            jnp.concatenate(place, axis=0),
            jnp.concatenate([hot(r16, 0), hot(r16, 1)], axis=0),
            (((1,), (1,)), ((), ())),
            preferred_element_type=F32,
        )
        if g == 0:
            acc[...] = part
            cnt[...] = some
        else:
            acc[...] += part
            cnt[...] += some

    for r in range(PH):
        base, side = (r % HALF) * TW, (r // HALF) * 128
        lanes_of = slice(side, side + 128)
        tile = acc[base : base + TW, lanes_of].reshape(NP, NQ, 128)
        fr[r, 1 : NP + 1] = tile
        first = acc[MAIN + r % HALF : MAIN + r % HALF + 1, lanes_of]
        last = acc[MAIN + HALF + r % HALF : MAIN + HALF + r % HALF + 1, lanes_of]
        fr[r, 0] = with_row(tile[NP - 1], 1, first, 0)
        fr[r, NP + 1] = with_row(tile[0], NQ - 1, last, NQ - 1)

    number = cnt[...]
    number = [
        with_row(number[TW - NQ : TW], 1, number[TW : TW + 1], 0),
        *(number[NQ * p : NQ * (p + 1)] for p in range(NP)),
        with_row(number[:NQ], NQ - 1, number[TW + 1 : TW + 2], NQ - 1),
    ]
    density = None
    for a in range(3):
        line = [sum(spread_ref[a, b] * number[p + b] for b in range(3)) for p in range(NP)]
        line = jnp.concatenate(line, axis=0)[:, a : a + TH]
        density = line if density is None else density + line
    scale = 1.0 / (1.0 + density)
    log_density = jnp.log(1.0 + density)

    for i in range(TH):
        data = None
        for a in range(3):
            for b in range(3):
                term = spread_ref[a, b] * fr[i + a, b : b + NP]
                data = term if data is None else data + term
        data = data.reshape(TW, F) * jnp.broadcast_to(scale[:, i : i + 1], (TW, F))
        mean[i * TW : (i + 1) * TW, :] = data.astype(BF)
    step = 4
    for i in range(0, TH, step):
        out = dot(mean[i * TW : (i + step) * TW, :], win_ref[...])
        for k in range(step):
            extra = jnp.broadcast_to(log_density[:, i + k : i + k + 1], (TW, C)) * wdens_ref[...]
            cell = (out[k * TW : (k + 1) * TW] + extra).astype(BF)
            grid_ref[i + k] = cell.reshape(NP, NQ, C)
            wide = cell.astype(F32)
            for c, at in enumerate((0, NQ, 5 * NQ - 1, 6 * NQ - 1)):
                cols[c, i + k : i + k + 1, :] = wide[at : at + 1]
    west_ref[...] = cols[0:2].astype(BF)
    east_ref[...] = cols[2:4].astype(BF)


def silu(v):
    return v / (1.0 + jnp.exp(-v))


def conv_kernel(
    lat_ref, grid_ref, north_ref, south_ref, west_ref, east_ref, one_ref, two_ref, out_ref, gp, hp, cs, hs, flat
):
    lat = lat_ref[0]
    keep_top = jnp.where(lat > 0, 1.0, 0.0)
    keep_bottom = jnp.where(lat < 15, 1.0, 0.0)
    cs[...] = jnp.zeros_like(cs)
    for c in range(4):
        ref = west_ref if c < 2 else east_ref
        cs[c, 2 : 2 + TH, :] = ref[c % 2].astype(F32)
    for ref, at in ((north_ref, 0), (south_ref, 2 + TH)):
        corner = ref[2 * TW : 2 * TW + 8].astype(F32)
        for c in range(4):
            cs[c, at : at + 2, :] = corner[2 * c : 2 * c + 2]
    for g in range(TH + 4):
        if g < 2:
            tile = north_ref[g * TW : (g + 1) * TW].reshape(NP, NQ, C)
        elif g < TH + 2:
            tile = grid_ref[g - 2]
        else:
            tile = south_ref[(g - TH - 2) * TW : (g - TH - 1) * TW].reshape(NP, NQ, C)
        gp[g, 1 : NP + 1] = tile
        first, last = tile[0].astype(F32), tile[NP - 1].astype(F32)
        cs[4, g : g + 1, :] = first[:1]
        cs[5, g : g + 1, :] = last[NQ - 1 :]
        gp[g, 0] = with_row(last, 1, cs[1, g : g + 1, :], 0).astype(BF)
        gp[g, NP + 1] = with_row(first, NQ - 1, cs[2, g : g + 1, :], NQ - 1).astype(BF)

    side = None
    for a in range(3):
        for b in range(3):
            lhs = jnp.concatenate(
                [cs[(0, 1, 4)[b], a : a + 32, :], cs[(5, 2, 3)[b], a : a + 32, :]], axis=0
            ).astype(BF)
            term = dot(lhs, one_ref[3 * a + b])
            side = term if side is None else side + term
    side = silu(side)
    line = iota((64, C), 0)
    side = jnp.where((line == 0) | (line == 32), side * keep_top, side)
    side = jnp.where((line == TH + 1) | (line == TH + 33), side * keep_bottom, side)
    hs[...] = side

    def rows_of(src, weight, start, count):
        total = None
        for a in range(3):
            for b in range(3):
                window = src[start + a : start + a + count, b : b + NP].reshape(count * TW, C)
                term = dot(window, weight[3 * a + b])
                total = term if total is None else total + term
        return total

    start = 0
    for count in (4, 4, 4, 4, 4, 4, 2):
        value = silu(rows_of(gp, one_ref, start, count))
        for k in range(count):
            g = start + k
            row = value[k * TW : (k + 1) * TW]
            if g == 0:
                row = row * keep_top
            if g == TH + 1:
                row = row * keep_bottom
            row = row.reshape(NP, NQ, C)
            hp[g, 1 : NP + 1] = row.astype(BF)
            hp[g, 0] = with_row(row[NP - 1], 1, hs[g : g + 1, :], 0).astype(BF)
            hp[g, NP + 1] = with_row(row[0], NQ - 1, hs[32 + g : 33 + g, :], NQ - 1).astype(BF)
        start += count

    step = 4
    for i in range(0, TH, step):
        value = rows_of(hp, two_ref, i, step).reshape(step, NP, NQ, C)
        value = value + grid_ref[i : i + step].astype(F32)
        for k in range(step):
            for p in range(NP):
                for h in range(2):
                    flat[h, pl.ds((i + k) * TW + p, NQ, stride=NP), :] = value[k, p, :, 128 * h : 128 * (h + 1)]
        for h in range(2):
            done = flat[h, i * TW : (i + step) * TW, :].astype(BF)
            out_ref[i : i + step, :, 128 * h : 128 * (h + 1)] = done.reshape(step, TW, 128)


def vmem(count):
    return [pl.BlockSpec(memory_space=pltpu.VMEM)] * count


def smem():
    return pl.BlockSpec(memory_space=pltpu.SMEM)


LIMIT = 60 * 1024 * 1024


def frame_call(received, spread, w_in, w_dens):
    return pl.pallas_call(
        frame_kernel,
        out_shape=(
            jax.ShapeDtypeStruct((TH, NP, NQ, C), BF),
            jax.ShapeDtypeStruct((2, TH, C), BF),
            jax.ShapeDtypeStruct((2, TH, C), BF),
        ),
        in_specs=[*vmem(1), smem(), *vmem(2)],
        out_specs=tuple(vmem(3)),
        scratch_shapes=[
            pltpu.VMEM((SOURCES * 8, 128), F32),
            pltpu.VMEM((4, 3, 32, 128), F32),
            pltpu.VMEM((LHS, C), F32),
            pltpu.VMEM((128, 32), F32),
            pltpu.VMEM((PH, NP + 2, NQ, F), F32),
            pltpu.VMEM((TH * TW, F), BF),
            pltpu.VMEM((4, TH, C), F32),
        ],
        compiler_params=pltpu.CompilerParams(vmem_limit_bytes=LIMIT),
        name="frame",
    )(received, spread, w_in, w_dens.reshape(1, C))


def conv_call(lat, grid, north, south, west, east, w_one, w_two):
    return pl.pallas_call(
        conv_kernel,
        out_shape=jax.ShapeDtypeStruct((TH, TW, C), BF),
        in_specs=[smem(), *vmem(7)],
        out_specs=vmem(1)[0],
        scratch_shapes=[
            pltpu.VMEM((TH + 4, NP + 2, NQ, C), BF),
            pltpu.VMEM((TH + 2, NP + 2, NQ, C), BF),
            pltpu.VMEM((6, 40, C), F32),
            pltpu.VMEM((64, C), F32),
            pltpu.VMEM((2, TH * TW, 128), F32),
        ],
        compiler_params=pltpu.CompilerParams(vmem_limit_bytes=LIMIT),
        name="conv",
    )(lat, grid, north, south, west, east, w_one.reshape(9, C, C), w_two.reshape(9, C, C))


def payload(features, cell_index, tile_rows):
    slot = jnp.arange(CAP, dtype=jnp.int32)
    cells = cell_index.reshape(SOURCES, CAP)
    r = cells // PW
    s = cells - r * PW
    j = s - 1
    q = j // NP
    pos = (j - q * NP) * NQ + q
    pos = jnp.where(s == 0, TW, jnp.where(s == PW - 1, TW + 1, pos))
    r = jnp.where(slot[None, :] < tile_rows[:, None], r, 63)
    where = jnp.stack([r, pos], axis=1).astype(F32).astype(BF)
    where = jnp.pad(where, ((0, 0), (0, 6), (0, 128 - CAP)))
    return jnp.concatenate([features.reshape(SOURCES, CAP, F), where], axis=1)


def step(axis, by, around):
    count = lax.axis_size(axis)
    return [(i, (i + by) % count) for i in range(count) if around or 0 <= i + by < count]


def shards(features, cell_index, tile_rows, spread, w_in, w_dens, w_one, w_two):
    sent = payload(features, cell_index, tile_rows)
    received = lax.all_to_all(sent, ("lat", "lon"), split_axis=0, concat_axis=0, tiled=True)
    grid, west_cols, east_cols = frame_call(received, spread, w_in, w_dens)
    from_west = lax.ppermute(east_cols, "lon", step("lon", 1, True))
    from_east = lax.ppermute(west_cols, "lon", step("lon", -1, True))

    def edge_rows(at):
        corner = jnp.concatenate([from_west[:, at : at + 2], from_east[:, at : at + 2]], axis=0)
        return jnp.concatenate([grid[at : at + 2].reshape(2 * TW, C), corner.reshape(8, C)], axis=0)

    from_north = lax.ppermute(edge_rows(TH - 2), "lat", step("lat", 1, False))
    from_south = lax.ppermute(edge_rows(0), "lat", step("lat", -1, False))
    lat = lax.axis_index("lat").reshape(1).astype(jnp.int32)
    return conv_call(lat, grid, from_north, from_south, from_west, from_east, w_one, w_two)


def solution(mesh):
    in_specs = (
        P(("lat", "lon"), None),
        P(("lat", "lon")),
        P(("lat", "lon")),
        P(),
        P(),
        P(),
        P(),
        P(),
    )
    out_specs = P("lat", "lon", None)
    return jax.shard_map(shards, mesh=mesh, in_specs=in_specs, out_specs=out_specs, check_vma=False)
```

```python
import functools

import jax
import jax.numpy as jnp
from jax import lax
from jax.experimental import pallas as pl
from jax.experimental.pallas import tpu as pltpu
from jax.sharding import PartitionSpec as P

TH = 24
TW = 96
F = 128
C = 256
CAP = 96
PH = 26
PW = 98
NP = 6
NQ = 16
HALF = PH // 2
SOURCES = 128
ROWS = CAP + 2
PAIRS = ROWS // 2
MAIN = HALF * TW
LHS = MAIN + 32
GROUPS = 7
PER = ROWS // GROUPS
BF = jnp.bfloat16
F32 = jnp.float32


def dot(a, b):
    return jnp.dot(a, b, preferred_element_type=F32)


def iota(shape, dim):
    return lax.broadcasted_iota(jnp.int32, shape, dim)


def with_row(tile, shift, row, at):
    rolled = pltpu.roll(tile, shift, 0)
    return jnp.where(iota(tile.shape, 0) == at, row, rolled)


def send_kernel(shift_ref, features_ref, cells_ref, used_ref, out_ref, flat, where, sems):
    cut = SOURCES // 4
    copies = [
        pltpu.make_async_copy(
            features_ref.at[cut * k : cut * (k + 1)],
            out_ref.at[cut * k : cut * (k + 1), 0 : PAIRS - 1],
            sems.at[k],
        )
        for k in range(4)
    ]
    for copy in copies:
        copy.start()
    lines = [cells_ref[pl.ds(v, 32, stride=3), :].astype(F32) for v in range(3)]
    lane = iota((32, 128), 1)
    cells = [
        lines[0],
        jnp.where(lane < 32, pltpu.roll(lines[0], 32, 1), pltpu.roll(lines[1], 32, 1)),
        jnp.where(lane < 64, pltpu.roll(lines[1], 64, 1), pltpu.roll(lines[2], 64, 1)),
        pltpu.roll(lines[2], 96, 1),
    ]
    for j, cell in enumerate(cells):
        r = jnp.floor((cell + 0.5) * (1.0 / PW))
        s = cell - r * PW
        q = jnp.floor((s - 0.5) * (1.0 / NP))
        pos = (s - 1.0 - q * NP) * NQ + q
        pos = jnp.where(s == 0.0, float(TW), jnp.where(s == PW - 1.0, TW + 1.0, pos))
        r = jnp.where(lane < used_ref[:, j : j + 1], r, 63.0)
        flat[pl.ds(2 * j, 32, stride=8), :] = pltpu.roll(r, shift_ref[0], 1)
        flat[pl.ds(2 * j + 1, 32, stride=8), :] = pltpu.roll(pos, shift_ref[0], 1)
    for t in range(SOURCES):
        where[t, 0] = flat[2 * t : 2 * t + 2, :].astype(BF)
    last = pltpu.make_async_copy(where, out_ref.at[:, PAIRS - 1 : PAIRS], sems.at[4])
    last.start()
    for copy in copies:
        copy.wait()
    last.wait()


def frame_kernel(
    x_ref, where_ref, spread_ref, win_ref, wdens_ref, grid_ref, west_ref, east_ref, c32, lanes, acc, cnt, fr, mean, cols
):
    for t in range(SOURCES):
        c32[2 * t : 2 * t + 2, :] = where_ref[t, PAIRS - 1].astype(F32)
    both = jnp.concatenate([c32[pl.ds(w, SOURCES, stride=2), :] for w in range(2)], axis=1).astype(BF)
    high = 104
    tile = iota((high, 128), 0).astype(F32) * 128.0
    first = jnp.floor((tile + 0.5) * (1.0 / ROWS))
    source = iota((high, 128), 1).astype(F32)
    picked = [dot(jnp.where(source == first + k, 1.0, 0.0).astype(BF), both) for k in range(3)]
    bound = (first + 1.0) * ROWS - tile

    def joined(side):
        parts = [part[:, 128 * side : 128 * (side + 1)] for part in picked]
        return jnp.where(source < bound, parts[0], jnp.where(source < bound + ROWS, parts[1], parts[2]))

    r, pos = joined(0), joined(1)
    low = jnp.where(r >= HALF, r - HALF, r)
    lanes[0] = r
    lanes[1] = low
    lanes[2] = pos
    lanes[3] = jnp.where(pos >= TW, low + HALF * (pos - TW), -1.0)
    upper = jnp.where(r >= HALF, 1.0, 0.0)
    upper = jnp.transpose(jnp.concatenate([upper, jnp.zeros((128 - high, 128), F32)], axis=0))

    for g in range(GROUPS):
        tiles = range(g * PER, (g + 1) * PER)
        width = PER * 128

        def row(which):
            pieces = [lanes[which, t : t + 1, :] for t in tiles]
            return jnp.broadcast_to(jnp.concatenate(pieces, axis=1), (16, width)).astype(BF)

        r16, low16, pos16, edge16 = (row(w) for w in range(4))
        one, zero = jnp.ones((), BF), jnp.zeros((), BF)
        ids = iota((16, width), 0).astype(F32).astype(BF)

        def hot(values, tile):
            return jnp.where(ids + jnp.asarray(16 * tile, BF) == values, one, zero)

        place = [hot(pos16, t) for t in range(8)]
        parts = []
        for k in range(HALF):
            at = jnp.where(low16 == jnp.asarray(k, BF), one, zero)
            parts += [b * at for b in place[:NP]]
        parts += [hot(edge16, 0), hot(edge16, 1)]
        left = jnp.concatenate(parts, axis=0)
        right = []
        for t in tiles:
            x = x_ref[128 * t : 128 * (t + 1), :]
            up = x * jnp.broadcast_to(upper[:, t : t + 1], (128, 128)).astype(BF)
            right.append(jnp.concatenate([x - up, up], axis=1))
        part = dot(left, jnp.concatenate(right, axis=0))
        some = lax.dot_general(
            jnp.concatenate(place, axis=0),
            jnp.concatenate([hot(r16, 0), hot(r16, 1)], axis=0),
            (((1,), (1,)), ((), ())),
            preferred_element_type=F32,
        )
        if g == 0:
            acc[...] = part
            cnt[...] = some
        else:
            acc[...] += part
            cnt[...] += some

    for r in range(PH):
        base, side = (r % HALF) * TW, (r // HALF) * 128
        lanes_of = slice(side, side + 128)
        tile = acc[base : base + TW, lanes_of].reshape(NP, NQ, 128)
        fr[r, 1 : NP + 1] = tile
        first = acc[MAIN + r % HALF : MAIN + r % HALF + 1, lanes_of]
        last = acc[MAIN + HALF + r % HALF : MAIN + HALF + r % HALF + 1, lanes_of]
        fr[r, 0] = with_row(tile[NP - 1], 1, first, 0)
        fr[r, NP + 1] = with_row(tile[0], NQ - 1, last, NQ - 1)

    number = cnt[...]
    number = [
        with_row(number[TW - NQ : TW], 1, number[TW : TW + 1], 0),
        *(number[NQ * p : NQ * (p + 1)] for p in range(NP)),
        with_row(number[:NQ], NQ - 1, number[TW + 1 : TW + 2], NQ - 1),
    ]
    density = None
    for a in range(3):
        line = [sum(spread_ref[a, b] * number[p + b] for b in range(3)) for p in range(NP)]
        line = jnp.concatenate(line, axis=0)[:, a : a + TH]
        density = line if density is None else density + line
    scale = 1.0 / (1.0 + density)
    log_density = jnp.log(1.0 + density)

    for i in range(TH):
        data = None
        for a in range(3):
            for b in range(3):
                term = spread_ref[a, b] * fr[i + a, b : b + NP]
                data = term if data is None else data + term
        data = data.reshape(TW, F) * jnp.broadcast_to(scale[:, i : i + 1], (TW, F))
        mean[i * TW : (i + 1) * TW, :] = data.astype(BF)
    step = 4
    for i in range(0, TH, step):
        out = dot(mean[i * TW : (i + step) * TW, :], win_ref[...])
        for k in range(step):
            extra = jnp.broadcast_to(log_density[:, i + k : i + k + 1], (TW, C)) * wdens_ref[...]
            cell = (out[k * TW : (k + 1) * TW] + extra).astype(BF)
            grid_ref[i + k] = cell.reshape(NP, NQ, C)
            wide = cell.astype(F32)
            for c, at in enumerate((0, NQ, 5 * NQ - 1, 6 * NQ - 1)):
                cols[c, i + k : i + k + 1, :] = wide[at : at + 1]
    west_ref[...] = cols[0:2].astype(BF)
    east_ref[...] = cols[2:4].astype(BF)


def silu(v):
    return v / (1.0 + jnp.exp(-v))


def conv_kernel(
    lat_ref, grid_ref, north_ref, south_ref, west_ref, east_ref, one_ref, two_ref, out_ref, gp, hp, cs, hs, flat, done, sems
):
    lat = lat_ref[0]
    keep_top = jnp.where(lat > 0, 1.0, 0.0)
    keep_bottom = jnp.where(lat < 15, 1.0, 0.0)
    cs[...] = jnp.zeros_like(cs)
    for c in range(4):
        ref = west_ref if c < 2 else east_ref
        cs[c, 2 : 2 + TH, :] = ref[c % 2].astype(F32)
    for ref, at in ((north_ref, 0), (south_ref, 2 + TH)):
        corner = ref[2 * TW : 2 * TW + 8].astype(F32)
        for c in range(4):
            cs[c, at : at + 2, :] = corner[2 * c : 2 * c + 2]
    for g in range(TH + 4):
        if g < 2:
            tile = north_ref[g * TW : (g + 1) * TW].reshape(NP, NQ, C)
        elif g < TH + 2:
            tile = grid_ref[g - 2]
        else:
            tile = south_ref[(g - TH - 2) * TW : (g - TH - 1) * TW].reshape(NP, NQ, C)
        gp[g, 1 : NP + 1] = tile
        first, last = tile[0].astype(F32), tile[NP - 1].astype(F32)
        cs[4, g : g + 1, :] = first[:1]
        cs[5, g : g + 1, :] = last[NQ - 1 :]
        gp[g, 0] = with_row(last, 1, cs[1, g : g + 1, :], 0).astype(BF)
        gp[g, NP + 1] = with_row(first, NQ - 1, cs[2, g : g + 1, :], NQ - 1).astype(BF)

    side = None
    for a in range(3):
        for b in range(3):
            lhs = jnp.concatenate(
                [cs[(0, 1, 4)[b], a : a + 32, :], cs[(5, 2, 3)[b], a : a + 32, :]], axis=0
            ).astype(BF)
            term = dot(lhs, one_ref[3 * a + b])
            side = term if side is None else side + term
    side = silu(side)
    line = iota((64, C), 0)
    side = jnp.where((line == 0) | (line == 32), side * keep_top, side)
    side = jnp.where((line == TH + 1) | (line == TH + 33), side * keep_bottom, side)
    hs[...] = side

    def rows_of(src, weight, start, count):
        total = None
        for a in range(3):
            for b in range(3):
                window = src[start + a : start + a + count, b : b + NP].reshape(count * TW, C)
                term = dot(window, weight[3 * a + b])
                total = term if total is None else total + term
        return total

    start = 0
    for count in (4, 4, 4, 4, 4, 4, 2):
        value = silu(rows_of(gp, one_ref, start, count))
        for k in range(count):
            g = start + k
            row = value[k * TW : (k + 1) * TW]
            if g == 0:
                row = row * keep_top
            if g == TH + 1:
                row = row * keep_bottom
            row = row.reshape(NP, NQ, C)
            hp[g, 1 : NP + 1] = row.astype(BF)
            hp[g, 0] = with_row(row[NP - 1], 1, hs[g : g + 1, :], 0).astype(BF)
            hp[g, NP + 1] = with_row(row[0], NQ - 1, hs[32 + g : 33 + g, :], NQ - 1).astype(BF)
        start += count

    step = 4
    copies = []
    for i in range(0, TH, step):
        value = rows_of(hp, two_ref, i, step).reshape(step, NP, NQ, C)
        value = value + grid_ref[i : i + step].astype(F32)
        for k in range(step):
            for p in range(NP):
                for h in range(2):
                    flat[h, pl.ds((i + k) * TW + p, NQ, stride=NP), :] = value[k, p, :, 128 * h : 128 * (h + 1)]
        for h in range(2):
            block = flat[h, i * TW : (i + step) * TW, :].astype(BF)
            done[i : i + step, :, 128 * h : 128 * (h + 1)] = block.reshape(step, TW, 128)
        copy = pltpu.make_async_copy(done.at[i : i + step], out_ref.at[i : i + step], sems.at[i // step])
        copy.start()
        copies.append(copy)
    for copy in copies:
        copy.wait()


def vmem(count):
    return [pl.BlockSpec(memory_space=pltpu.VMEM)] * count


def smem():
    return pl.BlockSpec(memory_space=pltpu.SMEM)


LIMIT = 40 * 1024 * 1024


def near(value):
    return pltpu.with_memory_space_constraint(value, pltpu.VMEM)


def send_call(features, cell_index, tile_rows):
    here = lax.axis_index("lat") * lax.axis_size("lon") + lax.axis_index("lon")
    shift = lax.rem(here * ROWS, 128).reshape(1).astype(jnp.int32)
    return pl.pallas_call(
        send_kernel,
        out_shape=pltpu.VMEM((SOURCES, PAIRS, 2, F), BF),
        in_specs=[smem(), pl.BlockSpec(memory_space=pl.ANY), *vmem(2)],
        out_specs=vmem(1)[0],
        scratch_shapes=[
            pltpu.VMEM((2 * SOURCES, 128), F32),
            pltpu.VMEM((SOURCES, 1, 2, F), BF),
            pltpu.SemaphoreType.DMA((5,)),
        ],
        compiler_params=pltpu.CompilerParams(vmem_limit_bytes=LIMIT),
        name="send",
    )(shift, features.reshape(SOURCES, PAIRS - 1, 2, F), cell_index.reshape(96, 128), tile_rows.reshape(32, 4))


def frame_call(received, spread, w_in, w_dens):
    return pl.pallas_call(
        frame_kernel,
        out_shape=(
            pltpu.VMEM((TH, NP, NQ, C), BF),
            pltpu.VMEM((2, TH, C), BF),
            pltpu.VMEM((2, TH, C), BF),
        ),
        in_specs=[*vmem(2), smem(), *vmem(2)],
        out_specs=tuple(vmem(3)),
        scratch_shapes=[
            pltpu.VMEM((SOURCES * 2, 128), F32),
            pltpu.VMEM((4, 104, 128), F32),
            pltpu.VMEM((LHS, C), F32),
            pltpu.VMEM((128, 32), F32),
            pltpu.VMEM((PH, NP + 2, NQ, F), F32),
            pltpu.VMEM((TH * TW, F), BF),
            pltpu.VMEM((4, TH, C), F32),
        ],
        compiler_params=pltpu.CompilerParams(vmem_limit_bytes=LIMIT),
        name="frame",
    )(near(received.reshape(SOURCES * ROWS, F)), near(received), spread, near(w_in), near(w_dens.reshape(1, C)))


def conv_call(lat, grid, north, south, west, east, w_one, w_two):
    return pl.pallas_call(
        conv_kernel,
        out_shape=jax.ShapeDtypeStruct((TH, TW, C), BF),
        in_specs=[smem(), *vmem(7)],
        out_specs=pl.BlockSpec(memory_space=pl.ANY),
        scratch_shapes=[
            pltpu.VMEM((TH + 4, NP + 2, NQ, C), BF),
            pltpu.VMEM((TH + 2, NP + 2, NQ, C), BF),
            pltpu.VMEM((6, 40, C), F32),
            pltpu.VMEM((64, C), F32),
            pltpu.VMEM((2, TH * TW, 128), F32),
            pltpu.VMEM((TH, TW, C), BF),
            pltpu.SemaphoreType.DMA((6,)),
        ],
        compiler_params=pltpu.CompilerParams(vmem_limit_bytes=LIMIT),
        name="conv",
    )(
        lat,
        near(grid),
        near(north),
        near(south),
        near(west),
        near(east),
        near(w_one.reshape(9, C, C)),
        near(w_two.reshape(9, C, C)),
    )


def step(axis, by, around):
    count = lax.axis_size(axis)
    return [(i, (i + by) % count) for i in range(count) if around or 0 <= i + by < count]


def shards(features, cell_index, tile_rows, spread, w_in, w_dens, w_one, w_two):
    sent = send_call(features, cell_index, tile_rows)
    received = lax.all_to_all(sent, ("lat", "lon"), split_axis=0, concat_axis=0, tiled=True)
    grid, west_cols, east_cols = frame_call(received, spread, w_in, w_dens)
    from_west = lax.ppermute(east_cols, "lon", step("lon", 1, True))
    from_east = lax.ppermute(west_cols, "lon", step("lon", -1, True))

    def edge_rows(at):
        corner = jnp.concatenate([from_west[:, at : at + 2], from_east[:, at : at + 2]], axis=0)
        return jnp.concatenate([grid[at : at + 2].reshape(2 * TW, C), corner.reshape(8, C)], axis=0)

    from_north = lax.ppermute(edge_rows(TH - 2), "lat", step("lat", 1, False))
    from_south = lax.ppermute(edge_rows(0), "lat", step("lat", -1, False))
    lat = lax.axis_index("lat").reshape(1).astype(jnp.int32)
    return conv_call(lat, grid, from_north, from_south, from_west, from_east, w_one, w_two)


def solution(mesh):
    in_specs = (
        P(("lat", "lon"), None),
        P(("lat", "lon")),
        P(("lat", "lon")),
        P(),
        P(),
        P(),
        P(),
        P(),
    )
    out_specs = P("lat", "lon", None)
    return jax.shard_map(shards, mesh=mesh, in_specs=in_specs, out_specs=out_specs, check_vma=False)
```

```python
import functools

import jax
import jax.numpy as jnp
from jax import lax
from jax.experimental import pallas as pl
from jax.experimental.pallas import tpu as pltpu
from jax.sharding import PartitionSpec as P

TH = 24
TW = 96
F = 128
C = 256
CAP = 96
PH = 26
PW = 98
NP = 6
NQ = 16
HALF = PH // 2
SOURCES = 128
ROWS = CAP + 2
PAIRS = ROWS // 2
MAIN = HALF * TW
EDGE = 2 * TW + 8
LHS = MAIN + 32
GROUPS = 7
PER = ROWS // GROUPS
BF = jnp.bfloat16
F32 = jnp.float32


def dot(a, b):
    return jnp.dot(a, b, preferred_element_type=F32)


def iota(shape, dim):
    return lax.broadcasted_iota(jnp.int32, shape, dim)


def with_row(tile, shift, row, at):
    rolled = pltpu.roll(tile, shift, 0)
    return jnp.where(iota(tile.shape, 0) == at, row, rolled)


def send_kernel(shift_ref, features_ref, index_ref, used_ref, out_ref, cells, flat, where, used, sems):
    fetch = pltpu.make_async_copy(index_ref, cells, sems.at[5])
    fetch.start()
    cut = SOURCES // 4
    copies = [
        pltpu.make_async_copy(
            features_ref.at[cut * k : cut * (k + 1)],
            out_ref.at[cut * k : cut * (k + 1), 0 : PAIRS - 1],
            sems.at[k],
        )
        for k in range(4)
    ]
    for copy in copies:
        copy.start()
    count = jnp.broadcast_to(used_ref[...].astype(F32), (128, 128))
    used[...] = jnp.transpose(count)
    fetch.wait()
    lines = [cells[pl.ds(v, 32, stride=3), :].astype(F32) for v in range(3)]
    lane = iota((32, 128), 1)
    blocks = [
        lines[0],
        jnp.where(lane < 32, pltpu.roll(lines[0], 32, 1), pltpu.roll(lines[1], 32, 1)),
        jnp.where(lane < 64, pltpu.roll(lines[1], 64, 1), pltpu.roll(lines[2], 64, 1)),
        pltpu.roll(lines[2], 96, 1),
    ]
    for j, cell in enumerate(blocks):
        r = jnp.floor((cell + 0.5) * (1.0 / PW))
        s = cell - r * PW
        q = jnp.floor((s - 0.5) * (1.0 / NP))
        pos = (s - 1.0 - q * NP) * NQ + q
        pos = jnp.where(s == 0.0, float(TW), jnp.where(s == PW - 1.0, TW + 1.0, pos))
        r = jnp.where(lane.astype(F32) < used[pl.ds(j, 32, stride=4), :], r, 63.0)
        flat[pl.ds(2 * j, 32, stride=8), :] = pltpu.roll(r, shift_ref[0], 1)
        flat[pl.ds(2 * j + 1, 32, stride=8), :] = pltpu.roll(pos, shift_ref[0], 1)
    for t in range(SOURCES):
        where[t, 0] = flat[2 * t : 2 * t + 2, :].astype(BF)
    last = pltpu.make_async_copy(where, out_ref.at[:, PAIRS - 1 : PAIRS], sems.at[4])
    last.start()
    for copy in copies:
        copy.wait()
    last.wait()


def frame_kernel(
    x_ref, where_ref, spread_ref, win_ref, wdens_ref, grid_ref, west_ref, east_ref, top_ref, bottom_ref, c32, lanes, acc, cnt, fr, mean, cols
):
    for t in range(SOURCES):
        c32[2 * t : 2 * t + 2, :] = where_ref[t, PAIRS - 1].astype(F32)
    both = jnp.concatenate([c32[pl.ds(w, SOURCES, stride=2), :] for w in range(2)], axis=1).astype(BF)
    high = 104
    tile = iota((high, 128), 0).astype(F32) * 128.0
    first = jnp.floor((tile + 0.5) * (1.0 / ROWS))
    source = iota((high, 128), 1).astype(F32)
    picked = [dot(jnp.where(source == first + k, 1.0, 0.0).astype(BF), both) for k in range(3)]
    bound = (first + 1.0) * ROWS - tile

    def joined(side):
        parts = [part[:, 128 * side : 128 * (side + 1)] for part in picked]
        return jnp.where(source < bound, parts[0], jnp.where(source < bound + ROWS, parts[1], parts[2]))

    r, pos = joined(0), joined(1)
    low = jnp.where(r >= HALF, r - HALF, r)
    lanes[0] = r
    lanes[1] = low
    lanes[2] = pos
    lanes[3] = jnp.where(pos >= TW, low + HALF * (pos - TW), -1.0)
    upper = jnp.where(r >= HALF, 1.0, 0.0)
    upper = jnp.transpose(jnp.concatenate([upper, jnp.zeros((128 - high, 128), F32)], axis=0))

    for g in range(GROUPS):
        tiles = range(g * PER, (g + 1) * PER)
        width = PER * 128

        def row(which):
            pieces = [lanes[which, t : t + 1, :] for t in tiles]
            return jnp.broadcast_to(jnp.concatenate(pieces, axis=1), (16, width)).astype(BF)

        r16, low16, pos16, edge16 = (row(w) for w in range(4))
        one, zero = jnp.ones((), BF), jnp.zeros((), BF)
        ids = iota((16, width), 0).astype(F32).astype(BF)

        def hot(values, tile):
            return jnp.where(ids + jnp.asarray(16 * tile, BF) == values, one, zero)

        place = [hot(pos16, t) for t in range(8)]
        parts = []
        for k in range(HALF):
            at = jnp.where(low16 == jnp.asarray(k, BF), one, zero)
            parts += [b * at for b in place[:NP]]
        parts += [hot(edge16, 0), hot(edge16, 1)]
        left = jnp.concatenate(parts, axis=0)
        right = []
        for t in tiles:
            x = x_ref[128 * t : 128 * (t + 1), :]
            up = x * jnp.broadcast_to(upper[:, t : t + 1], (128, 128)).astype(BF)
            right.append(jnp.concatenate([x - up, up], axis=1))
        part = dot(left, jnp.concatenate(right, axis=0))
        some = lax.dot_general(
            jnp.concatenate(place, axis=0),
            jnp.concatenate([hot(r16, 0), hot(r16, 1)], axis=0),
            (((1,), (1,)), ((), ())),
            preferred_element_type=F32,
        )
        if g == 0:
            acc[...] = part
            cnt[...] = some
        else:
            acc[...] += part
            cnt[...] += some

    for r in range(PH):
        base, side = (r % HALF) * TW, (r // HALF) * 128
        lanes_of = slice(side, side + 128)
        tile = acc[base : base + TW, lanes_of].reshape(NP, NQ, 128)
        fr[r, 1 : NP + 1] = tile
        first = acc[MAIN + r % HALF : MAIN + r % HALF + 1, lanes_of]
        last = acc[MAIN + HALF + r % HALF : MAIN + HALF + r % HALF + 1, lanes_of]
        fr[r, 0] = with_row(tile[NP - 1], 1, first, 0)
        fr[r, NP + 1] = with_row(tile[0], NQ - 1, last, NQ - 1)

    number = cnt[...]
    number = [
        with_row(number[TW - NQ : TW], 1, number[TW : TW + 1], 0),
        *(number[NQ * p : NQ * (p + 1)] for p in range(NP)),
        with_row(number[:NQ], NQ - 1, number[TW + 1 : TW + 2], NQ - 1),
    ]
    density = None
    for a in range(3):
        line = [sum(spread_ref[a, b] * number[p + b] for b in range(3)) for p in range(NP)]
        line = jnp.concatenate(line, axis=0)[:, a : a + TH]
        density = line if density is None else density + line
    scale = 1.0 / (1.0 + density)
    log_density = jnp.log(1.0 + density)

    for i in range(TH):
        data = None
        for a in range(3):
            for b in range(3):
                term = spread_ref[a, b] * fr[i + a, b : b + NP]
                data = term if data is None else data + term
        data = data.reshape(TW, F) * jnp.broadcast_to(scale[:, i : i + 1], (TW, F))
        mean[i * TW : (i + 1) * TW, :] = data.astype(BF)
    step = 4
    for i in range(0, TH, step):
        out = dot(mean[i * TW : (i + step) * TW, :], win_ref[...])
        for k in range(step):
            extra = jnp.broadcast_to(log_density[:, i + k : i + k + 1], (TW, C)) * wdens_ref[...]
            cell = (out[k * TW : (k + 1) * TW] + extra).astype(BF)
            grid_ref[i + k] = cell.reshape(NP, NQ, C)
            if i + k < 2:
                top_ref[(i + k) * TW : (i + k + 1) * TW, :] = cell
            if i + k >= TH - 2:
                bottom_ref[(i + k - TH + 2) * TW : (i + k - TH + 3) * TW, :] = cell
            wide = cell.astype(F32)
            for c, at in enumerate((0, NQ, 5 * NQ - 1, 6 * NQ - 1)):
                cols[c, i + k : i + k + 1, :] = wide[at : at + 1]
    west_ref[...] = cols[0:2].astype(BF)
    east_ref[...] = cols[2:4].astype(BF)


def silu(v):
    return v / (1.0 + jnp.exp(-v))


def corner_kernel(top_in, bottom_in, west_ref, east_ref, top_ref, bottom_ref, part):
    for source, ref, at in ((top_in, top_ref, 0), (bottom_in, bottom_ref, TH - 2)):
        for c in range(4):
            column = (west_ref if c < 2 else east_ref)[c % 2].astype(F32)
            part[2 * c : 2 * c + 2, :] = column[at : at + 2]
        ref[2 * TW : EDGE, :] = part[...].astype(BF)


def nine(weight, window):
    total = None
    for a in range(3):
        for b in range(3):
            term = dot(window(a, b), weight[3 * a + b])
            total = term if total is None else total + term
    return total


def rows_of(src, weight, start, count):
    return nine(weight, lambda a, b: src[start + a : start + a + count, b : b + NP].reshape(count * TW, C))


def padded(dst, at, tiles, first, last, before, after):
    dst[at, 1 : NP + 1] = tiles
    dst[at, 0] = with_row(last, 1, before, 0).astype(BF)
    dst[at, NP + 1] = with_row(first, NQ - 1, after, NQ - 1).astype(BF)


def spread_out(flat, at, tiles):
    for p in range(NP):
        for h in range(2):
            flat[h, pl.ds(at * TW + p, NQ, stride=NP), :] = tiles[p, :, 128 * h : 128 * (h + 1)]


def inner_one_kernel(grid_ref, one_ref, hp_ref, hcols_ref, gp):
    for g in range(TH):
        tile = grid_ref[g]
        first, last = tile[0].astype(F32), tile[NP - 1].astype(F32)
        padded(gp, g, tile, first, last, first[:1], last[NQ - 1 :])
    start = 0
    for count in (4, 4, 4, 4, 4, 2):
        value = silu(rows_of(gp, one_ref, start, count))
        for k in range(count):
            g = start + k + 2
            row = value[k * TW : (k + 1) * TW].reshape(NP, NQ, C)
            padded(hp_ref, g, row.astype(BF), row[0], row[NP - 1], row[0, :1], row[NP - 1, NQ - 1 :])
            for c, (p, q) in enumerate(((1, 0), (2, 0), (3, NQ - 1), (4, NQ - 1))):
                hcols_ref[c, g : g + 1, :] = row[p, q : q + 1]
        start += count


def inner_two_kernel(hp_ref, grid_ref, two_ref, out_ref, strips_ref, flat, done, sems):
    copies = []
    step = 4
    for i in range(2, TH - 2, step):
        value = rows_of(hp_ref, two_ref, i, step).reshape(step, NP, NQ, C)
        value = value + grid_ref[i : i + step].astype(F32)
        for k in range(step):
            spread_out(flat, i + k, value[k])
        for h in range(2):
            lanes = slice(128 * h, 128 * (h + 1))
            block = flat[h, i * TW : (i + step) * TW, :].astype(BF).reshape(step, TW, 128)
            done[i : i + step, :, lanes] = block
            strips_ref[0, i - 2 : i - 2 + step, :, lanes] = block[:, :8]
            strips_ref[1, i - 2 : i - 2 + step, :, lanes] = block[:, TW - 8 :]
        copy = pltpu.make_async_copy(done.at[i : i + step], out_ref.at[i : i + step], sems.at[i // step])
        copy.start()
        copies.append(copy)
    for copy in copies:
        copy.wait()


def ring_kernel(
    lat_ref,
    grid_ref,
    north_ref,
    south_ref,
    west_ref,
    east_ref,
    own_west_ref,
    own_east_ref,
    hp_ref,
    hcols_ref,
    strips_ref,
    one_ref,
    two_ref,
    partial_ref,
    out_ref,
    cs,
    gp,
    hc,
    hr,
    flat,
    oc,
    lines,
    strips,
    sems,
):
    lat = lat_ref[0]
    keep_top = jnp.where(lat > 0, 1.0, 0.0)
    keep_bottom = jnp.where(lat < 15, 1.0, 0.0)
    cs[:, 24:, :] = jnp.zeros((8, 16, C), F32)
    for n, ref in enumerate((west_ref, own_west_ref, own_east_ref, east_ref)):
        for c in range(2):
            cs[2 * n + c, 2 : 2 + TH, :] = ref[c].astype(F32)
    for ref, at in ((north_ref, 0), (south_ref, 2 + TH)):
        corner = ref[2 * TW : EDGE, :].astype(F32)
        for n, c in enumerate((0, 1, 6, 7)):
            cs[c, at : at + 2, :] = corner[2 * n : 2 * n + 2]
        for k in range(2):
            line = ref[k * TW : (k + 1) * TW, :].astype(F32)
            for c, place in ((2, 0), (3, NQ), (4, 5 * NQ - 1), (5, 6 * NQ - 1)):
                cs[c, at + k : at + k + 1, :] = line[place : place + 1]
            tile = ref[k * TW : (k + 1) * TW, :].reshape(NP, NQ, C)
            row = at + k
            slot = row if at == 0 else row - 20
            padded(gp, slot, tile, line[:NQ], line[TW - NQ :], cs[1, row : row + 1, :], cs[6, row : row + 1, :])
    for g, slot in ((0, 2), (1, 3), (TH - 2, 4), (TH - 1, 5)):
        tile = grid_ref[g]
        row = g + 2
        padded(
            gp,
            slot,
            tile,
            tile[0].astype(F32),
            tile[NP - 1].astype(F32),
            cs[1, row : row + 1, :],
            cs[6, row : row + 1, :],
        )

    def ring(rows, columns, a, b):
        parts = [rows[at + a : at + a + 2, b : b + NP].reshape(2 * TW, C) for at in (0, 4)]
        parts += [columns[c + b, a : a + 32, :].astype(BF) for c in (0, 1, 4, 5)]
        return jnp.concatenate(parts, axis=0)

    value = silu(nine(one_ref, functools.partial(ring, gp, cs)))
    line = iota((32, C), 0)
    for n, c in enumerate((0, 1, 6, 7)):
        column = value[4 * TW + 32 * n : 4 * TW + 32 * (n + 1)]
        column = jnp.where(line == 0, column * keep_top, column)
        hc[c, 0:32, :] = jnp.where(line == TH + 1, column * keep_bottom, column)
    for c in range(4):
        hc[2 + c, 0:32, :] = hcols_ref[c, 0:32, :]
    for c in range(8):
        hc[c, 32:40, :] = jnp.zeros((8, C), F32)
    for n, g in enumerate((0, 1, TH, TH + 1)):
        row = value[n * TW : (n + 1) * TW]
        if g == 0:
            row = row * keep_top
        if g == TH + 1:
            row = row * keep_bottom
        row = row.reshape(NP, NQ, C)
        for c, (p, q) in enumerate(((1, 0), (2, 0), (3, NQ - 1), (4, NQ - 1))):
            hc[2 + c, g : g + 1, :] = row[p, q : q + 1]
        slot = g if g < 4 else g - 18
        padded(
            hr, slot, row.astype(BF), row[0], row[NP - 1], hc[0, g : g + 1, :], hc[7, g : g + 1, :]
        )
    place = iota((NQ, C), 0)
    for g, slot in ((2, 2), (3, 3), (TH - 2, 4), (TH - 1, 5)):
        tile = hp_ref[g, 1 : NP + 1]
        first = jnp.where(place == 0, hc[1, g : g + 1, :], tile[0].astype(F32))
        last = jnp.where(place == NQ - 1, hc[6, g : g + 1, :], tile[NP - 1].astype(F32))
        padded(hr, slot, tile, first, last, hc[0, g : g + 1, :], hc[7, g : g + 1, :])
        hr[slot, 1] = first.astype(BF)
        hr[slot, NP] = last.astype(BF)

    value = nine(two_ref, functools.partial(ring, hr, hc))
    for n, i in enumerate((0, 1, TH - 2, TH - 1)):
        row = value[n * TW : (n + 1) * TW].reshape(NP, NQ, C) + grid_ref[i].astype(F32)
        spread_out(flat, n, row)
    copies = []
    for h in range(2):
        lines[:, :, 128 * h : 128 * (h + 1)] = flat[h].astype(BF).reshape(4, TW, 128)
    for n, i in enumerate((0, TH - 2)):
        copies.append(pltpu.make_async_copy(lines.at[2 * n : 2 * n + 2], out_ref.at[i : i + 2], sems.at[n]))
        copies[-1].start()
    for c in range(4):
        column = value[4 * TW + 32 * c : 4 * TW + 32 * c + TH]
        oc[c] = column + cs[2 + c, 2 : 2 + TH, :]
    place = iota((8, C), 0)
    for i in range(2, TH - 2):
        left, right = strips_ref[0, i - 2].astype(F32), strips_ref[1, i - 2].astype(F32)
        left = jnp.where(place == 0, oc[0, i : i + 1, :], jnp.where(place == 1, oc[1, i : i + 1, :], left))
        right = jnp.where(place == 6, oc[2, i : i + 1, :], jnp.where(place == 7, oc[3, i : i + 1, :], right))
        strips[0, i - 2] = left.astype(BF)
        strips[1, i - 2] = right.astype(BF)
    for n, at in enumerate((0, TW - 8)):
        copies.append(
            pltpu.make_async_copy(strips.at[n], out_ref.at[2 : TH - 2, at : at + 8], sems.at[2 + n])
        )
        copies[-1].start()
    for copy in copies:
        copy.wait()


def vmem(count):
    return [pl.BlockSpec(memory_space=pltpu.VMEM)] * count


def far(count):
    return [pl.BlockSpec(memory_space=pl.ANY)] * count


def smem():
    return pl.BlockSpec(memory_space=pltpu.SMEM)


LIMIT = 40 * 1024 * 1024


def in_hbm(value):
    return pltpu.with_memory_space_constraint(value, pltpu.HBM)


def near(value):
    return pltpu.with_memory_space_constraint(value, pltpu.VMEM)


def send_call(features, cell_index, tile_rows):
    here = lax.axis_index("lat") * lax.axis_size("lon") + lax.axis_index("lon")
    shift = lax.rem(here * ROWS, 128).reshape(1).astype(jnp.int32)
    return pl.pallas_call(
        send_kernel,
        out_shape=pltpu.VMEM((SOURCES, PAIRS, 2, F), BF),
        in_specs=[smem(), *far(2), *vmem(1)],
        out_specs=vmem(1)[0],
        scratch_shapes=[
            pltpu.VMEM((96, 128), jnp.int32),
            pltpu.VMEM((2 * SOURCES, 128), F32),
            pltpu.VMEM((SOURCES, 1, 2, F), BF),
            pltpu.VMEM((128, 128), F32),
            pltpu.SemaphoreType.DMA((6,)),
        ],
        compiler_params=pltpu.CompilerParams(vmem_limit_bytes=LIMIT),
        name="send",
    )(
        shift,
        in_hbm(features.reshape(SOURCES, PAIRS - 1, 2, F)),
        in_hbm(cell_index.reshape(96, 128)),
        near(tile_rows.reshape(1, 128)),
    )


def frame_call(received, spread, w_in, w_dens):
    return pl.pallas_call(
        frame_kernel,
        out_shape=(
            pltpu.VMEM((TH, NP, NQ, C), BF),
            pltpu.VMEM((2, TH, C), BF),
            pltpu.VMEM((2, TH, C), BF),
            pltpu.VMEM((EDGE, C), BF),
            pltpu.VMEM((EDGE, C), BF),
        ),
        in_specs=[*vmem(2), smem(), *vmem(2)],
        out_specs=tuple(vmem(5)),
        scratch_shapes=[
            pltpu.VMEM((SOURCES * 2, 128), F32),
            pltpu.VMEM((4, 104, 128), F32),
            pltpu.VMEM((LHS, C), F32),
            pltpu.VMEM((128, 32), F32),
            pltpu.VMEM((PH, NP + 2, NQ, F), F32),
            pltpu.VMEM((TH * TW, F), BF),
            pltpu.VMEM((4, TH, C), F32),
        ],
        compiler_params=pltpu.CompilerParams(vmem_limit_bytes=LIMIT),
        name="frame",
    )(near(received.reshape(SOURCES * ROWS, F)), near(received), spread, near(w_in), near(w_dens.reshape(1, C)))


def corner_call(top, bottom, west, east):
    return pl.pallas_call(
        corner_kernel,
        out_shape=(pltpu.VMEM((EDGE, C), BF),) * 2,
        in_specs=vmem(4),
        out_specs=tuple(vmem(2)),
        scratch_shapes=[pltpu.VMEM((8, C), F32)],
        input_output_aliases={0: 0, 1: 1},
        compiler_params=pltpu.CompilerParams(vmem_limit_bytes=LIMIT),
        name="corner",
    )(near(top), near(bottom), near(west), near(east))


def work(rows):
    return pl.CostEstimate(flops=2 * rows * TW * 9 * C * C, bytes_accessed=0, transcendentals=0)


def inner_one_call(grid, one):
    return pl.pallas_call(
        inner_one_kernel,
        out_shape=(pltpu.VMEM((TH + 2, NP + 2, NQ, C), BF), pltpu.VMEM((4, 40, C), F32)),
        in_specs=vmem(2),
        out_specs=tuple(vmem(2)),
        scratch_shapes=[pltpu.VMEM((TH, NP + 2, NQ, C), BF)],
        compiler_params=pltpu.CompilerParams(vmem_limit_bytes=LIMIT),
        cost_estimate=work(TH - 2),
        name="inner_one",
    )(near(grid), near(one))


def inner_two_call(hp, grid, two):
    return pl.pallas_call(
        inner_two_kernel,
        out_shape=(pltpu.HBM((TH, TW, C), BF), pltpu.VMEM((2, TH - 4, 8, C), BF)),
        in_specs=vmem(3),
        out_specs=(*far(1), *vmem(1)),
        scratch_shapes=[
            pltpu.VMEM((2, TH * TW, 128), F32),
            pltpu.VMEM((TH, TW, C), BF),
            pltpu.SemaphoreType.DMA((6,)),
        ],
        compiler_params=pltpu.CompilerParams(vmem_limit_bytes=LIMIT),
        cost_estimate=work(TH - 4),
        name="inner_two",
    )(near(hp), near(grid), near(two))


def ring_call(lat, grid, north, south, west, east, own_west, own_east, hp, hcols, strips, one, two, partial):
    inside = [grid, north, south, west, east, own_west, own_east, hp, hcols, strips, one, two]
    return pl.pallas_call(
        ring_kernel,
        out_shape=jax.ShapeDtypeStruct((TH, TW, C), BF),
        in_specs=[smem(), *vmem(12), *far(1)],
        out_specs=far(1)[0],
        scratch_shapes=[
            pltpu.VMEM((8, 40, C), F32),
            pltpu.VMEM((8, NP + 2, NQ, C), BF),
            pltpu.VMEM((8, 40, C), F32),
            pltpu.VMEM((8, NP + 2, NQ, C), BF),
            pltpu.VMEM((2, 4 * TW, 128), F32),
            pltpu.VMEM((4, TH, C), F32),
            pltpu.VMEM((4, TW, C), BF),
            pltpu.VMEM((2, TH - 4, 8, C), BF),
            pltpu.SemaphoreType.DMA((4,)),
        ],
        input_output_aliases={13: 0},
        compiler_params=pltpu.CompilerParams(vmem_limit_bytes=LIMIT),
        cost_estimate=work(8),
        name="ring",
    )(lat, *(near(value) for value in inside), partial)


def step(axis, by, around):
    count = lax.axis_size(axis)
    return [(i, (i + by) % count) for i in range(count) if around or 0 <= i + by < count]


def shards(features, cell_index, tile_rows, spread, w_in, w_dens, w_one, w_two):
    sent = send_call(features, cell_index, tile_rows)
    received = lax.all_to_all(sent, ("lat", "lon"), split_axis=0, concat_axis=0, tiled=True)
    grid, own_west, own_east, top, bottom = frame_call(received, spread, w_in, w_dens)
    one, two = w_one.reshape(9, C, C), w_two.reshape(9, C, C)
    from_west = lax.ppermute(own_east, "lon", step("lon", 1, True))
    from_east = lax.ppermute(own_west, "lon", step("lon", -1, True))
    hp, hcols = inner_one_call(grid, one)
    top, bottom = corner_call(top, bottom, from_west, from_east)
    from_north = lax.ppermute(bottom, "lat", step("lat", 1, False))
    from_south = lax.ppermute(top, "lat", step("lat", -1, False))
    partial, strips = inner_two_call(hp, grid, two)
    lat = lax.axis_index("lat").reshape(1).astype(jnp.int32)
    return ring_call(
        lat, grid, from_north, from_south, from_west, from_east, own_west, own_east, hp, hcols, strips, one, two, partial
    )


def solution(mesh):
    in_specs = (
        P(("lat", "lon"), None),
        P(("lat", "lon")),
        P(("lat", "lon")),
        P(),
        P(),
        P(),
        P(),
        P(),
    )
    out_specs = P("lat", "lon", None)
    return jax.shard_map(shards, mesh=mesh, in_specs=in_specs, out_specs=out_specs, check_vma=False)
```

```python
import functools

import jax
import jax.numpy as jnp
from jax import lax
from jax.experimental import pallas as pl
from jax.experimental.pallas import tpu as pltpu
from jax.sharding import PartitionSpec as P

TH = 24
TW = 96
F = 128
C = 256
CAP = 96
PH = 26
PW = 98
NP = 6
NQ = 16
HALF = PH // 2
SOURCES = 128
ROWS = CAP + 2
PAIRS = ROWS // 2
MAIN = HALF * TW
EDGE = 2 * TW + 8
LHS = MAIN + 32
GROUPS = 7
PER = ROWS // GROUPS
BF = jnp.bfloat16
F32 = jnp.float32


def dot(a, b):
    return jnp.dot(a, b, preferred_element_type=F32)


def iota(shape, dim):
    return lax.broadcasted_iota(jnp.int32, shape, dim)


def with_row(tile, shift, row, at):
    rolled = pltpu.roll(tile, shift, 0)
    return jnp.where(iota(tile.shape, 0) == at, row, rolled)


def send_kernel(shift_ref, features_ref, index_ref, used_ref, out_ref, cells, counts, flat, where, used, sems):
    fetch = pltpu.make_async_copy(index_ref, cells, sems.at[5])
    fetch.start()
    fetch_used = pltpu.make_async_copy(used_ref, counts, sems.at[6])
    fetch_used.start()
    cut = SOURCES // 4
    copies = [
        pltpu.make_async_copy(
            features_ref.at[cut * k : cut * (k + 1)],
            out_ref.at[cut * k : cut * (k + 1), 0 : PAIRS - 1],
            sems.at[k],
        )
        for k in range(4)
    ]
    for copy in copies:
        copy.start()
    fetch_used.wait()
    count = jnp.broadcast_to(counts[...].astype(F32), (128, 128))
    used[...] = jnp.transpose(count)
    fetch.wait()
    lines = [cells[pl.ds(v, 32, stride=3), :].astype(F32) for v in range(3)]
    lane = iota((32, 128), 1)
    blocks = [
        lines[0],
        jnp.where(lane < 32, pltpu.roll(lines[0], 32, 1), pltpu.roll(lines[1], 32, 1)),
        jnp.where(lane < 64, pltpu.roll(lines[1], 64, 1), pltpu.roll(lines[2], 64, 1)),
        pltpu.roll(lines[2], 96, 1),
    ]
    for j, cell in enumerate(blocks):
        r = jnp.floor((cell + 0.5) * (1.0 / PW))
        s = cell - r * PW
        q = jnp.floor((s - 0.5) * (1.0 / NP))
        pos = (s - 1.0 - q * NP) * NQ + q
        pos = jnp.where(s == 0.0, float(TW), jnp.where(s == PW - 1.0, TW + 1.0, pos))
        r = jnp.where(lane.astype(F32) < used[pl.ds(j, 32, stride=4), :], r, 63.0)
        flat[pl.ds(2 * j, 32, stride=8), :] = pltpu.roll(r, shift_ref[0], 1)
        flat[pl.ds(2 * j + 1, 32, stride=8), :] = pltpu.roll(pos, shift_ref[0], 1)
    for t in range(SOURCES):
        where[t, 0] = flat[2 * t : 2 * t + 2, :].astype(BF)
    last = pltpu.make_async_copy(where, out_ref.at[:, PAIRS - 1 : PAIRS], sems.at[4])
    last.start()
    for copy in copies:
        copy.wait()
    last.wait()


def frame_kernel(
    odd_ref,
    x_ref,
    where_ref,
    spread_ref,
    win_ref,
    wdens_ref,
    grid_ref,
    west_ref,
    east_ref,
    cols_a_ref,
    cols_b_ref,
    rows_a_ref,
    rows_b_ref,
    c32,
    lanes,
    acc,
    cnt,
    pads,
    mean,
    cols,
):
    for t in range(SOURCES):
        c32[2 * t : 2 * t + 2, :] = where_ref[t, PAIRS - 1].astype(F32)
    both = jnp.concatenate([c32[pl.ds(w, SOURCES, stride=2), :] for w in range(2)], axis=1).astype(BF)
    high = 104
    tile = iota((high, 128), 0).astype(F32) * 128.0
    first = jnp.floor((tile + 0.5) * (1.0 / ROWS))
    source = iota((high, 128), 1).astype(F32)
    picked = [dot(jnp.where(source == first + k, 1.0, 0.0).astype(BF), both) for k in range(3)]
    bound = (first + 1.0) * ROWS - tile

    def joined(side):
        parts = [part[:, 128 * side : 128 * (side + 1)] for part in picked]
        return jnp.where(source < bound, parts[0], jnp.where(source < bound + ROWS, parts[1], parts[2]))

    r, pos = joined(0), joined(1)
    low = jnp.where(r >= HALF, r - HALF, r)
    lanes[0] = r
    lanes[1] = low
    lanes[2] = pos
    lanes[3] = jnp.where(pos >= TW, low + HALF * (pos - TW), -1.0)
    upper = jnp.where(r >= HALF, 1.0, 0.0)
    upper = jnp.transpose(jnp.concatenate([upper, jnp.zeros((128 - high, 128), F32)], axis=0))

    for g in range(GROUPS):
        tiles = range(g * PER, (g + 1) * PER)
        width = PER * 128

        def row(which):
            pieces = [lanes[which, t : t + 1, :] for t in tiles]
            return jnp.broadcast_to(jnp.concatenate(pieces, axis=1), (16, width)).astype(BF)

        r16, low16, pos16, edge16 = (row(w) for w in range(4))
        one, zero = jnp.ones((), BF), jnp.zeros((), BF)
        ids = iota((16, width), 0).astype(F32).astype(BF)

        def hot(values, tile):
            return jnp.where(ids + jnp.asarray(16 * tile, BF) == values, one, zero)

        place = [hot(pos16, t) for t in range(8)]
        parts = []
        for k in range(HALF):
            at = jnp.where(low16 == jnp.asarray(k, BF), one, zero)
            parts += [b * at for b in place[:NP]]
        parts += [hot(edge16, 0), hot(edge16, 1)]
        left = jnp.concatenate(parts, axis=0)
        right = []
        for t in tiles:
            x = x_ref[128 * t : 128 * (t + 1), :]
            up = x * jnp.broadcast_to(upper[:, t : t + 1], (128, 128)).astype(BF)
            right.append(jnp.concatenate([x - up, up], axis=1))
        part = dot(left, jnp.concatenate(right, axis=0))
        some = lax.dot_general(
            jnp.concatenate([hot(r16, 0), hot(r16, 1)], axis=0),
            jnp.concatenate(place, axis=0),
            (((1,), (1,)), ((), ())),
            preferred_element_type=F32,
        )
        if g == 0:
            acc[...] = part
            cnt[...] = some
        else:
            acc[...] += part
            cnt[...] += some

    def tile(r, p):
        lanes_of = slice((r // HALF) * 128, (r // HALF) * 128 + 128)
        base = (r % HALF) * TW + NQ * (p - 1)
        return pads[r, p // NP] if p in (0, NP + 1) else acc[base : base + NQ, lanes_of]

    for r in range(PH):
        lanes_of = slice((r // HALF) * 128, (r // HALF) * 128 + 128)
        at = MAIN + r % HALF
        pads[r, 0] = with_row(tile(r, NP), 1, acc[at : at + 1, lanes_of], 0)
        pads[r, 1] = with_row(tile(r, 1), NQ - 1, acc[at + HALF : at + HALF + 1, lanes_of], NQ - 1)

    number = jnp.transpose(jnp.concatenate([cnt[...], jnp.zeros((96, 128), F32)], axis=0))
    number = [
        with_row(number[TW - NQ : TW], 1, number[TW : TW + 1], 0),
        *(number[NQ * p : NQ * (p + 1)] for p in range(NP)),
        with_row(number[:NQ], NQ - 1, number[TW + 1 : TW + 2], NQ - 1),
    ]
    density = None
    for a in range(3):
        line = [sum(spread_ref[a, b] * number[p + b] for b in range(3)) for p in range(NP)]
        line = jnp.concatenate(line, axis=0)[:, a : a + TH]
        density = line if density is None else density + line
    scale = 1.0 / (1.0 + density)
    log_density = jnp.log(1.0 + density)

    step = 4
    weights = [[spread_ref[a, b] for b in range(3)] for a in range(3)]

    def average(block):
        for i in range(block * step, (block + 1) * step):
            wide = jnp.broadcast_to(scale[:, i : i + 1], (TW, F))
            for p in range(NP):
                data = None
                for a in range(3):
                    for b in range(3):
                        term = weights[a][b] * tile(i + a, p + b)
                        data = term if data is None else data + term
                at = i * TW + p * NQ
                mean[at : at + NQ, :] = (data * wide[p * NQ : (p + 1) * NQ]).astype(BF)

    def project(block):
        return dot(mean[block * step * TW : (block + 1) * step * TW, :], win_ref[...])

    def finish(block, out):
        for k in range(step):
            i = block * step + k
            extra = jnp.broadcast_to(log_density[:, i : i + 1], (TW, C)) * wdens_ref[...]
            cell = (out[k * TW : (k + 1) * TW] + extra).astype(BF)
            grid_ref[i] = cell.reshape(NP, NQ, C)
            wide = cell.astype(F32)
            for c, at in enumerate((0, NQ, 5 * NQ - 1, 6 * NQ - 1)):
                cols[c, i : i + 1, :] = wide[at : at + 1]

    blocks = TH // step
    average(0)
    for n in range(blocks):
        out = project(n)
        if n + 1 < blocks:
            average(n + 1)
        finish(n, out)
    west_ref[...] = cols[0:2].astype(BF)
    east_ref[...] = cols[2:4].astype(BF)

    def give(odd, a_ref, b_ref, after, before):
        @pl.when(odd == 0)
        def _():
            a_ref[...] = after
            b_ref[...] = before

        @pl.when(odd != 0)
        def _():
            a_ref[...] = before
            b_ref[...] = after

    give(odd_ref[1], cols_a_ref, cols_b_ref, cols[2:4].astype(BF), cols[0:2].astype(BF))
    rows = [grid_ref[at : at + 2].reshape(2 * TW, C) for at in (TH - 2, 0)]
    give(odd_ref[0], rows_a_ref.at[: 2 * TW], rows_b_ref.at[: 2 * TW], *rows)


def silu(v):
    return v / (1.0 + jnp.exp(-v))


def corner_kernel(odd_ref, a_in, b_in, cols_a_ref, cols_b_ref, a_ref, b_ref, part):
    def write(lon_odd, lat_odd):
        west, east = (cols_a_ref, cols_b_ref) if lon_odd else (cols_b_ref, cols_a_ref)
        for ref, at in ((a_ref, 0 if lat_odd else TH - 2), (b_ref, TH - 2 if lat_odd else 0)):
            for c in range(4):
                column = (west if c < 2 else east)[c % 2].astype(F32)
                part[2 * c : 2 * c + 2, :] = column[at : at + 2]
            ref[2 * TW : EDGE, :] = part[...].astype(BF)

    for lat_odd in (0, 1):
        for lon_odd in (0, 1):
            pl.when((odd_ref[0] == lat_odd) & (odd_ref[1] == lon_odd))(functools.partial(write, lon_odd, lat_odd))


def nine(weight, window):
    total = None
    for a in range(3):
        for b in range(3):
            term = dot(window(a, b), weight[3 * a + b])
            total = term if total is None else total + term
    return total


def rows_of(src, weight, start, count):
    return nine(weight, lambda a, b: src[start + a : start + a + count, b : b + NP].reshape(count * TW, C))


def padded(dst, at, tiles, first, last, before, after):
    dst[at, 1 : NP + 1] = tiles
    dst[at, 0] = with_row(last, 1, before, 0).astype(BF)
    dst[at, NP + 1] = with_row(first, NQ - 1, after, NQ - 1).astype(BF)


def spread_out(flat, at, tiles):
    for p in range(NP):
        for h in range(2):
            flat[h, pl.ds(at * TW + p, NQ, stride=NP), :] = tiles[p, :, 128 * h : 128 * (h + 1)]


def inner_one_kernel(grid_ref, one_ref, hp_ref, hcols_ref, gp):
    for g in range(TH):
        tile = grid_ref[g]
        first, last = tile[0].astype(F32), tile[NP - 1].astype(F32)
        padded(gp, g, tile, first, last, first[:1], last[NQ - 1 :])
    start = 0
    for count in (4, 4, 4, 4, 4, 2):
        value = silu(rows_of(gp, one_ref, start, count))
        for k in range(count):
            g = start + k + 2
            row = value[k * TW : (k + 1) * TW].reshape(NP, NQ, C)
            padded(hp_ref, g, row.astype(BF), row[0], row[NP - 1], row[0, :1], row[NP - 1, NQ - 1 :])
            for c, (p, q) in enumerate(((1, 0), (2, 0), (3, NQ - 1), (4, NQ - 1))):
                hcols_ref[c, g : g + 1, :] = row[p, q : q + 1]
        start += count


def inner_two_kernel(hp_ref, grid_ref, two_ref, body_ref, flat):
    step = 4
    for i in range(2, TH - 2, step):
        value = rows_of(hp_ref, two_ref, i, step).reshape(step, NP, NQ, C)
        value = value + grid_ref[i : i + step].astype(F32)
        at = i - 2
        for k in range(step):
            spread_out(flat, at + k, value[k])
        for h in range(2):
            block = flat[h, at * TW : (at + step) * TW, :].astype(BF).reshape(step, TW, 128)
            body_ref[at : at + step, :, 128 * h : 128 * (h + 1)] = block


def ring_kernel(
    lat_ref,
    odd_ref,
    grid_ref,
    rows_a_ref,
    rows_b_ref,
    cols_a_ref,
    cols_b_ref,
    own_west_ref,
    own_east_ref,
    hp_ref,
    hcols_ref,
    body_ref,
    one_ref,
    two_ref,
    out_ref,
    north_ref,
    south_ref,
    west_ref,
    east_ref,
    cs,
    gp,
    hc,
    hr,
    flat,
    oc,
    lines,
    strips,
    sems,
):
    inside = pltpu.make_async_copy(
        body_ref.at[:, 8 : TW - 8], out_ref.at[2 : TH - 2, 8 : TW - 8], sems.at[4]
    )
    inside.start()
    lat = lat_ref[0]
    keep_top = jnp.where(lat > 0, 1.0, 0.0)
    keep_bottom = jnp.where(lat < 15, 1.0, 0.0)

    def take(odd, a_ref, b_ref, after_ref, before_ref):
        @pl.when(odd == 0)
        def _():
            after_ref[...] = a_ref[...]
            before_ref[...] = b_ref[...]

        @pl.when(odd != 0)
        def _():
            after_ref[...] = b_ref[...]
            before_ref[...] = a_ref[...]

    take(odd_ref[0], rows_a_ref, rows_b_ref, south_ref, north_ref)
    take(odd_ref[1], cols_a_ref, cols_b_ref, east_ref, west_ref)
    cs[:, 24:, :] = jnp.zeros((8, 16, C), F32)
    for n, ref in enumerate((west_ref, own_west_ref, own_east_ref, east_ref)):
        for c in range(2):
            cs[2 * n + c, 2 : 2 + TH, :] = ref[c].astype(F32)
    for ref, at in ((north_ref, 0), (south_ref, 2 + TH)):
        corner = ref[2 * TW : EDGE, :].astype(F32)
        for n, c in enumerate((0, 1, 6, 7)):
            cs[c, at : at + 2, :] = corner[2 * n : 2 * n + 2]
        for k in range(2):
            line = ref[k * TW : (k + 1) * TW, :].astype(F32)
            for c, place in ((2, 0), (3, NQ), (4, 5 * NQ - 1), (5, 6 * NQ - 1)):
                cs[c, at + k : at + k + 1, :] = line[place : place + 1]
            tile = ref[k * TW : (k + 1) * TW, :].reshape(NP, NQ, C)
            row = at + k
            slot = row if at == 0 else row - 20
            padded(gp, slot, tile, line[:NQ], line[TW - NQ :], cs[1, row : row + 1, :], cs[6, row : row + 1, :])
    for g, slot in ((0, 2), (1, 3), (TH - 2, 4), (TH - 1, 5)):
        tile = grid_ref[g]
        row = g + 2
        padded(
            gp,
            slot,
            tile,
            tile[0].astype(F32),
            tile[NP - 1].astype(F32),
            cs[1, row : row + 1, :],
            cs[6, row : row + 1, :],
        )

    def ring(rows, columns, a, b):
        parts = [rows[at + a : at + a + 2, b : b + NP].reshape(2 * TW, C) for at in (0, 4)]
        parts += [columns[c + b, a : a + 32, :].astype(BF) for c in (0, 1, 4, 5)]
        return jnp.concatenate(parts, axis=0)

    value = silu(nine(one_ref, functools.partial(ring, gp, cs)))
    line = iota((32, C), 0)
    for n, c in enumerate((0, 1, 6, 7)):
        column = value[4 * TW + 32 * n : 4 * TW + 32 * (n + 1)]
        column = jnp.where(line == 0, column * keep_top, column)
        hc[c, 0:32, :] = jnp.where(line == TH + 1, column * keep_bottom, column)
    for c in range(4):
        hc[2 + c, 0:32, :] = hcols_ref[c, 0:32, :]
    for c in range(8):
        hc[c, 32:40, :] = jnp.zeros((8, C), F32)
    for n, g in enumerate((0, 1, TH, TH + 1)):
        row = value[n * TW : (n + 1) * TW]
        if g == 0:
            row = row * keep_top
        if g == TH + 1:
            row = row * keep_bottom
        row = row.reshape(NP, NQ, C)
        for c, (p, q) in enumerate(((1, 0), (2, 0), (3, NQ - 1), (4, NQ - 1))):
            hc[2 + c, g : g + 1, :] = row[p, q : q + 1]
        slot = g if g < 4 else g - 18
        padded(
            hr, slot, row.astype(BF), row[0], row[NP - 1], hc[0, g : g + 1, :], hc[7, g : g + 1, :]
        )
    place = iota((NQ, C), 0)
    for g, slot in ((2, 2), (3, 3), (TH - 2, 4), (TH - 1, 5)):
        tile = hp_ref[g, 1 : NP + 1]
        first = jnp.where(place == 0, hc[1, g : g + 1, :], tile[0].astype(F32))
        last = jnp.where(place == NQ - 1, hc[6, g : g + 1, :], tile[NP - 1].astype(F32))
        padded(hr, slot, tile, first, last, hc[0, g : g + 1, :], hc[7, g : g + 1, :])
        hr[slot, 1] = first.astype(BF)
        hr[slot, NP] = last.astype(BF)

    value = nine(two_ref, functools.partial(ring, hr, hc))
    for n, i in enumerate((0, 1, TH - 2, TH - 1)):
        row = value[n * TW : (n + 1) * TW].reshape(NP, NQ, C) + grid_ref[i].astype(F32)
        spread_out(flat, n, row)
    copies = []
    for h in range(2):
        lines[:, :, 128 * h : 128 * (h + 1)] = flat[h].astype(BF).reshape(4, TW, 128)
    for n, i in enumerate((0, TH - 2)):
        copies.append(pltpu.make_async_copy(lines.at[2 * n : 2 * n + 2], out_ref.at[i : i + 2], sems.at[n]))
        copies[-1].start()
    for c in range(4):
        column = value[4 * TW + 32 * c : 4 * TW + 32 * c + TH]
        oc[c] = column + cs[2 + c, 2 : 2 + TH, :]
    place = iota((8, C), 0)
    for i in range(2, TH - 2):
        left, right = body_ref[i - 2, :8].astype(F32), body_ref[i - 2, TW - 8 :].astype(F32)
        left = jnp.where(place == 0, oc[0, i : i + 1, :], jnp.where(place == 1, oc[1, i : i + 1, :], left))
        right = jnp.where(place == 6, oc[2, i : i + 1, :], jnp.where(place == 7, oc[3, i : i + 1, :], right))
        strips[0, i - 2] = left.astype(BF)
        strips[1, i - 2] = right.astype(BF)
    for n, at in enumerate((0, TW - 8)):
        copies.append(
            pltpu.make_async_copy(strips.at[n], out_ref.at[2 : TH - 2, at : at + 8], sems.at[2 + n])
        )
        copies[-1].start()
    for copy in [*copies, inside]:
        copy.wait()


def vmem(count):
    return [pl.BlockSpec(memory_space=pltpu.VMEM)] * count


def far(count):
    return [pl.BlockSpec(memory_space=pl.ANY)] * count


def smem():
    return pl.BlockSpec(memory_space=pltpu.SMEM)


LIMIT = 40 * 1024 * 1024


def in_hbm(value):
    return pltpu.with_memory_space_constraint(value, pltpu.HBM)


def near(value):
    return pltpu.with_memory_space_constraint(value, pltpu.VMEM)


def send_call(features, cell_index, tile_rows):
    here = lax.axis_index("lat") * lax.axis_size("lon") + lax.axis_index("lon")
    shift = lax.rem(here * ROWS, 128).reshape(1).astype(jnp.int32)
    return pl.pallas_call(
        send_kernel,
        out_shape=pltpu.VMEM((SOURCES, PAIRS, 2, F), BF),
        in_specs=[smem(), *far(3)],
        out_specs=vmem(1)[0],
        scratch_shapes=[
            pltpu.VMEM((96, 128), jnp.int32),
            pltpu.VMEM((1, 128), jnp.int32),
            pltpu.VMEM((2 * SOURCES, 128), F32),
            pltpu.VMEM((SOURCES, 1, 2, F), BF),
            pltpu.VMEM((128, 128), F32),
            pltpu.SemaphoreType.DMA((7,)),
        ],
        compiler_params=pltpu.CompilerParams(vmem_limit_bytes=LIMIT),
        name="send",
    )(
        shift,
        in_hbm(features.reshape(SOURCES, PAIRS - 1, 2, F)),
        in_hbm(cell_index.reshape(96, 128)),
        in_hbm(tile_rows.reshape(1, 128)),
    )


def frame_call(odd, received, spread, w_in, w_dens):
    return pl.pallas_call(
        frame_kernel,
        out_shape=(
            pltpu.VMEM((TH, NP, NQ, C), BF),
            *(pltpu.VMEM((2, TH, C), BF),) * 4,
            *(pltpu.VMEM((EDGE, C), BF),) * 2,
        ),
        in_specs=[smem(), *vmem(2), smem(), *vmem(2)],
        out_specs=tuple(vmem(7)),
        scratch_shapes=[
            pltpu.VMEM((SOURCES * 2, 128), F32),
            pltpu.VMEM((4, 104, 128), F32),
            pltpu.VMEM((LHS, C), F32),
            pltpu.VMEM((32, 128), F32),
            pltpu.VMEM((PH, 2, NQ, F), F32),
            pltpu.VMEM((TH * TW, F), BF),
            pltpu.VMEM((4, TH, C), F32),
        ],
        compiler_params=pltpu.CompilerParams(vmem_limit_bytes=LIMIT),
        name="frame",
    )(odd, near(received.reshape(SOURCES * ROWS, F)), near(received), spread, near(w_in), near(w_dens.reshape(1, C)))


def corner_call(odd, rows_a, rows_b, cols_a, cols_b):
    return pl.pallas_call(
        corner_kernel,
        out_shape=(pltpu.VMEM((EDGE, C), BF),) * 2,
        in_specs=[smem(), *vmem(4)],
        out_specs=tuple(vmem(2)),
        scratch_shapes=[pltpu.VMEM((8, C), F32)],
        input_output_aliases={1: 0, 2: 1},
        compiler_params=pltpu.CompilerParams(vmem_limit_bytes=LIMIT),
        name="corner",
    )(odd, near(rows_a), near(rows_b), near(cols_a), near(cols_b))


def work(rows):
    return pl.CostEstimate(flops=2 * rows * TW * 9 * C * C, bytes_accessed=0, transcendentals=0)


def inner_one_call(grid, one):
    return pl.pallas_call(
        inner_one_kernel,
        out_shape=(pltpu.VMEM((TH + 2, NP + 2, NQ, C), BF), pltpu.VMEM((4, 40, C), F32)),
        in_specs=vmem(2),
        out_specs=tuple(vmem(2)),
        scratch_shapes=[pltpu.VMEM((TH, NP + 2, NQ, C), BF)],
        compiler_params=pltpu.CompilerParams(vmem_limit_bytes=LIMIT),
        cost_estimate=work(TH - 2),
        name="inner_one",
    )(near(grid), near(one))


def inner_two_call(hp, grid, two):
    return pl.pallas_call(
        inner_two_kernel,
        out_shape=pltpu.VMEM((TH - 4, TW, C), BF),
        in_specs=vmem(3),
        out_specs=vmem(1)[0],
        scratch_shapes=[pltpu.VMEM((2, (TH - 4) * TW, 128), F32)],
        compiler_params=pltpu.CompilerParams(vmem_limit_bytes=LIMIT),
        cost_estimate=work(TH - 4),
        name="inner_two",
    )(near(hp), near(grid), near(two))


def ring_call(lat, odd, *inside):
    return pl.pallas_call(
        ring_kernel,
        out_shape=jax.ShapeDtypeStruct((TH, TW, C), BF),
        in_specs=[smem(), smem(), *vmem(12)],
        out_specs=far(1)[0],
        scratch_shapes=[
            *(pltpu.VMEM((EDGE, C), BF),) * 2,
            *(pltpu.VMEM((2, TH, C), BF),) * 2,
            pltpu.VMEM((8, 40, C), F32),
            pltpu.VMEM((8, NP + 2, NQ, C), BF),
            pltpu.VMEM((8, 40, C), F32),
            pltpu.VMEM((8, NP + 2, NQ, C), BF),
            pltpu.VMEM((2, 4 * TW, 128), F32),
            pltpu.VMEM((4, TH, C), F32),
            pltpu.VMEM((4, TW, C), BF),
            pltpu.VMEM((2, TH - 4, 8, C), BF),
            pltpu.SemaphoreType.DMA((5,)),
        ],
        compiler_params=pltpu.CompilerParams(vmem_limit_bytes=LIMIT),
        cost_estimate=work(8),
        name="ring",
    )(lat, odd, *(near(value) for value in inside))


def swaps(axis, first, around):
    count = lax.axis_size(axis)
    pairs = [(i, (i + 1) % count) for i in range(first, count, 2) if around or i + 1 < count]
    return pairs + [(j, i) for i, j in pairs]


def shards(features, cell_index, tile_rows, spread, w_in, w_dens, w_one, w_two):
    sent = send_call(features, cell_index, tile_rows)
    received = lax.all_to_all(sent, ("lat", "lon"), split_axis=0, concat_axis=0, tiled=True)
    lat = lax.axis_index("lat").astype(jnp.int32)
    odd = jnp.stack([lat % 2, lax.axis_index("lon").astype(jnp.int32) % 2])
    grid, own_west, own_east, cols_a, cols_b, rows_a, rows_b = frame_call(odd, received, spread, w_in, w_dens)
    one, two = w_one.reshape(9, C, C), w_two.reshape(9, C, C)
    cols_b = lax.ppermute(cols_b, "lon", swaps("lon", 1, True))
    cols_a = lax.ppermute(cols_a, "lon", swaps("lon", 0, True))
    hp, hcols = inner_one_call(grid, one)
    rows_a, rows_b = corner_call(odd, rows_a, rows_b, cols_a, cols_b)
    rows_b = lax.ppermute(rows_b, "lat", swaps("lat", 1, False))
    rows_a = lax.ppermute(rows_a, "lat", swaps("lat", 0, False))
    body = inner_two_call(hp, grid, two)
    return ring_call(
        lat.reshape(1), odd, grid, rows_a, rows_b, cols_a, cols_b, own_west, own_east, hp, hcols, body, one, two
    )


def solution(mesh):
    in_specs = (
        P(("lat", "lon"), None),
        P(("lat", "lon")),
        P(("lat", "lon")),
        P(),
        P(),
        P(),
        P(),
        P(),
    )
    out_specs = P("lat", "lon", None)
    return jax.shard_map(shards, mesh=mesh, in_specs=in_specs, out_specs=out_specs, check_vma=False)
```

```python
import functools

import jax
import jax.numpy as jnp
from jax import lax
from jax.experimental import pallas as pl
from jax.experimental.pallas import tpu as pltpu
from jax.sharding import PartitionSpec as P


TH = 24
TW = 96
F = 128
C = 256
CAP = 96
PH = 26
PW = 98
NP = 6
NQ = 16
HALF = PH // 2
SOURCES = 128
ROWS = CAP + 2
PAIRS = ROWS // 2
MAIN = HALF * TW
EDGE = 2 * TW + 8
LHS = MAIN + 32
GROUPS = 7
PER = ROWS // GROUPS
BF = jnp.bfloat16
F32 = jnp.float32


def dot(a, b):
    return jnp.dot(a, b, preferred_element_type=F32)


def iota(shape, dim):
    return lax.broadcasted_iota(jnp.int32, shape, dim)


def places():
    return lax.axis_index("lat").astype(jnp.int32), lax.axis_index("lon").astype(jnp.int32)


def parities():
    lat, lon = places()
    return lax.rem(lat, 2), lax.rem(lon, 2)


def with_row(tile, shift, row, at):
    rolled = pltpu.roll(tile, shift, 0)
    return jnp.where(iota(tile.shape, 0) == at, row, rolled)


def send_kernel(features_ref, index_ref, used_ref, out_ref, cells, counts, flat, where, used, sems):
    fetch = pltpu.make_async_copy(index_ref, cells, sems.at[5])
    fetch.start()
    fetch_used = pltpu.make_async_copy(used_ref, counts, sems.at[6])
    fetch_used.start()
    cut = SOURCES // 4
    copies = [
        pltpu.make_async_copy(
            features_ref.at[cut * k : cut * (k + 1)],
            out_ref.at[cut * k : cut * (k + 1), 0 : PAIRS - 1],
            sems.at[k],
        )
        for k in range(4)
    ]
    for copy in copies:
        copy.start()
    fetch_used.wait()
    count = jnp.broadcast_to(counts[...].astype(F32), (128, 128))
    used[...] = jnp.transpose(count)
    fetch.wait()
    lines = [cells[pl.ds(v, 32, stride=3), :].astype(F32) for v in range(3)]
    lat, lon = places()
    shift = lax.rem((lat * 8 + lon) * ROWS, 128)
    lane = iota((32, 128), 1)
    blocks = [
        lines[0],
        jnp.where(lane < 32, pltpu.roll(lines[0], 32, 1), pltpu.roll(lines[1], 32, 1)),
        jnp.where(lane < 64, pltpu.roll(lines[1], 64, 1), pltpu.roll(lines[2], 64, 1)),
        pltpu.roll(lines[2], 96, 1),
    ]
    for j, cell in enumerate(blocks):
        r = jnp.floor((cell + 0.5) * (1.0 / PW))
        s = cell - r * PW
        q = jnp.floor((s - 0.5) * (1.0 / NP))
        pos = (s - 1.0 - q * NP) * NQ + q
        pos = jnp.where(s == 0.0, float(TW), jnp.where(s == PW - 1.0, TW + 1.0, pos))
        r = jnp.where(lane.astype(F32) < used[pl.ds(j, 32, stride=4), :], r, 63.0)
        flat[pl.ds(2 * j, 32, stride=8), :] = pltpu.roll(r, shift, 1)
        flat[pl.ds(2 * j + 1, 32, stride=8), :] = pltpu.roll(pos, shift, 1)
    for t in range(SOURCES):
        where[t, 0] = flat[2 * t : 2 * t + 2, :].astype(BF)
    last = pltpu.make_async_copy(where, out_ref.at[:, PAIRS - 1 : PAIRS], sems.at[4])
    last.start()
    for copy in copies:
        copy.wait()
    last.wait()


def frame_kernel(
    x_ref,
    where_ref,
    spread_ref,
    win_ref,
    wdens_ref,
    grid_ref,
    west_ref,
    east_ref,
    cols_a_ref,
    cols_b_ref,
    rows_a_ref,
    rows_b_ref,
    c32,
    lanes,
    acc,
    cnt,
    pads,
    mean,
    cols,
):
    for t in range(SOURCES):
        c32[2 * t : 2 * t + 2, :] = where_ref[t, PAIRS - 1].astype(F32)
    both = jnp.concatenate([c32[pl.ds(w, SOURCES, stride=2), :] for w in range(2)], axis=1).astype(BF)
    high = 104
    tile = iota((high, 128), 0).astype(F32) * 128.0
    first = jnp.floor((tile + 0.5) * (1.0 / ROWS))
    source = iota((high, 128), 1).astype(F32)
    picked = [dot(jnp.where(source == first + k, 1.0, 0.0).astype(BF), both) for k in range(3)]
    bound = (first + 1.0) * ROWS - tile

    def joined(side):
        parts = [part[:, 128 * side : 128 * (side + 1)] for part in picked]
        return jnp.where(source < bound, parts[0], jnp.where(source < bound + ROWS, parts[1], parts[2]))

    r, pos = joined(0), joined(1)
    low = jnp.where(r >= HALF, r - HALF, r)
    lanes[0] = r
    lanes[1] = low
    lanes[2] = pos
    lanes[3] = jnp.where(pos >= TW, low + HALF * (pos - TW), -1.0)
    upper = jnp.where(r >= HALF, 1.0, 0.0)
    upper = jnp.transpose(jnp.concatenate([upper, jnp.zeros((128 - high, 128), F32)], axis=0))

    for g in range(GROUPS):
        tiles = range(g * PER, (g + 1) * PER)
        width = PER * 128

        def row(which):
            pieces = [lanes[which, t : t + 1, :] for t in tiles]
            return jnp.broadcast_to(jnp.concatenate(pieces, axis=1), (16, width)).astype(BF)

        r16, low16, pos16, edge16 = (row(w) for w in range(4))
        one, zero = jnp.ones((), BF), jnp.zeros((), BF)
        ids = iota((16, width), 0).astype(F32).astype(BF)

        def hot(values, tile):
            return jnp.where(ids + jnp.asarray(16 * tile, BF) == values, one, zero)

        place = [hot(pos16, t) for t in range(8)]
        parts = []
        for k in range(HALF):
            at = jnp.where(low16 == jnp.asarray(k, BF), one, zero)
            parts += [b * at for b in place[:NP]]
        parts += [hot(edge16, 0), hot(edge16, 1)]
        left = jnp.concatenate(parts, axis=0)
        right = []
        for t in tiles:
            x = x_ref[128 * t : 128 * (t + 1), :]
            up = x * jnp.broadcast_to(upper[:, t : t + 1], (128, 128)).astype(BF)
            right.append(jnp.concatenate([x - up, up], axis=1))
        right = jnp.concatenate(right, axis=0)
        some = lax.dot_general(
            jnp.concatenate([hot(r16, 0), hot(r16, 1)], axis=0),
            jnp.concatenate(place, axis=0),
            (((1,), (1,)), ((), ())),
            preferred_element_type=F32,
        )
        if g == 0:
            acc[...] = dot(left, right)
            cnt[...] = some
        elif g + 1 < GROUPS:
            acc[...] += dot(left, right)
            cnt[...] += some
        else:
            cnt[...] += some

    def weight(a, b, shape):
        return jnp.broadcast_to(spread_ref[a : a + 1, b : b + 1], shape)

    def tile(r, p):
        lanes_of = slice((r // HALF) * 128, (r // HALF) * 128 + 128)
        base = (r % HALF) * TW + NQ * (p - 1)
        return pads[r, p // NP] if p in (0, NP + 1) else acc[base : base + NQ, lanes_of]

    def complete(start, stop):
        rows = slice(start * TW, stop * TW)
        acc[rows, :] += dot(left[rows], right)
        for r in (*range(start, stop), *range(HALF + start, HALF + stop)):
            lanes_of = slice((r // HALF) * 128, (r // HALF) * 128 + 128)
            at = MAIN + r % HALF
            pads[r, 0] = with_row(tile(r, NP), 1, acc[at : at + 1, lanes_of], 0)
            pads[r, 1] = with_row(tile(r, 1), NQ - 1, acc[at + HALF : at + HALF + 1, lanes_of], NQ - 1)

    acc[MAIN:, :] += dot(left[MAIN:], right)

    number = jnp.transpose(jnp.concatenate([cnt[...], jnp.zeros((96, 128), F32)], axis=0))
    number = [
        with_row(number[TW - NQ : TW], 1, number[TW : TW + 1], 0),
        *(number[NQ * p : NQ * (p + 1)] for p in range(NP)),
        with_row(number[:NQ], NQ - 1, number[TW + 1 : TW + 2], NQ - 1),
    ]
    density = None
    for a in range(3):
        line = [sum(weight(a, b, (NQ, 128)) * number[p + b] for b in range(3)) for p in range(NP)]
        line = jnp.concatenate(line, axis=0)[:, a : a + TH]
        density = line if density is None else density + line
    scale = 1.0 / (1.0 + density)
    log_density = jnp.log(1.0 + density)

    weights = [[weight(a, b, (NQ, F)) for b in range(3)] for a in range(3)]

    def average(rows):
        for i in rows:
            wide = jnp.broadcast_to(scale[:, i : i + 1], (TW, F))
            for p in range(NP):
                data = None
                for a in range(3):
                    for b in range(3):
                        term = weights[a][b] * tile(i + a, p + b)
                        data = term if data is None else data + term
                at = i * TW + p * NQ
                mean[at : at + NQ, :] = (data * wide[p * NQ : (p + 1) * NQ]).astype(BF)

    def project(rows):
        return dot(jnp.concatenate([mean[i * TW : (i + 1) * TW, :] for i in rows], axis=0), win_ref[...])

    def finish(rows, out):
        for k, i in enumerate(rows):
            extra = jnp.broadcast_to(log_density[:, i : i + 1], (TW, C)) * wdens_ref[...]
            cell = (out[k * TW : (k + 1) * TW] + extra).astype(BF)
            grid_ref[i] = cell.reshape(NP, NQ, C)
            wide = cell.astype(F32)
            for c, at in enumerate((0, NQ, 5 * NQ - 1, 6 * NQ - 1)):
                cols[c, i : i + 1, :] = wide[at : at + 1]

    plan = (
        (0, 5, ((0, 1, 2), (13, 14, 15))),
        (5, 9, ((3, 4, 5, 6), (16, 17, 18, 19))),
        (9, 13, ((7, 8, 9, 10), (20, 21, 22, 23), (11, 12))),
    )
    waiting = None
    for start, stop, sets in plan:
        complete(start, stop)
        for rows in sets:
            average(rows)
            out = project(rows)
            if waiting is not None:
                finish(*waiting)
            waiting = (rows, out)
    finish(*waiting)
    west_ref[...] = cols[0:2].astype(BF)
    east_ref[...] = cols[2:4].astype(BF)

    lat_odd, lon_odd = parities()

    def give(odd, a_ref, b_ref, after, before):
        @pl.when(odd == 0)
        def _():
            a_ref[...] = after
            b_ref[...] = before

        @pl.when(odd != 0)
        def _():
            a_ref[...] = before
            b_ref[...] = after

    give(lon_odd, cols_a_ref, cols_b_ref, cols[2:4].astype(BF), cols[0:2].astype(BF))
    rows = [grid_ref[at : at + 2].reshape(2 * TW, C) for at in (TH - 2, 0)]
    give(lat_odd, rows_a_ref.at[: 2 * TW], rows_b_ref.at[: 2 * TW], *rows)


def silu(v):
    return v / (1.0 + jnp.exp(-v))


def corner_kernel(a_in, b_in, cols_a_ref, cols_b_ref, a_ref, b_ref, part):
    def write(lon_odd, lat_odd):
        west, east = (cols_a_ref, cols_b_ref) if lon_odd else (cols_b_ref, cols_a_ref)
        for ref, at in ((a_ref, 0 if lat_odd else TH - 2), (b_ref, TH - 2 if lat_odd else 0)):
            for c in range(4):
                column = (west if c < 2 else east)[c % 2].astype(F32)
                part[2 * c : 2 * c + 2, :] = column[at : at + 2]
            ref[2 * TW : EDGE, :] = part[...].astype(BF)

    own = parities()
    for lat_odd in (0, 1):
        for lon_odd in (0, 1):
            pl.when((own[0] == lat_odd) & (own[1] == lon_odd))(functools.partial(write, lon_odd, lat_odd))


def nine(weight, window):
    total = None
    for a in range(3):
        for b in range(3):
            term = dot(window(a, b), weight[3 * a + b])
            total = term if total is None else total + term
    return total


def rows_of(src, weight, start, count):
    return nine(weight, lambda a, b: src[start + a : start + a + count, b : b + NP].reshape(count * TW, C))


def padded(dst, at, tiles, first, last, before, after):
    dst[at, 1 : NP + 1] = tiles
    dst[at, 0] = with_row(last, 1, before, 0).astype(BF)
    dst[at, NP + 1] = with_row(first, NQ - 1, after, NQ - 1).astype(BF)


def spread_out(flat, at, tiles):
    for p in range(NP):
        for h in range(2):
            flat[h, pl.ds(at * TW + p, NQ, stride=NP), :] = tiles[p, :, 128 * h : 128 * (h + 1)]


def inner_one_kernel(grid_ref, one_ref, hp_ref, hcols_ref, gp):
    for g in range(TH):
        tile = grid_ref[g]
        first, last = tile[0].astype(F32), tile[NP - 1].astype(F32)
        padded(gp, g, tile, first, last, first[:1], last[NQ - 1 :])
    start = 0
    for count in (4, 4, 4, 4, 4, 2):
        value = silu(rows_of(gp, one_ref, start, count))
        for k in range(count):
            g = start + k + 2
            row = value[k * TW : (k + 1) * TW].reshape(NP, NQ, C)
            padded(hp_ref, g, row.astype(BF), row[0], row[NP - 1], row[0, :1], row[NP - 1, NQ - 1 :])
            for c, (p, q) in enumerate(((1, 0), (2, 0), (3, NQ - 1), (4, NQ - 1))):
                hcols_ref[c, g : g + 1, :] = row[p, q : q + 1]
        start += count


def inner_two_kernel(hp_ref, grid_ref, two_ref, body_ref, flat):
    step = 4
    for i in range(2, TH - 2, step):
        value = rows_of(hp_ref, two_ref, i, step).reshape(step, NP, NQ, C)
        value = value + grid_ref[i : i + step].astype(F32)
        at = i - 2
        for k in range(step):
            spread_out(flat, at + k, value[k])
        for h in range(2):
            block = flat[h, at * TW : (at + step) * TW, :].astype(BF).reshape(step, TW, 128)
            body_ref[at : at + step, :, 128 * h : 128 * (h + 1)] = block


def ring_kernel(
    grid_ref,
    rows_a_ref,
    rows_b_ref,
    cols_a_ref,
    cols_b_ref,
    own_west_ref,
    own_east_ref,
    hp_ref,
    hcols_ref,
    body_ref,
    one_ref,
    two_ref,
    out_ref,
    north_ref,
    south_ref,
    west_ref,
    east_ref,
    cs,
    gp,
    hc,
    hr,
    flat,
    oc,
    lines,
    strips,
    sems,
):
    inside = pltpu.make_async_copy(
        body_ref.at[:, 8 : TW - 8], out_ref.at[2 : TH - 2, 8 : TW - 8], sems.at[4]
    )
    inside.start()
    lat, _ = places()
    lat_odd, lon_odd = parities()
    keep_top = jnp.where(lat > 0, 1.0, 0.0)
    keep_bottom = jnp.where(lat < 15, 1.0, 0.0)

    def take(odd, a_ref, b_ref, after_ref, before_ref):
        @pl.when(odd == 0)
        def _():
            after_ref[...] = a_ref[...]
            before_ref[...] = b_ref[...]

        @pl.when(odd != 0)
        def _():
            after_ref[...] = b_ref[...]
            before_ref[...] = a_ref[...]

    take(lat_odd, rows_a_ref, rows_b_ref, south_ref, north_ref)
    take(lon_odd, cols_a_ref, cols_b_ref, east_ref, west_ref)
    cs[:, 24:, :] = jnp.zeros((8, 16, C), F32)
    for n, ref in enumerate((west_ref, own_west_ref, own_east_ref, east_ref)):
        for c in range(2):
            cs[2 * n + c, 2 : 2 + TH, :] = ref[c].astype(F32)
    for ref, at in ((north_ref, 0), (south_ref, 2 + TH)):
        corner = ref[2 * TW : EDGE, :].astype(F32)
        for n, c in enumerate((0, 1, 6, 7)):
            cs[c, at : at + 2, :] = corner[2 * n : 2 * n + 2]
        for k in range(2):
            line = ref[k * TW : (k + 1) * TW, :].astype(F32)
            for c, place in ((2, 0), (3, NQ), (4, 5 * NQ - 1), (5, 6 * NQ - 1)):
                cs[c, at + k : at + k + 1, :] = line[place : place + 1]
            tile = ref[k * TW : (k + 1) * TW, :].reshape(NP, NQ, C)
            row = at + k
            slot = row if at == 0 else row - 20
            padded(gp, slot, tile, line[:NQ], line[TW - NQ :], cs[1, row : row + 1, :], cs[6, row : row + 1, :])
    for g, slot in ((0, 2), (1, 3), (TH - 2, 4), (TH - 1, 5)):
        tile = grid_ref[g]
        row = g + 2
        padded(
            gp,
            slot,
            tile,
            tile[0].astype(F32),
            tile[NP - 1].astype(F32),
            cs[1, row : row + 1, :],
            cs[6, row : row + 1, :],
        )

    def ring(rows, columns, a, b):
        parts = [rows[at + a : at + a + 2, b : b + NP].reshape(2 * TW, C) for at in (0, 4)]
        parts += [columns[c + b, a : a + 32, :].astype(BF) for c in (0, 1, 4, 5)]
        return jnp.concatenate(parts, axis=0)

    value = silu(nine(one_ref, functools.partial(ring, gp, cs)))
    line = iota((32, C), 0)
    for n, c in enumerate((0, 1, 6, 7)):
        column = value[4 * TW + 32 * n : 4 * TW + 32 * (n + 1)]
        column = jnp.where(line == 0, column * keep_top, column)
        hc[c, 0:32, :] = jnp.where(line == TH + 1, column * keep_bottom, column)
    for c in range(4):
        hc[2 + c, 0:32, :] = hcols_ref[c, 0:32, :]
    for c in range(8):
        hc[c, 32:40, :] = jnp.zeros((8, C), F32)
    for n, g in enumerate((0, 1, TH, TH + 1)):
        row = value[n * TW : (n + 1) * TW]
        if g == 0:
            row = row * keep_top
        if g == TH + 1:
            row = row * keep_bottom
        row = row.reshape(NP, NQ, C)
        for c, (p, q) in enumerate(((1, 0), (2, 0), (3, NQ - 1), (4, NQ - 1))):
            hc[2 + c, g : g + 1, :] = row[p, q : q + 1]
        slot = g if g < 4 else g - 18
        padded(
            hr, slot, row.astype(BF), row[0], row[NP - 1], hc[0, g : g + 1, :], hc[7, g : g + 1, :]
        )
    place = iota((NQ, C), 0)
    for g, slot in ((2, 2), (3, 3), (TH - 2, 4), (TH - 1, 5)):
        tile = hp_ref[g, 1 : NP + 1]
        first = jnp.where(place == 0, hc[1, g : g + 1, :], tile[0].astype(F32))
        last = jnp.where(place == NQ - 1, hc[6, g : g + 1, :], tile[NP - 1].astype(F32))
        padded(hr, slot, tile, first, last, hc[0, g : g + 1, :], hc[7, g : g + 1, :])
        hr[slot, 1] = first.astype(BF)
        hr[slot, NP] = last.astype(BF)

    value = nine(two_ref, functools.partial(ring, hr, hc))
    for n, i in enumerate((0, 1, TH - 2, TH - 1)):
        row = value[n * TW : (n + 1) * TW].reshape(NP, NQ, C) + grid_ref[i].astype(F32)
        spread_out(flat, n, row)
    copies = []
    for h in range(2):
        lines[:, :, 128 * h : 128 * (h + 1)] = flat[h].astype(BF).reshape(4, TW, 128)
    for n, i in enumerate((0, TH - 2)):
        copies.append(pltpu.make_async_copy(lines.at[2 * n : 2 * n + 2], out_ref.at[i : i + 2], sems.at[n]))
        copies[-1].start()
    for c in range(4):
        column = value[4 * TW + 32 * c : 4 * TW + 32 * c + TH]
        oc[c] = column + cs[2 + c, 2 : 2 + TH, :]
    place = iota((8, C), 0)
    for i in range(2, TH - 2):
        left, right = body_ref[i - 2, :8].astype(F32), body_ref[i - 2, TW - 8 :].astype(F32)
        left = jnp.where(place == 0, oc[0, i : i + 1, :], jnp.where(place == 1, oc[1, i : i + 1, :], left))
        right = jnp.where(place == 6, oc[2, i : i + 1, :], jnp.where(place == 7, oc[3, i : i + 1, :], right))
        strips[0, i - 2] = left.astype(BF)
        strips[1, i - 2] = right.astype(BF)
    for n, at in enumerate((0, TW - 8)):
        copies.append(
            pltpu.make_async_copy(strips.at[n], out_ref.at[2 : TH - 2, at : at + 8], sems.at[2 + n])
        )
        copies[-1].start()
    for copy in [*copies, inside]:
        copy.wait()


def vmem(count):
    return [pl.BlockSpec(memory_space=pltpu.VMEM)] * count


def far(count):
    return [pl.BlockSpec(memory_space=pl.ANY)] * count


LIMIT = 40 * 1024 * 1024


def in_hbm(value):
    return pltpu.with_memory_space_constraint(value, pltpu.HBM)


def near(value):
    return pltpu.with_memory_space_constraint(value, pltpu.VMEM)


def send_call(features, cell_index, tile_rows):
    return pl.pallas_call(
        send_kernel,
        out_shape=pltpu.VMEM((SOURCES, PAIRS, 2, F), BF),
        in_specs=far(3),
        out_specs=vmem(1)[0],
        scratch_shapes=[
            pltpu.VMEM((96, 128), jnp.int32),
            pltpu.VMEM((1, 128), jnp.int32),
            pltpu.VMEM((2 * SOURCES, 128), F32),
            pltpu.VMEM((SOURCES, 1, 2, F), BF),
            pltpu.VMEM((128, 128), F32),
            pltpu.SemaphoreType.DMA((7,)),
        ],
        compiler_params=pltpu.CompilerParams(vmem_limit_bytes=LIMIT),
        name="send",
    )(
        in_hbm(features.reshape(SOURCES, PAIRS - 1, 2, F)),
        in_hbm(cell_index.reshape(96, 128)),
        in_hbm(tile_rows.reshape(1, 128)),
    )


def frame_call(received, spread, w_in, w_dens):
    return pl.pallas_call(
        frame_kernel,
        out_shape=(
            pltpu.VMEM((TH, NP, NQ, C), BF),
            *(pltpu.VMEM((2, TH, C), BF),) * 4,
            *(pltpu.VMEM((EDGE, C), BF),) * 2,
        ),
        in_specs=vmem(5),
        out_specs=tuple(vmem(7)),
        scratch_shapes=[
            pltpu.VMEM((SOURCES * 2, 128), F32),
            pltpu.VMEM((4, 104, 128), F32),
            pltpu.VMEM((LHS, C), F32),
            pltpu.VMEM((32, 128), F32),
            pltpu.VMEM((PH, 2, NQ, F), F32),
            pltpu.VMEM((TH * TW, F), BF),
            pltpu.VMEM((4, TH, C), F32),
        ],
        compiler_params=pltpu.CompilerParams(vmem_limit_bytes=LIMIT),
        name="frame",
    )(near(received.reshape(SOURCES * ROWS, F)), near(received), near(spread), near(w_in), near(w_dens.reshape(1, C)))


def corner_call(rows_a, rows_b, cols_a, cols_b):
    return pl.pallas_call(
        corner_kernel,
        out_shape=(pltpu.VMEM((EDGE, C), BF),) * 2,
        in_specs=vmem(4),
        out_specs=tuple(vmem(2)),
        scratch_shapes=[pltpu.VMEM((8, C), F32)],
        input_output_aliases={0: 0, 1: 1},
        compiler_params=pltpu.CompilerParams(vmem_limit_bytes=LIMIT),
        name="corner",
    )(near(rows_a), near(rows_b), near(cols_a), near(cols_b))


def work(rows):
    return pl.CostEstimate(flops=2 * rows * TW * 9 * C * C, bytes_accessed=0, transcendentals=0)


def inner_one_call(grid, one):
    return pl.pallas_call(
        inner_one_kernel,
        out_shape=(pltpu.VMEM((TH + 2, NP + 2, NQ, C), BF), pltpu.VMEM((4, 40, C), F32)),
        in_specs=vmem(2),
        out_specs=tuple(vmem(2)),
        scratch_shapes=[pltpu.VMEM((TH, NP + 2, NQ, C), BF)],
        compiler_params=pltpu.CompilerParams(vmem_limit_bytes=LIMIT),
        cost_estimate=work(TH - 2),
        name="inner_one",
    )(near(grid), near(one))


def inner_two_call(hp, grid, two):
    return pl.pallas_call(
        inner_two_kernel,
        out_shape=pltpu.VMEM((TH - 4, TW, C), BF),
        in_specs=vmem(3),
        out_specs=vmem(1)[0],
        scratch_shapes=[pltpu.VMEM((2, (TH - 4) * TW, 128), F32)],
        compiler_params=pltpu.CompilerParams(vmem_limit_bytes=LIMIT),
        cost_estimate=work(TH - 4),
        name="inner_two",
    )(near(hp), near(grid), near(two))


def ring_call(*inside):
    return pl.pallas_call(
        ring_kernel,
        out_shape=jax.ShapeDtypeStruct((TH, TW, C), BF),
        in_specs=vmem(12),
        out_specs=far(1)[0],
        scratch_shapes=[
            *(pltpu.VMEM((EDGE, C), BF),) * 2,
            *(pltpu.VMEM((2, TH, C), BF),) * 2,
            pltpu.VMEM((8, 40, C), F32),
            pltpu.VMEM((8, NP + 2, NQ, C), BF),
            pltpu.VMEM((8, 40, C), F32),
            pltpu.VMEM((8, NP + 2, NQ, C), BF),
            pltpu.VMEM((2, 4 * TW, 128), F32),
            pltpu.VMEM((4, TH, C), F32),
            pltpu.VMEM((4, TW, C), BF),
            pltpu.VMEM((2, TH - 4, 8, C), BF),
            pltpu.SemaphoreType.DMA((5,)),
        ],
        compiler_params=pltpu.CompilerParams(vmem_limit_bytes=LIMIT),
        cost_estimate=work(8),
        name="ring",
    )(*(near(value) for value in inside))


def swaps(axis, first, around):
    count = lax.axis_size(axis)
    pairs = [(i, (i + 1) % count) for i in range(first, count, 2) if around or i + 1 < count]
    return pairs + [(j, i) for i, j in pairs]


def shards(features, cell_index, tile_rows, spread, w_in, w_dens, w_one, w_two):
    sent = send_call(features, cell_index, tile_rows)
    received = lax.all_to_all(sent, ("lat", "lon"), split_axis=0, concat_axis=0, tiled=True)
    grid, own_west, own_east, cols_a, cols_b, rows_a, rows_b = frame_call(received, spread, w_in, w_dens)
    one, two = w_one.reshape(9, C, C), w_two.reshape(9, C, C)
    cols_b = lax.ppermute(cols_b, "lon", swaps("lon", 1, True))
    cols_a = lax.ppermute(cols_a, "lon", swaps("lon", 0, True))
    hp, hcols = inner_one_call(grid, one)
    rows_a, rows_b = corner_call(rows_a, rows_b, cols_a, cols_b)
    rows_b = lax.ppermute(rows_b, "lat", swaps("lat", 1, False))
    rows_a = lax.ppermute(rows_a, "lat", swaps("lat", 0, False))
    body = inner_two_call(hp, grid, two)
    return ring_call(grid, rows_a, rows_b, cols_a, cols_b, own_west, own_east, hp, hcols, body, one, two)


def solution(mesh):
    in_specs = (
        P(("lat", "lon"), None),
        P(("lat", "lon")),
        P(("lat", "lon")),
        P(),
        P(),
        P(),
        P(),
        P(),
    )
    out_specs = P("lat", "lon", None)
    return jax.shard_map(shards, mesh=mesh, in_specs=in_specs, out_specs=out_specs, check_vma=False)
```

```python
import functools

import jax
import jax.numpy as jnp
from jax import lax
from jax.experimental import pallas as pl
from jax.experimental.pallas import tpu as pltpu
from jax.sharding import PartitionSpec as P


TH = 24
TW = 96
F = 128
C = 256
CAP = 96
PH = 26
PW = 98
NP = 6
NQ = 16
HALF = PH // 2
SOURCES = 128
ROWS = CAP + 2
PAIRS = ROWS // 2
MAIN = HALF * TW
LHS = MAIN + 32
GROUPS = 7
PER = ROWS // GROUPS
BF = jnp.bfloat16
F32 = jnp.float32


def dot(a, b):
    return jnp.dot(a, b, preferred_element_type=F32)


def iota(shape, dim):
    return lax.broadcasted_iota(jnp.int32, shape, dim)


def places():
    return lax.axis_index("lat").astype(jnp.int32), lax.axis_index("lon").astype(jnp.int32)


def parities():
    lat, lon = places()
    return lax.rem(lat, 2), lax.rem(lon, 2)


def with_row(tile, shift, row, at):
    rolled = pltpu.roll(tile, shift, 0)
    return jnp.where(iota(tile.shape, 0) == at, row, rolled)


def send_kernel(features_ref, index_ref, used_ref, out_ref, cells, counts, flat, where, used, sems):
    fetch = pltpu.make_async_copy(index_ref, cells, sems.at[5])
    fetch.start()
    fetch_used = pltpu.make_async_copy(used_ref, counts, sems.at[6])
    fetch_used.start()
    cut = SOURCES // 4
    copies = [
        pltpu.make_async_copy(
            features_ref.at[cut * k : cut * (k + 1)],
            out_ref.at[cut * k : cut * (k + 1), 0 : PAIRS - 1],
            sems.at[k],
        )
        for k in range(4)
    ]
    for copy in copies:
        copy.start()
    fetch_used.wait()
    count = jnp.broadcast_to(counts[...].astype(F32), (128, 128))
    used[...] = jnp.transpose(count)
    fetch.wait()
    lines = [cells[pl.ds(v, 32, stride=3), :].astype(F32) for v in range(3)]
    lat, lon = places()
    shift = lax.rem((lat * 8 + lon) * ROWS, 128)
    lane = iota((32, 128), 1)
    blocks = [
        lines[0],
        jnp.where(lane < 32, pltpu.roll(lines[0], 32, 1), pltpu.roll(lines[1], 32, 1)),
        jnp.where(lane < 64, pltpu.roll(lines[1], 64, 1), pltpu.roll(lines[2], 64, 1)),
        pltpu.roll(lines[2], 96, 1),
    ]
    for j, cell in enumerate(blocks):
        r = jnp.floor((cell + 0.5) * (1.0 / PW))
        s = cell - r * PW
        q = jnp.floor((s - 0.5) * (1.0 / NP))
        pos = (s - 1.0 - q * NP) * NQ + q
        pos = jnp.where(s == 0.0, float(TW), jnp.where(s == PW - 1.0, TW + 1.0, pos))
        r = jnp.where(lane.astype(F32) < used[pl.ds(j, 32, stride=4), :], r, 63.0)
        flat[pl.ds(2 * j, 32, stride=8), :] = pltpu.roll(r, shift, 1)
        flat[pl.ds(2 * j + 1, 32, stride=8), :] = pltpu.roll(pos, shift, 1)
    for t in range(SOURCES):
        where[t, 0] = flat[2 * t : 2 * t + 2, :].astype(BF)
    last = pltpu.make_async_copy(where, out_ref.at[:, PAIRS - 1 : PAIRS], sems.at[4])
    last.start()
    for copy in copies:
        copy.wait()
    last.wait()


def frame_kernel(
    x_ref,
    where_ref,
    spread_ref,
    win_ref,
    wdens_ref,
    grid_ref,
    west_ref,
    east_ref,
    rows_a_ref,
    rows_b_ref,
    c32,
    lanes,
    acc,
    cnt,
    pads,
    mean,
    cols,
):
    for t in range(SOURCES):
        c32[2 * t : 2 * t + 2, :] = where_ref[t, PAIRS - 1].astype(F32)
    both = jnp.concatenate([c32[pl.ds(w, SOURCES, stride=2), :] for w in range(2)], axis=1).astype(BF)
    high = 104
    tile = iota((high, 128), 0).astype(F32) * 128.0
    first = jnp.floor((tile + 0.5) * (1.0 / ROWS))
    source = iota((high, 128), 1).astype(F32)
    picked = [dot(jnp.where(source == first + k, 1.0, 0.0).astype(BF), both) for k in range(3)]
    bound = (first + 1.0) * ROWS - tile

    def joined(side):
        parts = [part[:, 128 * side : 128 * (side + 1)] for part in picked]
        return jnp.where(source < bound, parts[0], jnp.where(source < bound + ROWS, parts[1], parts[2]))

    r, pos = joined(0), joined(1)
    low = jnp.where(r >= HALF, r - HALF, r)
    lanes[0] = r
    lanes[1] = low
    lanes[2] = pos
    lanes[3] = jnp.where(pos >= TW, low + HALF * (pos - TW), -1.0)
    upper = jnp.where(r >= HALF, 1.0, 0.0)
    upper = jnp.transpose(jnp.concatenate([upper, jnp.zeros((128 - high, 128), F32)], axis=0))

    for g in range(GROUPS):
        tiles = range(g * PER, (g + 1) * PER)
        width = PER * 128

        def row(which):
            pieces = [lanes[which, t : t + 1, :] for t in tiles]
            return jnp.broadcast_to(jnp.concatenate(pieces, axis=1), (16, width)).astype(BF)

        r16, low16, pos16, edge16 = (row(w) for w in range(4))
        one, zero = jnp.ones((), BF), jnp.zeros((), BF)
        ids = iota((16, width), 0).astype(F32).astype(BF)

        def hot(values, tile):
            return jnp.where(ids + jnp.asarray(16 * tile, BF) == values, one, zero)

        place = [hot(pos16, t) for t in range(8)]
        parts = []
        for k in range(HALF):
            at = jnp.where(low16 == jnp.asarray(k, BF), one, zero)
            parts += [b * at for b in place[:NP]]
        parts += [hot(edge16, 0), hot(edge16, 1)]
        left = jnp.concatenate(parts, axis=0)
        right = []
        for t in tiles:
            x = x_ref[128 * t : 128 * (t + 1), :]
            up = x * jnp.broadcast_to(upper[:, t : t + 1], (128, 128)).astype(BF)
            right.append(jnp.concatenate([x - up, up], axis=1))
        right = jnp.concatenate(right, axis=0)
        some = lax.dot_general(
            jnp.concatenate([hot(r16, 0), hot(r16, 1)], axis=0),
            jnp.concatenate(place, axis=0),
            (((1,), (1,)), ((), ())),
            preferred_element_type=F32,
        )
        if g == 0:
            acc[...] = dot(left, right)
            cnt[...] = some
        else:
            acc[...] += dot(left, right)
            cnt[...] += some

    def weight(a, b, shape):
        return jnp.broadcast_to(spread_ref[a : a + 1, b : b + 1], shape)

    def tile(r, p):
        lanes_of = slice((r // HALF) * 128, (r // HALF) * 128 + 128)
        base = (r % HALF) * TW + NQ * (p - 1)
        return pads[r, p // NP] if p in (0, NP + 1) else acc[base : base + NQ, lanes_of]

    for r in range(PH):
        lanes_of = slice((r // HALF) * 128, (r // HALF) * 128 + 128)
        at = MAIN + r % HALF
        pads[r, 0] = with_row(tile(r, NP), 1, acc[at : at + 1, lanes_of], 0)
        pads[r, 1] = with_row(tile(r, 1), NQ - 1, acc[at + HALF : at + HALF + 1, lanes_of], NQ - 1)

    number = jnp.transpose(jnp.concatenate([cnt[...], jnp.zeros((96, 128), F32)], axis=0))
    number = [
        with_row(number[TW - NQ : TW], 1, number[TW : TW + 1], 0),
        *(number[NQ * p : NQ * (p + 1)] for p in range(NP)),
        with_row(number[:NQ], NQ - 1, number[TW + 1 : TW + 2], NQ - 1),
    ]
    density = None
    for a in range(3):
        line = [sum(weight(a, b, (NQ, 128)) * number[p + b] for b in range(3)) for p in range(NP)]
        line = jnp.concatenate(line, axis=0)[:, a : a + TH]
        density = line if density is None else density + line
    scale = 1.0 / (1.0 + density)
    log_density = jnp.log(1.0 + density)

    weights = [[weight(a, b, (NQ, F)) for b in range(3)] for a in range(3)]

    def average(rows):
        for i in rows:
            wide = jnp.broadcast_to(scale[:, i : i + 1], (TW, F))
            for p in range(NP):
                data = None
                for a in range(3):
                    for b in range(3):
                        term = weights[a][b] * tile(i + a, p + b)
                        data = term if data is None else data + term
                at = i * TW + p * NQ
                mean[at : at + NQ, :] = (data * wide[p * NQ : (p + 1) * NQ]).astype(BF)

    def project(rows):
        return dot(jnp.concatenate([mean[i * TW : (i + 1) * TW, :] for i in rows], axis=0), win_ref[...])

    def finish(rows, out):
        for k, i in enumerate(rows):
            extra = jnp.broadcast_to(log_density[:, i : i + 1], (TW, C)) * wdens_ref[...]
            cell = (out[k * TW : (k + 1) * TW] + extra).astype(BF)
            grid_ref[i] = cell.reshape(NP, NQ, C)
            wide = cell.astype(F32)
            for c, at in enumerate((0, NQ, 5 * NQ - 1, 6 * NQ - 1)):
                cols[c, i : i + 1, :] = wide[at : at + 1]

    sets = [range(i, i + 4) for i in range(0, TH, 4)]
    average(sets[0])
    for n, rows in enumerate(sets):
        out = project(rows)
        if n + 1 < len(sets):
            average(sets[n + 1])
        finish(rows, out)
    west_ref[...] = cols[0:2].astype(BF)
    east_ref[...] = cols[2:4].astype(BF)

    lat_odd, _ = parities()
    rows = [grid_ref[at : at + 2].reshape(2 * TW, C) for at in (TH - 2, 0)]
    give(lat_odd, rows_a_ref, rows_b_ref, *rows)


def give(odd, a_ref, b_ref, after, before):
    @pl.when(odd == 0)
    def _():
        a_ref[...] = after
        b_ref[...] = before

    @pl.when(odd != 0)
    def _():
        a_ref[...] = before
        b_ref[...] = after


def silu(v):
    return v / (1.0 + jnp.exp(-v))


def column_kernel(rows_a_ref, rows_b_ref, west_ref, east_ref, a_ref, b_ref, tall):
    lat_odd, lon_odd = parities()
    tall[:, 24:, :] = jnp.zeros((4, 8, C), F32)
    for c in range(4):
        tall[c, 2 : 2 + TH, :] = (west_ref if c < 2 else east_ref)[c % 2].astype(F32)

    def halo(north, south):
        for ref, at in ((north, 0), (south, 2 + TH)):
            for k in range(2):
                for c, p in enumerate((0, 1, 4, 5)):
                    tile = ref[k * TW + p * NQ : k * TW + (p + 1) * NQ, :].astype(F32)
                    tall[c, at + k : at + k + 1, :] = tile[:1] if c < 2 else tile[NQ - 1 :]

    pl.when(lat_odd == 0)(lambda: halo(rows_b_ref, rows_a_ref))
    pl.when(lat_odd != 0)(lambda: halo(rows_a_ref, rows_b_ref))
    give(lon_odd, a_ref, b_ref, tall[2:4].astype(BF), tall[0:2].astype(BF))


def nine(weight, window):
    total = None
    for a in range(3):
        for b in range(3):
            term = dot(window(a, b), weight[3 * a + b])
            total = term if total is None else total + term
    return total


def rows_of(src, weight, start, count):
    return nine(weight, lambda a, b: src[start + a : start + a + count, b : b + NP].reshape(count * TW, C))


def padded(dst, at, tiles, first, last, before, after):
    dst[at, 1 : NP + 1] = tiles
    dst[at, 0] = with_row(last, 1, before, 0).astype(BF)
    dst[at, NP + 1] = with_row(first, NQ - 1, after, NQ - 1).astype(BF)


def spread_out(flat, at, tiles):
    for p in range(NP):
        for h in range(2):
            flat[h, pl.ds(at * TW + p, NQ, stride=NP), :] = tiles[p, :, 128 * h : 128 * (h + 1)]


def inner_one_kernel(grid_ref, one_ref, hp_ref, hcols_ref, gp):
    for g in range(TH):
        tile = grid_ref[g]
        first, last = tile[0].astype(F32), tile[NP - 1].astype(F32)
        padded(gp, g, tile, first, last, first[:1], last[NQ - 1 :])
    start = 0
    for count in (4, 4, 4, 4, 4, 2):
        value = silu(rows_of(gp, one_ref, start, count))
        for k in range(count):
            g = start + k + 2
            row = value[k * TW : (k + 1) * TW].reshape(NP, NQ, C)
            padded(hp_ref, g, row.astype(BF), row[0], row[NP - 1], row[0, :1], row[NP - 1, NQ - 1 :])
            for c, (p, q) in enumerate(((1, 0), (2, 0), (3, NQ - 1), (4, NQ - 1))):
                hcols_ref[c, g : g + 1, :] = row[p, q : q + 1]
        start += count


def inner_two_kernel(hp_ref, grid_ref, two_ref, body_ref, flat):
    step = 4
    for i in range(2, TH - 2, step):
        value = rows_of(hp_ref, two_ref, i, step).reshape(step, NP, NQ, C)
        value = value + grid_ref[i : i + step].astype(F32)
        at = i - 2
        for k in range(step):
            spread_out(flat, at + k, value[k])
        for h in range(2):
            block = flat[h, at * TW : (at + step) * TW, :].astype(BF).reshape(step, TW, 128)
            body_ref[at : at + step, :, 128 * h : 128 * (h + 1)] = block


def keeps():
    lat, _ = places()
    return jnp.where(lat > 0, 1.0, 0.0), jnp.where(lat < 15, 1.0, 0.0)


def edge_kernel(
    grid_ref, rows_a_ref, rows_b_ref, hp_ref, one_ref, two_ref, out_ref, ecols_ref, north_ref, south_ref, gp, hr, flat
):
    keep_top, keep_bottom = keeps()
    lat_odd, _ = parities()

    @pl.when(lat_odd == 0)
    def _():
        south_ref[...] = rows_a_ref[...]
        north_ref[...] = rows_b_ref[...]

    @pl.when(lat_odd != 0)
    def _():
        south_ref[...] = rows_b_ref[...]
        north_ref[...] = rows_a_ref[...]

    tiles = [north_ref[k * TW : (k + 1) * TW, :].reshape(NP, NQ, C) for k in range(2)]
    tiles += [grid_ref[g] for g in (0, 1, TH - 2, TH - 1)]
    tiles += [south_ref[k * TW : (k + 1) * TW, :].reshape(NP, NQ, C) for k in range(2)]
    for slot, tile in enumerate(tiles):
        first, last = tile[0].astype(F32), tile[NP - 1].astype(F32)
        padded(gp, slot, tile, first, last, first[:1], last[NQ - 1 :])

    def window(src, a, b):
        return jnp.concatenate(
            [src[at + a : at + a + 2, b : b + NP].reshape(2 * TW, C) for at in (0, 4)], axis=0
        )

    value = silu(nine(one_ref, functools.partial(window, gp)))
    for n, slot in enumerate((0, 1, 6, 7)):
        row = value[n * TW : (n + 1) * TW]
        if n == 0:
            row = row * keep_top
        if n == 3:
            row = row * keep_bottom
        row = row.reshape(NP, NQ, C)
        for c, (p, q) in enumerate(((1, 0), (2, 0), (3, NQ - 1), (4, NQ - 1))):
            ecols_ref[c, n : n + 1, :] = row[p, q : q + 1]
        padded(hr, slot, row.astype(BF), row[0], row[NP - 1], row[0, :1], row[NP - 1, NQ - 1 :])
    for slot, g in ((2, 2), (3, 3), (4, TH - 2), (5, TH - 1)):
        hr[slot] = hp_ref[g]
    value = nine(two_ref, functools.partial(window, hr))
    for n, i in enumerate((0, 1, TH - 2, TH - 1)):
        spread_out(flat, n, value[n * TW : (n + 1) * TW].reshape(NP, NQ, C) + grid_ref[i].astype(F32))
    for h in range(2):
        out_ref[:, :, 128 * h : 128 * (h + 1)] = flat[h].astype(BF).reshape(4, TW, 128)


def last_kernel(
    sent_a_ref,
    sent_b_ref,
    got_a_ref,
    got_b_ref,
    hcols_ref,
    ecols_ref,
    body_ref,
    edge_ref,
    one_ref,
    two_ref,
    out_ref,
    cs,
    hc,
    oc,
    strips,
    sems,
):
    middle = slice(8, TW - 8)
    copies = [
        pltpu.make_async_copy(body_ref.at[:, middle], out_ref.at[2 : TH - 2, middle], sems.at[0]),
        pltpu.make_async_copy(edge_ref.at[:2, middle], out_ref.at[:2, middle], sems.at[1]),
        pltpu.make_async_copy(edge_ref.at[2:, middle], out_ref.at[TH - 2 :, middle], sems.at[2]),
    ]
    for copy in copies:
        copy.start()
    keep_top, keep_bottom = keeps()
    _, lon_odd = parities()
    cs[:, 32:, :] = jnp.zeros((8, 8, C), F32)
    hc[:, 32:, :] = jnp.zeros((8, 8, C), F32)

    def fill(got_before, sent_before, sent_after, got_after):
        for n, ref in enumerate((got_before, sent_before, sent_after, got_after)):
            cs[2 * n : 2 * n + 2, 0:32, :] = ref[...].astype(F32)

    pl.when(lon_odd == 0)(lambda: fill(got_b_ref, sent_b_ref, sent_a_ref, got_a_ref))
    pl.when(lon_odd != 0)(lambda: fill(got_a_ref, sent_a_ref, sent_b_ref, got_b_ref))

    def window(src, a, b):
        return jnp.concatenate([src[c + b, a : a + 32, :].astype(BF) for c in (0, 1, 4, 5)], axis=0)

    value = silu(nine(one_ref, functools.partial(window, cs)))
    line = iota((32, C), 0)
    for n, c in enumerate((0, 1, 6, 7)):
        column = value[32 * n : 32 * (n + 1)]
        column = jnp.where(line == 0, column * keep_top, column)
        hc[c, 0:32, :] = jnp.where(line == TH + 1, column * keep_bottom, column)
    for c in range(4):
        hc[2 + c, 0:32, :] = hcols_ref[c, 0:32, :]
        hc[2 + c, 0:2, :] = ecols_ref[c, 0:2, :]
        hc[2 + c, TH : TH + 2, :] = ecols_ref[c, 2:4, :]
    value = nine(two_ref, functools.partial(window, hc))
    for c in range(4):
        oc[c] = value[32 * c : 32 * c + TH] + cs[2 + c, 2 : 2 + TH, :]
    place = iota((8, C), 0)
    for i in range(TH):
        if 2 <= i < TH - 2:
            rows, at = body_ref, i - 2
        else:
            rows, at = edge_ref, i if i < 2 else i - TH + 4
        left, right = rows[at, :8].astype(F32), rows[at, TW - 8 :].astype(F32)
        left = jnp.where(place == 0, oc[0, i : i + 1, :], jnp.where(place == 1, oc[1, i : i + 1, :], left))
        right = jnp.where(place == 6, oc[2, i : i + 1, :], jnp.where(place == 7, oc[3, i : i + 1, :], right))
        strips[0, i] = left.astype(BF)
        strips[1, i] = right.astype(BF)
    for n, at in enumerate((0, TW - 8)):
        copies.append(pltpu.make_async_copy(strips.at[n], out_ref.at[:, at : at + 8], sems.at[3 + n]))
        copies[-1].start()
    for copy in copies:
        copy.wait()


def vmem(count):
    return [pl.BlockSpec(memory_space=pltpu.VMEM)] * count


def far(count):
    return [pl.BlockSpec(memory_space=pl.ANY)] * count


LIMIT = 40 * 1024 * 1024


def in_hbm(value):
    return pltpu.with_memory_space_constraint(value, pltpu.HBM)


def near(value):
    return pltpu.with_memory_space_constraint(value, pltpu.VMEM)


def send_call(features, cell_index, tile_rows):
    return pl.pallas_call(
        send_kernel,
        out_shape=pltpu.VMEM((SOURCES, PAIRS, 2, F), BF),
        in_specs=far(3),
        out_specs=vmem(1)[0],
        scratch_shapes=[
            pltpu.VMEM((96, 128), jnp.int32),
            pltpu.VMEM((1, 128), jnp.int32),
            pltpu.VMEM((2 * SOURCES, 128), F32),
            pltpu.VMEM((SOURCES, 1, 2, F), BF),
            pltpu.VMEM((128, 128), F32),
            pltpu.SemaphoreType.DMA((7,)),
        ],
        compiler_params=pltpu.CompilerParams(vmem_limit_bytes=LIMIT),
        name="send",
    )(
        in_hbm(features.reshape(SOURCES, PAIRS - 1, 2, F)),
        in_hbm(cell_index.reshape(96, 128)),
        in_hbm(tile_rows.reshape(1, 128)),
    )


def frame_call(received, spread, w_in, w_dens):
    return pl.pallas_call(
        frame_kernel,
        out_shape=(
            pltpu.VMEM((TH, NP, NQ, C), BF),
            *(pltpu.VMEM((2, TH, C), BF),) * 2,
            *(pltpu.VMEM((2 * TW, C), BF),) * 2,
        ),
        in_specs=vmem(5),
        out_specs=tuple(vmem(5)),
        scratch_shapes=[
            pltpu.VMEM((SOURCES * 2, 128), F32),
            pltpu.VMEM((4, 104, 128), F32),
            pltpu.VMEM((LHS, C), F32),
            pltpu.VMEM((32, 128), F32),
            pltpu.VMEM((PH, 2, NQ, F), F32),
            pltpu.VMEM((TH * TW, F), BF),
            pltpu.VMEM((4, TH, C), F32),
        ],
        compiler_params=pltpu.CompilerParams(vmem_limit_bytes=LIMIT),
        name="frame",
    )(near(received.reshape(SOURCES * ROWS, F)), near(received), near(spread), near(w_in), near(w_dens.reshape(1, C)))


def column_call(rows_a, rows_b, west, east):
    return pl.pallas_call(
        column_kernel,
        out_shape=(pltpu.VMEM((2, 32, C), BF),) * 2,
        in_specs=vmem(4),
        out_specs=tuple(vmem(2)),
        scratch_shapes=[pltpu.VMEM((4, 32, C), F32)],
        compiler_params=pltpu.CompilerParams(vmem_limit_bytes=LIMIT),
        name="column",
    )(*(near(value) for value in (rows_a, rows_b, west, east)))


def work(rows):
    return pl.CostEstimate(flops=2 * rows * TW * 9 * C * C, bytes_accessed=0, transcendentals=0)


def inner_one_call(grid, one):
    return pl.pallas_call(
        inner_one_kernel,
        out_shape=(pltpu.VMEM((TH + 2, NP + 2, NQ, C), BF), pltpu.VMEM((4, 40, C), F32)),
        in_specs=vmem(2),
        out_specs=tuple(vmem(2)),
        scratch_shapes=[pltpu.VMEM((TH, NP + 2, NQ, C), BF)],
        compiler_params=pltpu.CompilerParams(vmem_limit_bytes=LIMIT),
        cost_estimate=work(TH - 2),
        name="inner_one",
    )(near(grid), near(one))


def inner_two_call(hp, grid, two):
    return pl.pallas_call(
        inner_two_kernel,
        out_shape=pltpu.VMEM((TH - 4, TW, C), BF),
        in_specs=vmem(3),
        out_specs=vmem(1)[0],
        scratch_shapes=[pltpu.VMEM((2, (TH - 4) * TW, 128), F32)],
        compiler_params=pltpu.CompilerParams(vmem_limit_bytes=LIMIT),
        cost_estimate=work(TH - 4),
        name="inner_two",
    )(near(hp), near(grid), near(two))


def edge_call(*inside):
    return pl.pallas_call(
        edge_kernel,
        out_shape=(pltpu.VMEM((4, TW, C), BF), pltpu.VMEM((4, 8, C), F32)),
        in_specs=vmem(6),
        out_specs=tuple(vmem(2)),
        scratch_shapes=[
            *(pltpu.VMEM((2 * TW, C), BF),) * 2,
            *(pltpu.VMEM((8, NP + 2, NQ, C), BF),) * 2,
            pltpu.VMEM((2, 4 * TW, 128), F32),
        ],
        compiler_params=pltpu.CompilerParams(vmem_limit_bytes=LIMIT),
        cost_estimate=work(8),
        name="edge",
    )(*(near(value) for value in inside))


def last_call(*inside):
    return pl.pallas_call(
        last_kernel,
        out_shape=jax.ShapeDtypeStruct((TH, TW, C), BF),
        in_specs=vmem(10),
        out_specs=far(1)[0],
        scratch_shapes=[
            *(pltpu.VMEM((8, 40, C), F32),) * 2,
            pltpu.VMEM((4, TH, C), F32),
            pltpu.VMEM((2, TH, 8, C), BF),
            pltpu.SemaphoreType.DMA((5,)),
        ],
        compiler_params=pltpu.CompilerParams(vmem_limit_bytes=LIMIT),
        cost_estimate=work(3),
        name="last",
    )(*(near(value) for value in inside))


def swaps(axis, first, around):
    count = lax.axis_size(axis)
    pairs = [(i, (i + 1) % count) for i in range(first, count, 2) if around or i + 1 < count]
    return pairs + [(j, i) for i, j in pairs]


def shards(features, cell_index, tile_rows, spread, w_in, w_dens, w_one, w_two):
    sent = send_call(features, cell_index, tile_rows)
    received = lax.all_to_all(sent, ("lat", "lon"), split_axis=0, concat_axis=0, tiled=True)
    grid, west, east, rows_a, rows_b = frame_call(received, spread, w_in, w_dens)
    one, two = w_one.reshape(9, C, C), w_two.reshape(9, C, C)
    rows_b = lax.ppermute(rows_b, "lat", swaps("lat", 1, False))
    rows_a = lax.ppermute(rows_a, "lat", swaps("lat", 0, False))
    hp, hcols = inner_one_call(grid, one)
    body = inner_two_call(hp, grid, two)
    sent_a, sent_b = column_call(rows_a, rows_b, west, east)
    got_b = lax.ppermute(sent_b, "lon", swaps("lon", 1, True))
    got_a = lax.ppermute(sent_a, "lon", swaps("lon", 0, True))
    edge, ecols = edge_call(grid, rows_a, rows_b, hp, one, two)
    return last_call(sent_a, sent_b, got_a, got_b, hcols, ecols, body, edge, one, two)


def solution(mesh):
    in_specs = (
        P(("lat", "lon"), None),
        P(("lat", "lon")),
        P(("lat", "lon")),
        P(),
        P(),
        P(),
        P(),
        P(),
    )
    out_specs = P("lat", "lon", None)
    return jax.shard_map(shards, mesh=mesh, in_specs=in_specs, out_specs=out_specs, check_vma=False)
```

```python
import functools

import jax
import jax.numpy as jnp
from jax import lax
from jax.experimental import pallas as pl
from jax.experimental.pallas import tpu as pltpu
from jax.sharding import PartitionSpec as P


TH = 24
TW = 96
F = 128
C = 256
CAP = 96
PH = 26
PW = 98
NP = 6
NQ = 16
HALF = PH // 2
SOURCES = 128
ROWS = CAP + 2
PAIRS = ROWS // 2
MAIN = HALF * TW
LHS = MAIN + 32
GROUPS = 7
CUT = 10
PER = ROWS // GROUPS
BF = jnp.bfloat16
F32 = jnp.float32


def dot(a, b):
    return jnp.dot(a, b, preferred_element_type=F32)


def iota(shape, dim):
    return lax.broadcasted_iota(jnp.int32, shape, dim)


def places():
    return lax.axis_index("lat").astype(jnp.int32), lax.axis_index("lon").astype(jnp.int32)


def parities():
    lat, lon = places()
    return lax.rem(lat, 2), lax.rem(lon, 2)


def with_row(tile, shift, row, at):
    rolled = pltpu.roll(tile, shift, 0)
    return jnp.where(iota(tile.shape, 0) == at, row, rolled)


def send_kernel(features_ref, index_ref, used_ref, out_ref, cells, counts, flat, where, used, sems):
    fetch = pltpu.make_async_copy(index_ref, cells, sems.at[5])
    fetch.start()
    fetch_used = pltpu.make_async_copy(used_ref, counts, sems.at[6])
    fetch_used.start()
    cut = SOURCES // 4
    copies = [
        pltpu.make_async_copy(
            features_ref.at[cut * k : cut * (k + 1)],
            out_ref.at[cut * k : cut * (k + 1), 0 : PAIRS - 1],
            sems.at[k],
        )
        for k in range(4)
    ]
    for copy in copies:
        copy.start()
    fetch_used.wait()
    count = jnp.broadcast_to(counts[...].astype(F32), (128, 128))
    used[...] = jnp.transpose(count)
    fetch.wait()
    lines = [cells[pl.ds(v, 32, stride=3), :].astype(F32) for v in range(3)]
    lat, lon = places()
    shift = lax.rem((lat * 8 + lon) * ROWS, 128)
    lane = iota((32, 128), 1)
    blocks = [
        lines[0],
        jnp.where(lane < 32, pltpu.roll(lines[0], 32, 1), pltpu.roll(lines[1], 32, 1)),
        jnp.where(lane < 64, pltpu.roll(lines[1], 64, 1), pltpu.roll(lines[2], 64, 1)),
        pltpu.roll(lines[2], 96, 1),
    ]
    for j, cell in enumerate(blocks):
        r = jnp.floor((cell + 0.5) * (1.0 / PW))
        s = cell - r * PW
        q = jnp.floor((s - 0.5) * (1.0 / NP))
        pos = (s - 1.0 - q * NP) * NQ + q
        pos = jnp.where(s == 0.0, float(TW), jnp.where(s == PW - 1.0, TW + 1.0, pos))
        r = jnp.where(lane.astype(F32) < used[pl.ds(j, 32, stride=4), :], r, 63.0)
        flat[pl.ds(2 * j, 32, stride=8), :] = pltpu.roll(r, shift, 1)
        flat[pl.ds(2 * j + 1, 32, stride=8), :] = pltpu.roll(pos, shift, 1)
    for t in range(SOURCES):
        where[t, 0] = flat[2 * t : 2 * t + 2, :].astype(BF)
    last = pltpu.make_async_copy(where, out_ref.at[:, PAIRS - 1 : PAIRS], sems.at[4])
    last.start()
    for copy in copies:
        copy.wait()
    last.wait()


def frame_kernel(
    x_ref,
    where_ref,
    spread_ref,
    win_ref,
    wdens_ref,
    grid_ref,
    west_ref,
    east_ref,
    rows_a_ref,
    rows_b_ref,
    c32,
    lanes,
    acc,
    cnt,
    pads,
    mean,
    cols,
):
    for t in range(SOURCES):
        c32[2 * t : 2 * t + 2, :] = where_ref[t, PAIRS - 1].astype(F32)
    both = jnp.concatenate([c32[pl.ds(w, SOURCES, stride=2), :] for w in range(2)], axis=1).astype(BF)
    high = 104
    tile = iota((high, 128), 0).astype(F32) * 128.0
    first = jnp.floor((tile + 0.5) * (1.0 / ROWS))
    source = iota((high, 128), 1).astype(F32)
    picked = [dot(jnp.where(source == first + k, 1.0, 0.0).astype(BF), both) for k in range(3)]
    bound = (first + 1.0) * ROWS - tile

    def joined(side):
        parts = [part[:, 128 * side : 128 * (side + 1)] for part in picked]
        return jnp.where(source < bound, parts[0], jnp.where(source < bound + ROWS, parts[1], parts[2]))

    r, pos = joined(0), joined(1)
    low = jnp.where(r >= HALF, r - HALF, r)
    lanes[0] = r
    lanes[1] = low
    lanes[2] = pos
    lanes[3] = jnp.where(pos >= TW, low + HALF * (pos - TW), -1.0)
    upper = jnp.where(r >= HALF, 1.0, 0.0)
    upper = jnp.transpose(jnp.concatenate([upper, jnp.zeros((128 - high, 128), F32)], axis=0))

    for g in range(GROUPS):
        tiles = range(g * PER, (g + 1) * PER)
        width = PER * 128

        def row(which):
            pieces = [lanes[which, t : t + 1, :] for t in tiles]
            return jnp.broadcast_to(jnp.concatenate(pieces, axis=1), (16, width)).astype(BF)

        r16, low16, pos16, edge16 = (row(w) for w in range(4))
        one, zero = jnp.ones((), BF), jnp.zeros((), BF)
        ids = iota((16, width), 0).astype(F32).astype(BF)

        def hot(values, tile):
            return jnp.where(ids + jnp.asarray(16 * tile, BF) == values, one, zero)

        place = [hot(pos16, t) for t in range(8)]
        parts = []
        for k in range(HALF):
            at = jnp.where(low16 == jnp.asarray(k, BF), one, zero)
            parts += [b * at for b in place[:NP]]
        parts += [hot(edge16, 0), hot(edge16, 1)]
        left = jnp.concatenate(parts, axis=0)
        right = []
        for t in tiles:
            x = x_ref[128 * t : 128 * (t + 1), :]
            up = x * jnp.broadcast_to(upper[:, t : t + 1], (128, 128)).astype(BF)
            right.append(jnp.concatenate([x - up, up], axis=1))
        right = jnp.concatenate(right, axis=0)
        some = lax.dot_general(
            jnp.concatenate([hot(r16, 0), hot(r16, 1)], axis=0),
            jnp.concatenate(place, axis=0),
            (((1,), (1,)), ((), ())),
            preferred_element_type=F32,
        )
        if g == 0:
            acc[...] = dot(left, right)
            cnt[...] = some
        else:
            acc[...] += dot(left, right)
            cnt[...] += some

    def weight(a, b, shape):
        return jnp.broadcast_to(spread_ref[a : a + 1, b : b + 1], shape)

    def tile(r, p):
        lanes_of = slice((r // HALF) * 128, (r // HALF) * 128 + 128)
        base = (r % HALF) * TW + NQ * (p - 1)
        return pads[r, p // NP] if p in (0, NP + 1) else acc[base : base + NQ, lanes_of]

    for r in range(PH):
        lanes_of = slice((r // HALF) * 128, (r // HALF) * 128 + 128)
        at = MAIN + r % HALF
        pads[r, 0] = with_row(tile(r, NP), 1, acc[at : at + 1, lanes_of], 0)
        pads[r, 1] = with_row(tile(r, 1), NQ - 1, acc[at + HALF : at + HALF + 1, lanes_of], NQ - 1)

    number = jnp.transpose(jnp.concatenate([cnt[...], jnp.zeros((96, 128), F32)], axis=0))
    number = [
        with_row(number[TW - NQ : TW], 1, number[TW : TW + 1], 0),
        *(number[NQ * p : NQ * (p + 1)] for p in range(NP)),
        with_row(number[:NQ], NQ - 1, number[TW + 1 : TW + 2], NQ - 1),
    ]
    density = None
    for a in range(3):
        line = [sum(weight(a, b, (NQ, 128)) * number[p + b] for b in range(3)) for p in range(NP)]
        line = jnp.concatenate(line, axis=0)[:, a : a + TH]
        density = line if density is None else density + line
    scale = 1.0 / (1.0 + density)
    log_density = jnp.log(1.0 + density)

    weights = [[weight(a, b, (NQ, F)) for b in range(3)] for a in range(3)]

    def average(rows):
        for i in rows:
            wide = jnp.broadcast_to(scale[:, i : i + 1], (TW, F))
            for p in range(NP):
                data = None
                for a in range(3):
                    for b in range(3):
                        term = weights[a][b] * tile(i + a, p + b)
                        data = term if data is None else data + term
                at = i * TW + p * NQ
                mean[at : at + NQ, :] = (data * wide[p * NQ : (p + 1) * NQ]).astype(BF)

    def project(rows):
        return dot(jnp.concatenate([mean[i * TW : (i + 1) * TW, :] for i in rows], axis=0), win_ref[...])

    def finish(rows, out):
        for k, i in enumerate(rows):
            extra = jnp.broadcast_to(log_density[:, i : i + 1], (TW, C)) * wdens_ref[...]
            cell = (out[k * TW : (k + 1) * TW] + extra).astype(BF)
            grid_ref[i] = cell.reshape(NP, NQ, C)
            wide = cell.astype(F32)
            for c, at in enumerate((0, NQ, 5 * NQ - 1, 6 * NQ - 1)):
                cols[c, i : i + 1, :] = wide[at : at + 1]

    sets = [range(i, i + 4) for i in range(0, TH, 4)]
    average(sets[0])
    for n, rows in enumerate(sets):
        out = project(rows)
        if n + 1 < len(sets):
            average(sets[n + 1])
        finish(rows, out)
    west_ref[...] = cols[0:2].astype(BF)
    east_ref[...] = cols[2:4].astype(BF)

    lat_odd, _ = parities()
    rows = [grid_ref[at : at + 2].reshape(2 * TW, C) for at in (TH - 2, 0)]
    rows_a_ref[...], rows_b_ref[...] = chosen(lat_odd, *rows)


def chosen(odd, a, b):
    return jnp.where(odd == 0, a, b), jnp.where(odd == 0, b, a)


def silu(v):
    return v / (1.0 + jnp.exp(-v))


def column_kernel(rows_a_ref, rows_b_ref, west_ref, east_ref, a_ref, b_ref, tall):
    lat_odd, lon_odd = parities()
    tall[:, 24:, :] = jnp.zeros((4, 8, C), F32)
    for c in range(4):
        tall[c, 2 : 2 + TH, :] = (west_ref if c < 2 else east_ref)[c % 2].astype(F32)

    def halo(north, south):
        for ref, at in ((north, 0), (south, 2 + TH)):
            for k in range(2):
                for c, p in enumerate((0, 1, 4, 5)):
                    tile = ref[k * TW + p * NQ : k * TW + (p + 1) * NQ, :].astype(F32)
                    tall[c, at + k : at + k + 1, :] = tile[:1] if c < 2 else tile[NQ - 1 :]

    pl.when(lat_odd == 0)(lambda: halo(rows_b_ref, rows_a_ref))
    pl.when(lat_odd != 0)(lambda: halo(rows_a_ref, rows_b_ref))
    after, before = chosen(lon_odd, tall[2:4], tall[0:2])
    a_ref[...] = after.astype(BF)
    b_ref[...] = before.astype(BF)


def nine(weight, window):
    total = None
    for a in range(3):
        for b in range(3):
            term = dot(window(a, b), weight[3 * a + b])
            total = term if total is None else total + term
    return total


def rows_of(src, weight, start, count):
    return nine(weight, lambda a, b: src[start + a : start + a + count, b : b + NP].reshape(count * TW, C))


def padded(dst, at, tiles, first, last, before, after):
    dst[at, 1 : NP + 1] = tiles
    dst[at, 0] = with_row(last, 1, before, 0).astype(BF)
    dst[at, NP + 1] = with_row(first, NQ - 1, after, NQ - 1).astype(BF)


def spread_out(flat, at, tiles):
    for p in range(NP):
        for h in range(2):
            flat[h, pl.ds(at * TW + p, NQ, stride=NP), :] = tiles[p, :, 128 * h : 128 * (h + 1)]


def inner_one_kernel(grid_ref, one_ref, hp_ref, hcols_ref, gp):
    for g in range(TH):
        tile = grid_ref[g]
        first, last = tile[0].astype(F32), tile[NP - 1].astype(F32)
        padded(gp, g, tile, first, last, first[:1], last[NQ - 1 :])
    start = 0
    for count in (4, 4, 4, 4, 4, 2):
        value = silu(rows_of(gp, one_ref, start, count))
        for k in range(count):
            g = start + k + 2
            row = value[k * TW : (k + 1) * TW].reshape(NP, NQ, C)
            padded(hp_ref, g, row.astype(BF), row[0], row[NP - 1], row[0, :1], row[NP - 1, NQ - 1 :])
            for c, (p, q) in enumerate(((1, 0), (2, 0), (3, NQ - 1), (4, NQ - 1))):
                hcols_ref[c, g : g + 1, :] = row[p, q : q + 1]
        start += count


def inner_two_kernel(begin, end, hp_ref, grid_ref, two_ref, body_ref, flat):
    step = 4
    for i in range(begin, end, step):
        value = rows_of(hp_ref, two_ref, i, step).reshape(step, NP, NQ, C)
        value = value + grid_ref[i : i + step].astype(F32)
        at = i - begin
        for k in range(step):
            spread_out(flat, at + k, value[k])
        for h in range(2):
            block = flat[h, at * TW : (at + step) * TW, :].astype(BF).reshape(step, TW, 128)
            body_ref[at : at + step, :, 128 * h : 128 * (h + 1)] = block


def keeps():
    lat, _ = places()
    return jnp.where(lat > 0, 1.0, 0.0), jnp.where(lat < 15, 1.0, 0.0)


def edge_kernel(
    grid_ref,
    rows_a_ref,
    rows_b_ref,
    hp_ref,
    body_ref,
    rest_ref,
    one_ref,
    two_ref,
    out_ref,
    ecols_ref,
    partial_ref,
    gp,
    hr,
    flat,
    sems,
):
    copies = [
        pltpu.make_async_copy(body_ref, partial_ref.at[2:CUT], sems.at[0]),
        pltpu.make_async_copy(rest_ref, partial_ref.at[CUT : TH - 2], sems.at[1]),
    ]
    for copy in copies:
        copy.start()
    keep_top, keep_bottom = keeps()
    lat_odd, _ = parities()

    south, north = chosen(lat_odd, rows_a_ref[...], rows_b_ref[...])
    tiles = [north[k * TW : (k + 1) * TW, :].reshape(NP, NQ, C) for k in range(2)]
    tiles += [grid_ref[g] for g in (0, 1, TH - 2, TH - 1)]
    tiles += [south[k * TW : (k + 1) * TW, :].reshape(NP, NQ, C) for k in range(2)]
    for slot, tile in enumerate(tiles):
        first, last = tile[0].astype(F32), tile[NP - 1].astype(F32)
        padded(gp, slot, tile, first, last, first[:1], last[NQ - 1 :])

    def window(src, a, b):
        return jnp.concatenate(
            [src[at + a : at + a + 2, b : b + NP].reshape(2 * TW, C) for at in (0, 4)], axis=0
        )

    value = silu(nine(one_ref, functools.partial(window, gp)))
    for n, slot in enumerate((0, 1, 6, 7)):
        row = value[n * TW : (n + 1) * TW]
        if n == 0:
            row = row * keep_top
        if n == 3:
            row = row * keep_bottom
        row = row.reshape(NP, NQ, C)
        for c, (p, q) in enumerate(((1, 0), (2, 0), (3, NQ - 1), (4, NQ - 1))):
            ecols_ref[c, n : n + 1, :] = row[p, q : q + 1]
        padded(hr, slot, row.astype(BF), row[0], row[NP - 1], row[0, :1], row[NP - 1, NQ - 1 :])
    for slot, g in ((2, 2), (3, 3), (4, TH - 2), (5, TH - 1)):
        hr[slot] = hp_ref[g]
    value = nine(two_ref, functools.partial(window, hr))
    for n, i in enumerate((0, 1, TH - 2, TH - 1)):
        spread_out(flat, n, value[n * TW : (n + 1) * TW].reshape(NP, NQ, C) + grid_ref[i].astype(F32))
    for h in range(2):
        out_ref[:, :, 128 * h : 128 * (h + 1)] = flat[h].astype(BF).reshape(4, TW, 128)
    for copy in copies:
        copy.wait()


def last_kernel(
    sent_a_ref,
    sent_b_ref,
    got_a_ref,
    got_b_ref,
    hcols_ref,
    ecols_ref,
    body_ref,
    rest_ref,
    edge_ref,
    one_ref,
    two_ref,
    partial_ref,
    out_ref,
    cs,
    hc,
    oc,
    strips,
    sems,
):
    middle = slice(8, TW - 8)
    copies = [
        pltpu.make_async_copy(edge_ref.at[:2, middle], out_ref.at[:2, middle], sems.at[1]),
        pltpu.make_async_copy(edge_ref.at[2:, middle], out_ref.at[TH - 2 :, middle], sems.at[2]),
    ]
    for copy in copies:
        copy.start()
    keep_top, keep_bottom = keeps()
    _, lon_odd = parities()
    cs[:, 32:, :] = jnp.zeros((8, 8, C), F32)
    hc[:, 32:, :] = jnp.zeros((8, 8, C), F32)

    got_after, got_before = chosen(lon_odd, got_a_ref[...].astype(F32), got_b_ref[...].astype(F32))
    sent_after, sent_before = chosen(lon_odd, sent_a_ref[...].astype(F32), sent_b_ref[...].astype(F32))
    for n, value in enumerate((got_before, sent_before, sent_after, got_after)):
        cs[2 * n : 2 * n + 2, 0:32, :] = value

    def window(src, a, b):
        return jnp.concatenate([src[c + b, a : a + 32, :].astype(BF) for c in (0, 1, 4, 5)], axis=0)

    value = silu(nine(one_ref, functools.partial(window, cs)))
    line = iota((32, C), 0)
    for n, c in enumerate((0, 1, 6, 7)):
        column = value[32 * n : 32 * (n + 1)]
        column = jnp.where(line == 0, column * keep_top, column)
        hc[c, 0:32, :] = jnp.where(line == TH + 1, column * keep_bottom, column)
    for c in range(4):
        hc[2 + c, 0:32, :] = hcols_ref[c, 0:32, :]
        hc[2 + c, 0:2, :] = ecols_ref[c, 0:2, :]
        hc[2 + c, TH : TH + 2, :] = ecols_ref[c, 2:4, :]
    value = nine(two_ref, functools.partial(window, hc))
    for c in range(4):
        oc[c] = value[32 * c : 32 * c + TH] + cs[2 + c, 2 : 2 + TH, :]
    place = iota((8, C), 0)
    for i in range(TH):
        if 2 <= i < CUT:
            rows, at = body_ref, i - 2
        elif CUT <= i < TH - 2:
            rows, at = rest_ref, i - CUT
        else:
            rows, at = edge_ref, i if i < 2 else i - TH + 4
        left, right = rows[at, :8].astype(F32), rows[at, TW - 8 :].astype(F32)
        left = jnp.where(place == 0, oc[0, i : i + 1, :], jnp.where(place == 1, oc[1, i : i + 1, :], left))
        right = jnp.where(place == 6, oc[2, i : i + 1, :], jnp.where(place == 7, oc[3, i : i + 1, :], right))
        strips[0, i] = left.astype(BF)
        strips[1, i] = right.astype(BF)
    for n, at in enumerate((0, TW - 8)):
        copies.append(pltpu.make_async_copy(strips.at[n], out_ref.at[:, at : at + 8], sems.at[3 + n]))
        copies[-1].start()
    for copy in copies:
        copy.wait()


def vmem(count):
    return [pl.BlockSpec(memory_space=pltpu.VMEM)] * count


def far(count):
    return [pl.BlockSpec(memory_space=pl.ANY)] * count


LIMIT = 40 * 1024 * 1024


def in_hbm(value):
    return pltpu.with_memory_space_constraint(value, pltpu.HBM)


def near(value):
    return pltpu.with_memory_space_constraint(value, pltpu.VMEM)


def send_call(features, cell_index, tile_rows):
    return pl.pallas_call(
        send_kernel,
        out_shape=pltpu.VMEM((SOURCES, PAIRS, 2, F), BF),
        in_specs=far(3),
        out_specs=vmem(1)[0],
        scratch_shapes=[
            pltpu.VMEM((96, 128), jnp.int32),
            pltpu.VMEM((1, 128), jnp.int32),
            pltpu.VMEM((2 * SOURCES, 128), F32),
            pltpu.VMEM((SOURCES, 1, 2, F), BF),
            pltpu.VMEM((128, 128), F32),
            pltpu.SemaphoreType.DMA((7,)),
        ],
        compiler_params=pltpu.CompilerParams(vmem_limit_bytes=LIMIT),
        name="send",
    )(
        in_hbm(features.reshape(SOURCES, PAIRS - 1, 2, F)),
        in_hbm(cell_index.reshape(96, 128)),
        in_hbm(tile_rows.reshape(1, 128)),
    )


def frame_call(received, spread, w_in, w_dens):
    return pl.pallas_call(
        frame_kernel,
        out_shape=(
            pltpu.VMEM((TH, NP, NQ, C), BF),
            *(pltpu.VMEM((2, TH, C), BF),) * 2,
            *(pltpu.VMEM((2 * TW, C), BF),) * 2,
        ),
        in_specs=vmem(5),
        out_specs=tuple(vmem(5)),
        scratch_shapes=[
            pltpu.VMEM((SOURCES * 2, 128), F32),
            pltpu.VMEM((4, 104, 128), F32),
            pltpu.VMEM((LHS, C), F32),
            pltpu.VMEM((32, 128), F32),
            pltpu.VMEM((PH, 2, NQ, F), F32),
            pltpu.VMEM((TH * TW, F), BF),
            pltpu.VMEM((4, TH, C), F32),
        ],
        compiler_params=pltpu.CompilerParams(vmem_limit_bytes=LIMIT),
        name="frame",
    )(near(received.reshape(SOURCES * ROWS, F)), near(received), near(spread), near(w_in), near(w_dens.reshape(1, C)))


def column_call(rows_a, rows_b, west, east):
    return pl.pallas_call(
        column_kernel,
        out_shape=(pltpu.VMEM((2, 32, C), BF),) * 2,
        in_specs=vmem(4),
        out_specs=tuple(vmem(2)),
        scratch_shapes=[pltpu.VMEM((4, 32, C), F32)],
        compiler_params=pltpu.CompilerParams(vmem_limit_bytes=LIMIT),
        name="column",
    )(*(near(value) for value in (rows_a, rows_b, west, east)))


def work(rows):
    return pl.CostEstimate(flops=2 * rows * TW * 9 * C * C, bytes_accessed=0, transcendentals=0)


def inner_one_call(grid, one):
    return pl.pallas_call(
        inner_one_kernel,
        out_shape=(pltpu.VMEM((TH + 2, NP + 2, NQ, C), BF), pltpu.VMEM((4, 40, C), F32)),
        in_specs=vmem(2),
        out_specs=tuple(vmem(2)),
        scratch_shapes=[pltpu.VMEM((TH, NP + 2, NQ, C), BF)],
        compiler_params=pltpu.CompilerParams(vmem_limit_bytes=LIMIT),
        cost_estimate=work(TH - 2),
        name="inner_one",
    )(near(grid), near(one))


def inner_two_call(begin, end, hp, grid, two):
    return pl.pallas_call(
        functools.partial(inner_two_kernel, begin, end),
        out_shape=pltpu.VMEM((end - begin, TW, C), BF),
        in_specs=vmem(3),
        out_specs=vmem(1)[0],
        scratch_shapes=[pltpu.VMEM((2, (end - begin) * TW, 128), F32)],
        compiler_params=pltpu.CompilerParams(vmem_limit_bytes=LIMIT),
        cost_estimate=work(end - begin),
    )(near(hp), near(grid), near(two))


def edge_call(*inside):
    return pl.pallas_call(
        edge_kernel,
        out_shape=(pltpu.VMEM((4, TW, C), BF), pltpu.VMEM((4, 8, C), F32), pltpu.HBM((TH, TW, C), BF)),
        in_specs=vmem(8),
        out_specs=(*vmem(2), *far(1)),
        scratch_shapes=[
            *(pltpu.VMEM((8, NP + 2, NQ, C), BF),) * 2,
            pltpu.VMEM((2, 4 * TW, 128), F32),
            pltpu.SemaphoreType.DMA((2,)),
        ],
        compiler_params=pltpu.CompilerParams(vmem_limit_bytes=LIMIT),
        cost_estimate=work(8),
        name="edge",
    )(*(near(value) for value in inside))


def last_call(partial, *inside):
    return pl.pallas_call(
        last_kernel,
        out_shape=jax.ShapeDtypeStruct((TH, TW, C), BF),
        in_specs=[*vmem(11), *far(1)],
        out_specs=far(1)[0],
        scratch_shapes=[
            *(pltpu.VMEM((8, 40, C), F32),) * 2,
            pltpu.VMEM((4, TH, C), F32),
            pltpu.VMEM((2, TH, 8, C), BF),
            pltpu.SemaphoreType.DMA((6,)),
        ],
        input_output_aliases={11: 0},
        compiler_params=pltpu.CompilerParams(vmem_limit_bytes=LIMIT),
        cost_estimate=work(3),
        name="last",
    )(*(near(value) for value in inside), partial)


def swaps(axis, first, around):
    count = lax.axis_size(axis)
    pairs = [(i, (i + 1) % count) for i in range(first, count, 2) if around or i + 1 < count]
    return pairs + [(j, i) for i, j in pairs]


def shards(features, cell_index, tile_rows, spread, w_in, w_dens, w_one, w_two):
    sent = send_call(features, cell_index, tile_rows)
    received = lax.all_to_all(sent, ("lat", "lon"), split_axis=0, concat_axis=0, tiled=True)
    grid, west, east, rows_a, rows_b = frame_call(received, spread, w_in, w_dens)
    one, two = w_one.reshape(9, C, C), w_two.reshape(9, C, C)
    rows_b = lax.ppermute(rows_b, "lat", swaps("lat", 1, False))
    rows_a = lax.ppermute(rows_a, "lat", swaps("lat", 0, False))
    hp, hcols = inner_one_call(grid, one)
    body = inner_two_call(2, CUT, hp, grid, two)
    sent_a, sent_b = column_call(rows_a, rows_b, west, east)
    got_b = lax.ppermute(sent_b, "lon", swaps("lon", 1, True))
    got_a = lax.ppermute(sent_a, "lon", swaps("lon", 0, True))
    rest = inner_two_call(CUT, TH - 2, hp, grid, two)
    edge, ecols, partial = edge_call(grid, rows_a, rows_b, hp, body, rest, one, two)
    return last_call(partial, sent_a, sent_b, got_a, got_b, hcols, ecols, body, rest, edge, one, two)


def solution(mesh):
    in_specs = (
        P(("lat", "lon"), None),
        P(("lat", "lon")),
        P(("lat", "lon")),
        P(),
        P(),
        P(),
        P(),
        P(),
    )
    out_specs = P("lat", "lon", None)
    return jax.shard_map(shards, mesh=mesh, in_specs=in_specs, out_specs=out_specs, check_vma=False)
```

```python
import functools

import jax
import jax.numpy as jnp
from jax import lax
from jax.experimental import pallas as pl
from jax.experimental.pallas import tpu as pltpu
from jax.sharding import PartitionSpec as P


TH = 24
TW = 96
F = 128
C = 256
CAP = 96
PH = 26
PW = 98
NP = 6
NQ = 16
HALF = PH // 2
SOURCES = 128
ROWS = CAP + 2
PAIRS = ROWS // 2
MAIN = HALF * TW
LHS = MAIN + 32
GROUPS = 7
CUT = 10
PER = ROWS // GROUPS
BF = jnp.bfloat16
F32 = jnp.float32


def dot(a, b):
    return jnp.dot(a, b, preferred_element_type=F32)


def iota(shape, dim):
    return lax.broadcasted_iota(jnp.int32, shape, dim)


def places():
    return lax.axis_index("lat").astype(jnp.int32), lax.axis_index("lon").astype(jnp.int32)


def parities():
    lat, lon = places()
    return lax.rem(lat, 2), lax.rem(lon, 2)


def with_row(tile, shift, row, at):
    rolled = pltpu.roll(tile, shift, 0)
    return jnp.where(iota(tile.shape, 0) == at, row, rolled)


def send_kernel(features_ref, index_ref, used_ref, out_ref, cells, counts, flat, where, used, sems):
    fetch = pltpu.make_async_copy(index_ref, cells, sems.at[5])
    fetch.start()
    fetch_used = pltpu.make_async_copy(used_ref, counts, sems.at[6])
    fetch_used.start()
    cut = SOURCES // 4
    copies = [
        pltpu.make_async_copy(
            features_ref.at[cut * k : cut * (k + 1)],
            out_ref.at[cut * k : cut * (k + 1), 0 : PAIRS - 1],
            sems.at[k],
        )
        for k in range(4)
    ]
    for copy in copies:
        copy.start()
    fetch_used.wait()
    count = jnp.broadcast_to(counts[...].astype(F32), (128, 128))
    used[...] = jnp.transpose(count)
    fetch.wait()
    lines = [cells[pl.ds(v, 32, stride=3), :].astype(F32) for v in range(3)]
    lat, lon = places()
    shift = lax.rem((lat * 8 + lon) * ROWS, 128)
    lane = iota((32, 128), 1)
    blocks = [
        lines[0],
        jnp.where(lane < 32, pltpu.roll(lines[0], 32, 1), pltpu.roll(lines[1], 32, 1)),
        jnp.where(lane < 64, pltpu.roll(lines[1], 64, 1), pltpu.roll(lines[2], 64, 1)),
        pltpu.roll(lines[2], 96, 1),
    ]
    for j, cell in enumerate(blocks):
        r = jnp.floor((cell + 0.5) * (1.0 / PW))
        s = cell - r * PW
        q = jnp.floor((s - 0.5) * (1.0 / NP))
        pos = (s - 1.0 - q * NP) * NQ + q
        pos = jnp.where(s == 0.0, float(TW), jnp.where(s == PW - 1.0, TW + 1.0, pos))
        r = jnp.where(lane.astype(F32) < used[pl.ds(j, 32, stride=4), :], r, 63.0)
        flat[pl.ds(2 * j, 32, stride=8), :] = pltpu.roll(r, shift, 1)
        flat[pl.ds(2 * j + 1, 32, stride=8), :] = pltpu.roll(pos, shift, 1)
    for t in range(SOURCES):
        where[t, 0] = flat[2 * t : 2 * t + 2, :].astype(BF)
    last = pltpu.make_async_copy(where, out_ref.at[:, PAIRS - 1 : PAIRS], sems.at[4])
    last.start()
    for copy in copies:
        copy.wait()
    last.wait()


def frame_kernel(
    x_ref,
    where_ref,
    spread_ref,
    win_ref,
    wdens_ref,
    grid_ref,
    west_ref,
    east_ref,
    rows_a_ref,
    rows_b_ref,
    c32,
    lanes,
    acc,
    cnt,
    pads,
    mean,
    cols,
):
    for t in range(SOURCES):
        c32[2 * t : 2 * t + 2, :] = where_ref[t, PAIRS - 1].astype(F32)
    both = jnp.concatenate([c32[pl.ds(w, SOURCES, stride=2), :] for w in range(2)], axis=1).astype(BF)
    high = 104
    tile = iota((high, 128), 0).astype(F32) * 128.0
    first = jnp.floor((tile + 0.5) * (1.0 / ROWS))
    source = iota((high, 128), 1).astype(F32)
    picked = [dot(jnp.where(source == first + k, 1.0, 0.0).astype(BF), both) for k in range(3)]
    bound = (first + 1.0) * ROWS - tile

    def joined(side):
        parts = [part[:, 128 * side : 128 * (side + 1)] for part in picked]
        return jnp.where(source < bound, parts[0], jnp.where(source < bound + ROWS, parts[1], parts[2]))

    r, pos = joined(0), joined(1)
    low = jnp.where(r >= HALF, r - HALF, r)
    lanes[0] = r
    lanes[1] = low
    lanes[2] = pos
    lanes[3] = jnp.where(pos >= TW, low + HALF * (pos - TW), -1.0)
    upper = jnp.where(r >= HALF, 1.0, 0.0)
    upper = jnp.transpose(jnp.concatenate([upper, jnp.zeros((128 - high, 128), F32)], axis=0))

    for g in range(GROUPS):
        tiles = range(g * PER, (g + 1) * PER)
        width = PER * 128

        def row(which):
            pieces = [lanes[which, t : t + 1, :] for t in tiles]
            return jnp.broadcast_to(jnp.concatenate(pieces, axis=1), (16, width)).astype(BF)

        r16, low16, pos16, edge16 = (row(w) for w in range(4))
        one, zero = jnp.ones((), BF), jnp.zeros((), BF)
        ids = iota((16, width), 0).astype(F32).astype(BF)

        def hot(values, tile):
            return jnp.where(ids + jnp.asarray(16 * tile, BF) == values, one, zero)

        place = [hot(pos16, t) for t in range(8)]
        parts = []
        for k in range(HALF):
            at = jnp.where(low16 == jnp.asarray(k, BF), one, zero)
            parts += [b * at for b in place[:NP]]
        parts += [hot(edge16, 0), hot(edge16, 1)]
        left = jnp.concatenate(parts, axis=0)
        right = []
        for t in tiles:
            x = x_ref[128 * t : 128 * (t + 1), :]
            up = x * jnp.broadcast_to(upper[:, t : t + 1], (128, 128)).astype(BF)
            right.append(jnp.concatenate([x - up, up], axis=1))
        right = jnp.concatenate(right, axis=0)
        some = lax.dot_general(
            jnp.concatenate([hot(r16, 0), hot(r16, 1)], axis=0),
            jnp.concatenate(place, axis=0),
            (((1,), (1,)), ((), ())),
            preferred_element_type=F32,
        )
        if g == 0:
            acc[...] = dot(left, right)
            cnt[...] = some
        else:
            acc[...] += dot(left, right)
            cnt[...] += some

    def weight(a, b, shape):
        return jnp.broadcast_to(spread_ref[a : a + 1, b : b + 1], shape)

    def tile(r, p):
        lanes_of = slice((r // HALF) * 128, (r // HALF) * 128 + 128)
        base = (r % HALF) * TW + NQ * (p - 1)
        return pads[r, p // NP] if p in (0, NP + 1) else acc[base : base + NQ, lanes_of]

    for r in range(PH):
        lanes_of = slice((r // HALF) * 128, (r // HALF) * 128 + 128)
        at = MAIN + r % HALF
        pads[r, 0] = with_row(tile(r, NP), 1, acc[at : at + 1, lanes_of], 0)
        pads[r, 1] = with_row(tile(r, 1), NQ - 1, acc[at + HALF : at + HALF + 1, lanes_of], NQ - 1)

    number = jnp.transpose(jnp.concatenate([cnt[...], jnp.zeros((96, 128), F32)], axis=0))
    number = [
        with_row(number[TW - NQ : TW], 1, number[TW : TW + 1], 0),
        *(number[NQ * p : NQ * (p + 1)] for p in range(NP)),
        with_row(number[:NQ], NQ - 1, number[TW + 1 : TW + 2], NQ - 1),
    ]
    density = None
    for a in range(3):
        line = [sum(weight(a, b, (NQ, 128)) * number[p + b] for b in range(3)) for p in range(NP)]
        line = jnp.concatenate(line, axis=0)[:, a : a + TH]
        density = line if density is None else density + line
    scale = 1.0 / (1.0 + density)
    log_density = jnp.log(1.0 + density)

    weights = [[weight(a, b, (NQ, F)) for b in range(3)] for a in range(3)]

    def average(rows):
        for i in rows:
            wide = jnp.broadcast_to(scale[:, i : i + 1], (TW, F))
            for p in range(NP):
                data = None
                for a in range(3):
                    for b in range(3):
                        term = weights[a][b] * tile(i + a, p + b)
                        data = term if data is None else data + term
                at = i * TW + p * NQ
                mean[at : at + NQ, :] = (data * wide[p * NQ : (p + 1) * NQ]).astype(BF)

    def project(rows):
        return dot(jnp.concatenate([mean[i * TW : (i + 1) * TW, :] for i in rows], axis=0), win_ref[...])

    def finish(rows, out):
        for k, i in enumerate(rows):
            extra = jnp.broadcast_to(log_density[:, i : i + 1], (TW, C)) * wdens_ref[...]
            cell = (out[k * TW : (k + 1) * TW] + extra).astype(BF)
            grid_ref[i] = cell.reshape(NP, NQ, C)
            wide = cell.astype(F32)
            for c, at in enumerate((0, NQ, 5 * NQ - 1, 6 * NQ - 1)):
                cols[c, i : i + 1, :] = wide[at : at + 1]

    sets = [range(i, i + 4) for i in range(0, TH, 4)]
    average(sets[0])
    for n, rows in enumerate(sets):
        out = project(rows)
        if n + 1 < len(sets):
            average(sets[n + 1])
        finish(rows, out)
    west_ref[...] = cols[0:2].astype(BF)
    east_ref[...] = cols[2:4].astype(BF)

    lat_odd, _ = parities()
    rows = [grid_ref[at : at + 2].reshape(2 * TW, C) for at in (TH - 2, 0)]
    rows_a_ref[...], rows_b_ref[...] = chosen(lat_odd, *rows)


def chosen(odd, a, b):
    return jnp.where(odd == 0, a, b), jnp.where(odd == 0, b, a)


def silu(v):
    return v / (1.0 + jnp.exp(-v))


def column_kernel(rows_a_ref, rows_b_ref, west_ref, east_ref, a_ref, b_ref, tall):
    lat_odd, lon_odd = parities()
    tall[:, 24:, :] = jnp.zeros((4, 8, C), F32)
    for c in range(4):
        tall[c, 2 : 2 + TH, :] = (west_ref if c < 2 else east_ref)[c % 2].astype(F32)

    def halo(north, south):
        for ref, at in ((north, 0), (south, 2 + TH)):
            for k in range(2):
                for c, p in enumerate((0, 1, 4, 5)):
                    tile = ref[k * TW + p * NQ : k * TW + (p + 1) * NQ, :].astype(F32)
                    tall[c, at + k : at + k + 1, :] = tile[:1] if c < 2 else tile[NQ - 1 :]

    pl.when(lat_odd == 0)(lambda: halo(rows_b_ref, rows_a_ref))
    pl.when(lat_odd != 0)(lambda: halo(rows_a_ref, rows_b_ref))
    after, before = chosen(lon_odd, tall[2:4], tall[0:2])
    a_ref[...] = after.astype(BF)
    b_ref[...] = before.astype(BF)


def nine(weight, window):
    total = None
    for a in range(3):
        for b in range(3):
            term = dot(window(a, b), weight[3 * a + b])
            total = term if total is None else total + term
    return total


def rows_of(src, weight, start, count):
    return nine(weight, lambda a, b: src[start + a : start + a + count, b : b + NP].reshape(count * TW, C))


def padded(dst, at, tiles, first, last, before, after):
    dst[at, 1 : NP + 1] = tiles
    dst[at, 0] = with_row(last, 1, before, 0).astype(BF)
    dst[at, NP + 1] = with_row(first, NQ - 1, after, NQ - 1).astype(BF)


def spread_out(flat, at, tiles):
    for p in range(NP):
        for h in range(2):
            flat[h, pl.ds(at * TW + p, NQ, stride=NP), :] = tiles[p, :, 128 * h : 128 * (h + 1)]


def inner_one_kernel(grid_ref, one_ref, hp_ref, hcols_ref, gp):
    for g in range(TH):
        tile = grid_ref[g]
        first, last = tile[0].astype(F32), tile[NP - 1].astype(F32)
        padded(gp, g, tile, first, last, first[:1], last[NQ - 1 :])
    start = 0
    for count in (4, 4, 4, 4, 4, 2):
        value = silu(rows_of(gp, one_ref, start, count))
        for k in range(count):
            g = start + k + 2
            row = value[k * TW : (k + 1) * TW].reshape(NP, NQ, C)
            padded(hp_ref, g, row.astype(BF), row[0], row[NP - 1], row[0, :1], row[NP - 1, NQ - 1 :])
            for c, (p, q) in enumerate(((1, 0), (2, 0), (3, NQ - 1), (4, NQ - 1))):
                hcols_ref[c, g : g + 1, :] = row[p, q : q + 1]
        start += count


def inner_two_kernel(begin, end, hp_ref, grid_ref, two_ref, body_ref, flat):
    step = 4
    for i in range(begin, end, step):
        value = rows_of(hp_ref, two_ref, i, step).reshape(step, NP, NQ, C)
        value = value + grid_ref[i : i + step].astype(F32)
        at = i - begin
        for k in range(step):
            spread_out(flat, at + k, value[k])
        for h in range(2):
            block = flat[h, at * TW : (at + step) * TW, :].astype(BF).reshape(step, TW, 128)
            body_ref[at : at + step, :, 128 * h : 128 * (h + 1)] = block


def keeps():
    lat, _ = places()
    return jnp.where(lat > 0, 1.0, 0.0), jnp.where(lat < 15, 1.0, 0.0)


def edge_kernel(
    grid_ref,
    rows_a_ref,
    rows_b_ref,
    hp_ref,
    body_ref,
    rest_ref,
    one_ref,
    two_ref,
    out_ref,
    ecols_ref,
    partial_ref,
    gp,
    hr,
    flat,
    sems,
):
    copies = [
        pltpu.make_async_copy(body_ref, partial_ref.at[2:CUT], sems.at[0]),
        pltpu.make_async_copy(rest_ref, partial_ref.at[CUT : TH - 2], sems.at[1]),
    ]
    for copy in copies:
        copy.start()
    keep_top, keep_bottom = keeps()
    lat_odd, _ = parities()

    south, north = chosen(lat_odd, rows_a_ref[...], rows_b_ref[...])
    tiles = [north[k * TW : (k + 1) * TW, :].reshape(NP, NQ, C) for k in range(2)]
    tiles += [grid_ref[g] for g in (0, 1, TH - 2, TH - 1)]
    tiles += [south[k * TW : (k + 1) * TW, :].reshape(NP, NQ, C) for k in range(2)]
    for slot, tile in enumerate(tiles):
        first, last = tile[0].astype(F32), tile[NP - 1].astype(F32)
        padded(gp, slot, tile, first, last, first[:1], last[NQ - 1 :])

    def window(src, a, b):
        return jnp.concatenate(
            [src[at + a : at + a + 2, b : b + NP].reshape(2 * TW, C) for at in (0, 4)], axis=0
        )

    value = silu(nine(one_ref, functools.partial(window, gp)))
    for n, slot in enumerate((0, 1, 6, 7)):
        row = value[n * TW : (n + 1) * TW]
        if n == 0:
            row = row * keep_top
        if n == 3:
            row = row * keep_bottom
        row = row.reshape(NP, NQ, C)
        for c, (p, q) in enumerate(((1, 0), (2, 0), (3, NQ - 1), (4, NQ - 1))):
            ecols_ref[c, n : n + 1, :] = row[p, q : q + 1]
        padded(hr, slot, row.astype(BF), row[0], row[NP - 1], row[0, :1], row[NP - 1, NQ - 1 :])
    for slot, g in ((2, 2), (3, 3), (4, TH - 2), (5, TH - 1)):
        hr[slot] = hp_ref[g]
    value = nine(two_ref, functools.partial(window, hr))
    for n, i in enumerate((0, 1, TH - 2, TH - 1)):
        spread_out(flat, n, value[n * TW : (n + 1) * TW].reshape(NP, NQ, C) + grid_ref[i].astype(F32))
    for h in range(2):
        out_ref[:, :, 128 * h : 128 * (h + 1)] = flat[h].astype(BF).reshape(4, TW, 128)
    for copy in copies:
        copy.wait()


def last_kernel(
    sent_a_ref,
    sent_b_ref,
    got_a_ref,
    got_b_ref,
    hcols_ref,
    ecols_ref,
    body_ref,
    rest_ref,
    edge_ref,
    one_ref,
    two_ref,
    partial_ref,
    out_ref,
    cs,
    hc,
    oc,
    strips,
    sems,
):
    middle = slice(8, TW - 8)
    copies = [
        pltpu.make_async_copy(edge_ref.at[:2, middle], out_ref.at[:2, middle], sems.at[1]),
        pltpu.make_async_copy(edge_ref.at[2:, middle], out_ref.at[TH - 2 :, middle], sems.at[2]),
    ]
    for copy in copies:
        copy.start()
    keep_top, keep_bottom = keeps()
    _, lon_odd = parities()
    cs[:, 32:, :] = jnp.zeros((8, 8, C), F32)
    hc[:, 32:, :] = jnp.zeros((8, 8, C), F32)

    got_after, got_before = chosen(lon_odd, got_a_ref[...].astype(F32), got_b_ref[...].astype(F32))
    sent_after, sent_before = chosen(lon_odd, sent_a_ref[...].astype(F32), sent_b_ref[...].astype(F32))
    for n, value in enumerate((got_before, sent_before, sent_after, got_after)):
        cs[2 * n : 2 * n + 2, 0:32, :] = value

    def window(src, a, b):
        return jnp.concatenate([src[c + b, a : a + 32, :].astype(BF) for c in (0, 1, 4, 5)], axis=0)

    value = silu(nine(one_ref, functools.partial(window, cs)))
    line = iota((32, C), 0)
    for n, c in enumerate((0, 1, 6, 7)):
        column = value[32 * n : 32 * (n + 1)]
        column = jnp.where(line == 0, column * keep_top, column)
        hc[c, 0:32, :] = jnp.where(line == TH + 1, column * keep_bottom, column)
    for c in range(4):
        hc[2 + c, 0:32, :] = hcols_ref[c, 0:32, :]
        hc[2 + c, 0:2, :] = ecols_ref[c, 0:2, :]
        hc[2 + c, TH : TH + 2, :] = ecols_ref[c, 2:4, :]
    value = nine(two_ref, functools.partial(window, hc))
    for c in range(4):
        oc[c] = value[32 * c : 32 * c + TH] + cs[2 + c, 2 : 2 + TH, :]
    place = iota((8, C), 0)
    for n, (at, first) in enumerate(((0, 0), (TW - 8, 6))):
        for i in range(TH):
            if 2 <= i < CUT:
                rows, line = body_ref, i - 2
            elif CUT <= i < TH - 2:
                rows, line = rest_ref, i - CUT
            else:
                rows, line = edge_ref, i if i < 2 else i - TH + 4
            strip = rows[line, at : at + 8].astype(F32)
            for k in range(2):
                strip = jnp.where(place == first + k, oc[2 * n + k, i : i + 1, :], strip)
            strips[n, i] = strip.astype(BF)
        copies.append(pltpu.make_async_copy(strips.at[n], out_ref.at[:, at : at + 8], sems.at[3 + n]))
        copies[-1].start()
    for copy in copies:
        copy.wait()


def vmem(count):
    return [pl.BlockSpec(memory_space=pltpu.VMEM)] * count


def far(count):
    return [pl.BlockSpec(memory_space=pl.ANY)] * count


LIMIT = 40 * 1024 * 1024


def in_hbm(value):
    return pltpu.with_memory_space_constraint(value, pltpu.HBM)


def near(value):
    return pltpu.with_memory_space_constraint(value, pltpu.VMEM)


def send_call(features, cell_index, tile_rows):
    return pl.pallas_call(
        send_kernel,
        out_shape=pltpu.VMEM((SOURCES, PAIRS, 2, F), BF),
        in_specs=far(3),
        out_specs=vmem(1)[0],
        scratch_shapes=[
            pltpu.VMEM((96, 128), jnp.int32),
            pltpu.VMEM((1, 128), jnp.int32),
            pltpu.VMEM((2 * SOURCES, 128), F32),
            pltpu.VMEM((SOURCES, 1, 2, F), BF),
            pltpu.VMEM((128, 128), F32),
            pltpu.SemaphoreType.DMA((7,)),
        ],
        compiler_params=pltpu.CompilerParams(vmem_limit_bytes=LIMIT),
        name="send",
    )(
        in_hbm(features.reshape(SOURCES, PAIRS - 1, 2, F)),
        in_hbm(cell_index.reshape(96, 128)),
        in_hbm(tile_rows.reshape(1, 128)),
    )


def frame_call(received, spread, w_in, w_dens):
    return pl.pallas_call(
        frame_kernel,
        out_shape=(
            pltpu.VMEM((TH, NP, NQ, C), BF),
            *(pltpu.VMEM((2, TH, C), BF),) * 2,
            *(pltpu.VMEM((2 * TW, C), BF),) * 2,
        ),
        in_specs=vmem(5),
        out_specs=tuple(vmem(5)),
        scratch_shapes=[
            pltpu.VMEM((SOURCES * 2, 128), F32),
            pltpu.VMEM((4, 104, 128), F32),
            pltpu.VMEM((LHS, C), F32),
            pltpu.VMEM((32, 128), F32),
            pltpu.VMEM((PH, 2, NQ, F), F32),
            pltpu.VMEM((TH * TW, F), BF),
            pltpu.VMEM((4, TH, C), F32),
        ],
        compiler_params=pltpu.CompilerParams(vmem_limit_bytes=LIMIT),
        name="frame",
    )(near(received.reshape(SOURCES * ROWS, F)), near(received), near(spread), near(w_in), near(w_dens.reshape(1, C)))


def column_call(rows_a, rows_b, west, east):
    return pl.pallas_call(
        column_kernel,
        out_shape=(pltpu.VMEM((2, 32, C), BF),) * 2,
        in_specs=vmem(4),
        out_specs=tuple(vmem(2)),
        scratch_shapes=[pltpu.VMEM((4, 32, C), F32)],
        compiler_params=pltpu.CompilerParams(vmem_limit_bytes=LIMIT),
        name="column",
    )(*(near(value) for value in (rows_a, rows_b, west, east)))


def work(rows):
    return pl.CostEstimate(flops=2 * rows * TW * 9 * C * C, bytes_accessed=0, transcendentals=0)


def inner_one_call(grid, one):
    return pl.pallas_call(
        inner_one_kernel,
        out_shape=(pltpu.VMEM((TH + 2, NP + 2, NQ, C), BF), pltpu.VMEM((4, 40, C), F32)),
        in_specs=vmem(2),
        out_specs=tuple(vmem(2)),
        scratch_shapes=[pltpu.VMEM((TH, NP + 2, NQ, C), BF)],
        compiler_params=pltpu.CompilerParams(vmem_limit_bytes=LIMIT),
        cost_estimate=work(TH - 2),
        name="inner_one",
    )(near(grid), near(one))


def inner_two_call(begin, end, hp, grid, two):
    return pl.pallas_call(
        functools.partial(inner_two_kernel, begin, end),
        out_shape=pltpu.VMEM((end - begin, TW, C), BF),
        in_specs=vmem(3),
        out_specs=vmem(1)[0],
        scratch_shapes=[pltpu.VMEM((2, (end - begin) * TW, 128), F32)],
        compiler_params=pltpu.CompilerParams(vmem_limit_bytes=LIMIT),
        cost_estimate=work(end - begin),
    )(near(hp), near(grid), near(two))


def edge_call(*inside):
    return pl.pallas_call(
        edge_kernel,
        out_shape=(pltpu.VMEM((4, TW, C), BF), pltpu.VMEM((4, 8, C), F32), pltpu.HBM((TH, TW, C), BF)),
        in_specs=vmem(8),
        out_specs=(*vmem(2), *far(1)),
        scratch_shapes=[
            *(pltpu.VMEM((8, NP + 2, NQ, C), BF),) * 2,
            pltpu.VMEM((2, 4 * TW, 128), F32),
            pltpu.SemaphoreType.DMA((2,)),
        ],
        compiler_params=pltpu.CompilerParams(vmem_limit_bytes=LIMIT),
        cost_estimate=work(8),
        name="edge",
    )(*(near(value) for value in inside))


def last_call(partial, *inside):
    return pl.pallas_call(
        last_kernel,
        out_shape=jax.ShapeDtypeStruct((TH, TW, C), BF),
        in_specs=[*vmem(11), *far(1)],
        out_specs=far(1)[0],
        scratch_shapes=[
            *(pltpu.VMEM((8, 40, C), F32),) * 2,
            pltpu.VMEM((4, TH, C), F32),
            pltpu.VMEM((2, TH, 8, C), BF),
            pltpu.SemaphoreType.DMA((6,)),
        ],
        input_output_aliases={11: 0},
        compiler_params=pltpu.CompilerParams(vmem_limit_bytes=LIMIT),
        cost_estimate=work(3),
        name="last",
    )(*(near(value) for value in inside), partial)


def swaps(axis, first, around):
    count = lax.axis_size(axis)
    pairs = [(i, (i + 1) % count) for i in range(first, count, 2) if around or i + 1 < count]
    return pairs + [(j, i) for i, j in pairs]


def shards(features, cell_index, tile_rows, spread, w_in, w_dens, w_one, w_two):
    sent = send_call(features, cell_index, tile_rows)
    received = lax.all_to_all(sent, ("lat", "lon"), split_axis=0, concat_axis=0, tiled=True)
    grid, west, east, rows_a, rows_b = frame_call(received, spread, w_in, w_dens)
    one, two = w_one.reshape(9, C, C), w_two.reshape(9, C, C)
    rows_b = lax.ppermute(rows_b, "lat", swaps("lat", 1, False))
    rows_a = lax.ppermute(rows_a, "lat", swaps("lat", 0, False))
    hp, hcols = inner_one_call(grid, one)
    body = inner_two_call(2, CUT, hp, grid, two)
    sent_a, sent_b = column_call(rows_a, rows_b, west, east)
    got_b = lax.ppermute(sent_b, "lon", swaps("lon", 1, True))
    got_a = lax.ppermute(sent_a, "lon", swaps("lon", 0, True))
    rest = inner_two_call(CUT, TH - 2, hp, grid, two)
    edge, ecols, partial = edge_call(grid, rows_a, rows_b, hp, body, rest, one, two)
    return last_call(partial, sent_a, sent_b, got_a, got_b, hcols, ecols, body, rest, edge, one, two)


def solution(mesh):
    in_specs = (
        P(("lat", "lon"), None),
        P(("lat", "lon")),
        P(("lat", "lon")),
        P(),
        P(),
        P(),
        P(),
        P(),
    )
    out_specs = P("lat", "lon", None)
    return jax.shard_map(shards, mesh=mesh, in_specs=in_specs, out_specs=out_specs, check_vma=False)
```
